32 devices in a mesh: parts: 2 (over y), view: 4 (over x, core), tile: 4 (over z).
Axes of the slice: x: 2, y: 2, z: 4, core: 2. Of those that a mesh axis runs over, the one named last changes fastest.
Arguments:
- data: float32 [8, 32, 48, 32], P(('parts', 'view'), 'tile'), parts along dimension 0, may hold values from 0.25 to 4
- labels: int32 [8, 32, 48, 32], P(('parts', 'view'), 'tile'), parts along dimension 0, may hold values from 0 to 3
- kernel: float32 [4, 32, 9], P('view'), may hold values from 0.1 to 1
- offsets: int32 [4, 32], P('view'), may hold values from -2 to 2
Outputs:
- estimate: float32 [8, 32, 48, 32], P(('parts', 'view'), 'tile'), parts along dimension 0
The draws below stay inside these ranges and needn't reach their ends.
There are 2 independent parts, one for each index of `parts`. The reference program is written for one: setup_inputs(seed, part) draws one part's arguments, and reference() takes and returns one part's arrays. A program takes and returns all parts, laid end to end along the dimension named above; an argument that names none is the same for every part. Nothing has to cross between parts.
All inputs are finite; a program needn't handle non-finite values.
Results may differ from the reference program's by a relative error of at most 0.000088.
Values sent between devices are 32-bit elements; how exact they have to be, the bound alone decides.
A program may use at most 64 MiB of HBM per device.

```python
import math
import jax
import jax.numpy as jnp
from jax import lax

Y = 48
ITERS = 2
SWEEPS = 4
TAPS = 9
VIEWS = 4
X = 32
Z = 32


def plant(array, rng, smallest, top_value):
    shape = array.shape
    index_at = [jax.random.randint(jax.random.fold_in(rng, axis), (), 0, shape[axis]) for axis in range(len(shape))]
    array = array.at[tuple(index_at)].set(smallest)
    longest = shape.index(max(shape))
    index_at[longest] = (index_at[longest] + 1) % shape[longest]
    return array.at[tuple(index_at)].set(top_value)


def block_scale(own_key, extent, cuts, smallest, top_value):
    def one(dim, blocks):
        draws = jax.random.uniform(jax.random.fold_in(jax.random.fold_in(own_key, 6), dim), (blocks,), jnp.float32, smallest / len(cuts), top_value / len(cuts))
        return jnp.repeat(jnp.exp(draws), extent[dim] // blocks).reshape((-1,) + (1,) * (len(extent) - dim - 1))

    level = one(*cuts[0])
    for cut in cuts[1:]:
        level = level * one(*cut)
    return level


def setup_inputs(seed: int = 0, part: int = 0) -> dict:
    key_list = jax.random.split(jax.random.key(seed), 5)
    part_splits = jax.random.split(jax.random.fold_in(key_list[4], part), 5)
    return {
        "data": jnp.clip(jnp.exp(math.log(4.0) - 2.7725887 * jax.random.uniform(part_splits[0], (VIEWS, X, Y, Z), jnp.float32) ** block_scale(part_splits[0], (VIEWS, X, Y, Z), ((0, 4), (1, 4)), -0.2, 0.2)), 0.25, 4.0),
        "labels": plant(jax.random.randint(part_splits[1], (VIEWS, X, Y, Z), 0, 4), jax.random.fold_in(part_splits[1], 1), 0, 3).astype(jnp.int32),
        "kernel": jnp.clip(jnp.exp(math.log(1.0) - 2.3025851 * jax.random.uniform(key_list[2], (VIEWS, Z, TAPS), jnp.float32) ** block_scale(key_list[2], (VIEWS, Z, TAPS), ((0, 4),), -0.2, 0.2)), 0.1, 1.0),
        "offsets": plant(jax.random.randint(key_list[3], (VIEWS, Z), -2, 3), jax.random.fold_in(key_list[3], 1), -2, 2).astype(jnp.int32),
    }


WEAK = 0.2
TAU = 0.15

def band(kernel, offsets):
    depth_cells = kernel.shape[0]
    taps = jnp.arange(kernel.shape[1], dtype=jnp.int32) - 4
    depth = jnp.arange(depth_cells, dtype=jnp.int32)
    index = jnp.clip(depth[:, None] + taps[None, :] + offsets[:, None], 0, depth_cells - 1).astype(jnp.int32)
    weight = kernel / lax.optimization_barrier(jnp.sum(kernel, axis=1, keepdims=True))
    return (index, weight)

def blur_taps(field, index, weight):
    total = jnp.zeros_like(field)
    for k in range(index.shape[1]):
        total = total + jnp.take(field, index[:, k], axis=2) * weight[:, k]
    return total

def adjoint_taps(ratio, index, weight):
    total = jnp.zeros_like(ratio)
    for k in range(index.shape[1]):
        total = total.at[:, :, index[:, k]].add(ratio * weight[:, k])
    return total

def axis_term(field, region, axis):
    count = field.shape[axis]
    upper = lax.slice_in_dim(field, 1, count, axis=axis)
    lower = lax.slice_in_dim(field, 0, count - 1, axis=axis)
    same = jnp.where(lax.slice_in_dim(region, 1, count, axis=axis) == lax.slice_in_dim(region, 0, count - 1, axis=axis), 1.0, WEAK)
    flux = same * (upper - lower)
    after = [(0, 0)] * 3
    before = [(0, 0)] * 3
    after[axis] = (0, 1)
    before[axis] = (1, 0)
    return jnp.pad(flux, after) - jnp.pad(flux, before)

def sweep_whole(field, region):
    total = axis_term(field, region, 0) + axis_term(field, region, 1) + axis_term(field, region, 2)
    return field + TAU * total

def reference(data, labels, kernel, offsets):
    bands = [band(kernel[v], offsets[v]) for v in range(VIEWS)]
    current = [data[v] for v in range(VIEWS)]
    for step in range(ITERS):
        correction = [adjoint_taps(data[v] / blur_taps(current[v], *bands[v]), *bands[v]) for v in range(VIEWS)]
        paired = [jnp.sqrt(correction[v] * jnp.rot90(correction[(v + 2) % 4], 2, axes=(0, 2))) for v in range(VIEWS)]
        joined = [jnp.sqrt(paired[v] * jnp.rot90(paired[v ^ 1], 3 if v % 2 == 0 else 1, axes=(0, 2))) for v in range(VIEWS)]
        current = [current[v] * joined[v] for v in range(VIEWS)]
        for sweep in range(SWEEPS):
            current = [sweep_whole(current[v], labels[v]) for v in range(VIEWS)]
    return jnp.stack(current)
```

```python
import functools

import jax
import jax.numpy as jnp
from jax import lax
from jax.experimental import pallas as pl
from jax.experimental.pallas import tpu as pltpu
from jax.sharding import PartitionSpec as P

ITERS = 2
SWEEPS = 4


WEAK = 0.2
TAU = 0.15


def extended(cells, sides, width):
    for axis, dim in sides:
        count = lax.axis_size(axis)
        ends = count - 1
        head = lax.slice_in_dim(cells, 0, width, axis=dim)
        tail = lax.slice_in_dim(cells, cells.shape[dim] - width, cells.shape[dim], axis=dim)
        cells = jnp.concatenate(
            [
                lax.ppermute(tail, axis, [(i, (i + 1) % count) for i in range(ends)]),
                cells,
                lax.ppermute(head, axis, [((i + 1) % count, i) for i in range(ends)]),
            ],
            axis=dim,
        )
    return cells


def swapped(block, axis, stride):
    count = lax.axis_size(axis)
    route = []
    for low in range(count):
        high = low | 1 << stride
        if high != low and high < count:
            route += [(low, high), (high, low)]
    return lax.ppermute(block, axis, route)


def band(kernel, offsets):
    depth_cells = kernel.shape[0]
    taps = jnp.arange(kernel.shape[1], dtype=jnp.int32) - 4
    depth = jnp.arange(depth_cells, dtype=jnp.int32)
    index = jnp.clip(depth[:, None] + taps[None, :] + offsets[:, None], 0, depth_cells - 1)
    weight = kernel / jnp.sum(kernel, axis=1, keepdims=True)
    return (index, weight)


def axis_term(field, region, axis):
    count = field.shape[axis]
    upper = lax.slice_in_dim(field, 1, count, axis=axis)
    lower = lax.slice_in_dim(field, 0, count - 1, axis=axis)
    same = jnp.where(
        lax.slice_in_dim(region, 1, count, axis=axis)
        == lax.slice_in_dim(region, 0, count - 1, axis=axis),
        1.0,
        WEAK,
    )
    flux = same * (upper - lower)
    after = [(0, 0)] * 3
    before = [(0, 0)] * 3
    after[axis] = (0, 1)
    before[axis] = (1, 0)
    return jnp.pad(flux, after) - jnp.pad(flux, before)


def sweep_rows(field, region, first_row, total_rows):
    extent = field.shape[0]
    global_rows = first_row + jnp.arange(extent, dtype=jnp.int32)
    inside = ((global_rows >= 0) & (global_rows < total_rows)).astype(field.dtype)[:, None, None]
    same = jnp.where(region[1:] == region[:-1], 1.0, WEAK) * inside[1:] * inside[:-1]
    flux = same * (field[1:] - field[:-1])
    inner = field[1:-1]
    inner_labels = region[1:-1]
    total = (
        flux[1:] - flux[:-1] + axis_term(inner, inner_labels, 1) + axis_term(inner, inner_labels, 2)
    )
    return inner + TAU * total


def regroup(received, tiles):
    slab, rows, depth_cells = received.shape
    blocks = received.reshape(slab, rows, tiles, depth_cells // tiles)
    return blocks.transpose(3, 1, 2, 0).reshape(depth_cells // tiles, rows, depth_cells)


def on_device(data, labels, kernel, offsets):
    recorded = data[0]
    region = labels[0]
    index, weight = band(kernel[0], offsets[0])
    tiles = lax.axis_size("tile")
    slab, rows, depth_cells = recorded.shape
    total_rows = slab * tiles
    start = lax.axis_index("tile") * slab
    parity = lax.axis_index("view") % 2
    columns = jnp.arange(depth_cells, dtype=jnp.int32)
    matrix = jnp.sum(weight[:, :, None] * (index[:, :, None] == columns[None, None, :]), axis=1)
    label_ext = extended(region, (("tile", 0),), 4)
    current = recorded
    for step in range(ITERS):
        forward_flat = jnp.dot(
            current.reshape(-1, depth_cells), matrix.T, precision=lax.Precision.HIGHEST
        )
        field = recorded / forward_flat.reshape(current.shape)
        flat = jnp.dot(field.reshape(-1, depth_cells), matrix, precision=lax.Precision.HIGHEST)
        correction = flat.reshape(field.shape)
        turned = correction
        for repeat in range(2):
            turned = regroup(
                lax.all_to_all(
                    jnp.flip(turned, 2), "tile", split_axis=2, concat_axis=2, tiled=True
                ),
                tiles,
            )
        turned = swapped(turned, "view", 1)
        paired = jnp.sqrt(correction * turned)
        outgoing = jnp.where(parity == 0, jnp.flip(paired, 2), paired)
        rotated = regroup(
            lax.all_to_all(outgoing, "tile", split_axis=2, concat_axis=2, tiled=True), tiles
        )
        rotated = jnp.where(parity == 1, jnp.flip(rotated, 2), rotated)
        partner = swapped(rotated, "view", 0)
        current = current * jnp.sqrt(paired * partner)
        widened = extended(current, (("tile", 0),), 4)
        for sweep in range(SWEEPS):
            extent = widened.shape[0]
            widened = sweep_rows(
                widened, label_ext[sweep : sweep + extent], start - 4 + sweep, total_rows
            )
        current = widened
    return current[None]


def gathered(parts, b_of, slot, depth):
    fold = len(parts)
    lanes = parts[0].shape[1]
    total = None
    for k in range(fold):
        amount = (depth * (k - b_of[k])) % lanes
        piece = pltpu.roll(parts[k], amount, 1) if amount else parts[k]
        total = piece if total is None else jnp.where(slot == k, piece, total)
    return total


def turning(lanes, depth, flip_z):
    row_ids = lax.broadcasted_iota(jnp.int32, (lanes, lanes), 0)
    lane_ids = lax.broadcasted_iota(jnp.int32, (lanes, lanes), 1)
    same_block = (row_ids // depth) == (lane_ids // depth)
    aim = jnp.where(flip_z, depth - 1 - lane_ids % depth, lane_ids % depth)
    return same_block, jnp.where(same_block & (row_ids % depth == aim), 1.0, 0.0).astype(jnp.float32)


def exact(a, b):
    return jnp.dot(a, b, precision=lax.Precision.HIGHEST, preferred_element_type=jnp.float32)


def product(a, b, contract):
    return lax.dot_general(a, b, (contract, ((), ())), preferred_element_type=jnp.float32)


def halves(a):
    high = a.astype(jnp.bfloat16)
    return high, (a - high.astype(jnp.float32)).astype(jnp.bfloat16)


def permuted(a, turn):
    high, low = halves(a)
    turn = turn.astype(jnp.bfloat16)
    return product(high, turn, ((1,), (0,))) + product(low, turn, ((1,), (0,)))


def blurred(a, matrix, contract):
    high, low = halves(a)
    return product(high, matrix[0], contract) + (
        product(low, matrix[0], contract) + product(high, matrix[1], contract)
    )


def fused(tiles, data_ref, labels_ref, taps_ref, shift_ref, unpacked, raw, raw_labels, taps_buf, shift_buf, mixed, packed, packed_labels, held, held_labels, mats, est, coef, outgoing, incoming, leave, back, around, slab_coef, settled, sent, in_sem, data_sem, label_sem, mat_sem, swap_sem, back_sem, side_sem, send, send_side):
    mesh_id = pl.DeviceIdType.MESH
    slab, depth, rows = data_ref.shape[1:]
    lanes = packed.shape[2]
    fold = lanes // depth
    groups = rows // fold
    per_tile = groups // tiles
    width = held.shape[1]
    cells = held.shape[2]
    span = back.shape[1]
    pad = (span - slab) // 2
    view = lax.axis_index("view")
    tile = lax.axis_index("tile")
    part = lax.axis_index("parts")
    half = view // 2
    core = view % 2
    role = (half + tile) % 2
    flip_x = (view == 1) | (view == 2)
    flip_z = view >= 2

    def toggled(d):
        t = tile
        bit = 1
        while bit <= d:
            if d & bit:
                t = t + bit - 2 * bit * (t // bit % 2)
            bit *= 2
        return t

    others = [
        ((1 - half if away else half), toggled(d))
        for d in range(tiles - 1, -1, -1)
        for away in (1, 0)
        if d or away
    ]
    across = (part, 2 * half + 1 - core, tile)

    barrier = pltpu.get_barrier_semaphore()
    for h, t in others:
        pl.semaphore_signal(
            barrier, inc=1, device_id=(part, 2 * h + core, t), device_id_type=mesh_id
        )
    pl.semaphore_signal(barrier, inc=1, device_id=across, device_id_type=mesh_id)

    for source, target, sem in ((data_ref, raw, 0), (labels_ref, raw_labels, 1)):
        for x in range(slab):
            at = jnp.where(flip_x, slab - 1 - x, x)
            pltpu.make_async_copy(
                source.at[0, x],
                target.at[pl.ds(pl.multiple_of(at * depth, 8), depth)],
                in_sem.at[sem],
            ).start()
    small = [
        pltpu.make_async_copy(taps_ref, taps_buf, in_sem.at[2]),
        pltpu.make_async_copy(shift_ref, shift_buf, in_sem.at[3]),
    ]
    for copy in small:
        copy.start()

    def whole(ref, sem):
        pltpu.make_async_copy(ref, ref, sem).wait()

    same_block, turn = turning(lanes, depth, flip_z)
    slot = lax.broadcasted_iota(jnp.int32, (mixed.shape[1] // fold, lanes), 1) // depth
    blocks = slab * depth // lanes

    def pack(source, target, fill, turner):
        edge = jnp.full((1, slab, lanes), fill, jnp.float32)
        target[0:1] = edge
        target[groups + 1 : groups + 2] = edge
        for j in range(blocks):
            mixed[j, 0:rows] = turner(source[lanes * j : lanes * (j + 1), :])
        for j in range(blocks):
            parts = [
                mixed[j, pl.ds(b, mixed.shape[1] // fold, stride=fold), :] for b in range(fold)
            ]
            for k in range(fold):
                line = gathered(parts, [k] * fold, slot, depth)
                target[1 : groups + 1, fold * j + k, :] = line[:groups]

    def turned_labels(block):
        block = block.astype(jnp.float32).T.astype(jnp.bfloat16)
        return product(block, turn.astype(jnp.bfloat16), ((1,), (0,)))

    place = jnp.where(flip_x, tiles - 1 - tile, tile)
    spot = pl.ds(pl.multiple_of(place * slab, 8), slab)

    def scatter(source, target, sem):
        def piece(h, t):
            return source.at[pl.ds(per_tile * t + (h + t) % 2, width)]

        dst = target.at[half, :, spot, :]
        for h, t in others:
            pltpu.make_async_remote_copy(
                src_ref=piece(h, t),
                dst_ref=dst,
                send_sem=send,
                recv_sem=sem,
                device_id=(part, 2 * h + core, t),
                device_id_type=mesh_id,
            ).start()
        pltpu.make_async_copy(piece(half, tile), dst, sem).start()

    whole(raw, in_sem.at[0])
    pack(raw, packed, 1.0, lambda v: permuted(v.T, turn))
    pl.semaphore_wait(barrier, len(others) + 1)
    scatter(packed, held, data_sem)

    for copy in small:
        copy.wait()
    count = taps_buf.shape[0]
    taps = [jnp.concatenate([taps_buf[k]] * fold, axis=1) for k in range(count)]
    scale = taps[0]
    for k in range(1, count):
        scale = scale + taps[k]
    shift = jnp.concatenate([shift_buf[...]] * fold, axis=1)
    level = lax.broadcasted_iota(jnp.int32, (1, lanes), 1) % depth
    strip_row = lax.broadcasted_iota(jnp.int32, (depth, lanes), 0)
    strip_aim = jnp.where(flip_z, depth - 1 - strip_row, strip_row)
    strip = jnp.zeros((depth, lanes), jnp.float32)
    for k in range(count):
        index = jnp.clip(level + (k - 4) + shift, 0, depth - 1)
        strip = strip + jnp.where(index == strip_aim, taps[k] / scale, 0.0)
    strip = exact(strip, turn)
    mats[pl.ds(half, 1)] = strip[None]
    mat_copy = pltpu.make_async_remote_copy(
        src_ref=mats.at[half],
        dst_ref=mats.at[half],
        send_sem=send,
        recv_sem=mat_sem,
        device_id=(part, 2 * (1 - half) + core, tile),
        device_id_type=mesh_id,
    )
    mat_copy.start()

    whole(raw_labels, in_sem.at[1])
    pack(raw_labels, packed_labels, 0.0, turned_labels)
    scatter(packed_labels, held_labels, label_sem)

    inner_labels = packed_labels.at[pl.ds(1, groups)]

    def beside(side):
        onto = place + 1 - 2 * side
        t = jnp.where(flip_x, tiles - 1 - onto, onto)
        return pltpu.make_async_remote_copy(
            src_ref=inner_labels,
            dst_ref=around.at[:, pl.ds(2 * slab * side, slab), :],
            send_sem=send_side.at[side],
            recv_sem=side_sem.at[side],
            device_id=(part, view, jnp.clip(t, 0, tiles - 1)),
            device_id_type=mesh_id,
        )

    has_above = place < tiles - 1
    has_below = place > 0

    @pl.when(has_above)
    def _():
        beside(0).start()

    @pl.when(has_below)
    def _():
        beside(1).start()

    @pl.when(jnp.logical_not(has_below))
    def _():
        around[:, 0:slab, :] = jnp.zeros((groups, slab, lanes), jnp.float32)

    @pl.when(jnp.logical_not(has_above))
    def _():
        around[:, 2 * slab : 3 * slab, :] = jnp.zeros((groups, slab, lanes), jnp.float32)

    around[:, slab : 2 * slab, :] = packed_labels[1 : groups + 1]
    for s in range(2):
        for k in range(leave.shape[1]):
            leave[s, k, 0:pad] = jnp.zeros((pad, lanes), jnp.float32)
            leave[s, k, pad + cells : 2 * pad + cells] = jnp.zeros((pad, lanes), jnp.float32)

    lane = lax.broadcasted_iota(jnp.int32, (cells, lanes), 1)
    sub = lax.broadcasted_iota(jnp.int32, (cells, lanes), 0)
    first = per_tile * tile - 1 + role

    def lanes_of(field):
        return lane[: field.shape[0]]

    def ahead_y(fields, g):
        after = fields[(g + 1) % len(fields)]
        return jnp.where(
            lanes_of(fields[g]) < lanes - depth,
            pltpu.roll(fields[g], lanes - depth, 1),
            pltpu.roll(after, lanes - depth, 1),
        )

    def behind_y(fields, g):
        return jnp.where(
            lanes_of(fields[g]) < depth,
            pltpu.roll(fields[g - 1], depth, 1),
            pltpu.roll(fields[g], depth, 1),
        )

    def weights(regions, x_inside, y_first):
        strong, weak = TAU, TAU * WEAK
        high = regions[0].shape[0]
        count = len(regions)
        lane_of = lanes_of(regions[0])
        up_y = []
        for g in range(count):
            e_y = jnp.where(ahead_y(regions, g) == regions[g], strong, weak)
            y = fold * (y_first + g) + lane_of // depth
            up_y.append(jnp.where((y >= 0) & (y < rows - 1), e_y, 0.0))
        result = []
        for g in range(count):
            mine = regions[g]
            up_x = jnp.where(pltpu.roll(mine, high - 1, 0) == mine, strong, weak)
            up_x = jnp.where(x_inside, up_x, 0.0)
            up_z = jnp.where(pltpu.roll(mine, lanes - 1, 1) == mine, strong, weak)
            up_z = jnp.where(lane_of % depth == depth - 1, 0.0, up_z)
            down_x = pltpu.roll(up_x, 1, 0)
            down_z = pltpu.roll(up_z, 1, 1)
            down_y = behind_y(up_y, g)
            middle = 1.0 - (((up_x + down_x) + (up_z + down_z)) + (up_y[g] + down_y))
            result.append((middle, up_x, down_x, up_y[g], down_y, up_z, down_z))
        return result

    def swept(fields, factors, g):
        f = fields[g]
        high = f.shape[0]
        middle, up_x, down_x, up_y, down_y, up_z, down_z = factors
        return (
            (middle * f + up_x * pltpu.roll(f, high - 1, 0))
            + (down_x * pltpu.roll(f, 1, 0) + up_z * pltpu.roll(f, lanes - 1, 1))
        ) + (
            down_z * pltpu.roll(f, 1, 1)
            + (up_y * ahead_y(fields, g) + down_y * behind_y(fields, g))
        )

    def transposed(p, chosen):
        flipped = p.T
        result = []
        for g in chosen:
            piece = flipped[0:depth]
            if g:
                piece = pltpu.roll(piece, (lanes - depth * g) % lanes, 1)
            for b in range(1, fold):
                part_b = flipped[depth * b : depth * (b + 1)]
                amount = (depth * (b - g)) % lanes
                if amount:
                    part_b = pltpu.roll(part_b, amount, 1)
                piece = jnp.where(lane // depth == b, part_b, piece)
            result.append(piece)
        return result

    whole(held, data_sem)
    mat_copy.wait_recv()
    blurs = [
        halves(jnp.where(same_block, jnp.concatenate([mats[s]] * fold, axis=0), 0.0))
        for s in range(2)
    ]

    def paired_of(chosen, currents):
        corrections = []
        for s in range(2):
            recorded = jnp.concatenate([held[s, g] for g in chosen], axis=0)
            current = recorded if currents is None else jnp.concatenate(currents[s], axis=0)
            ratio = recorded / blurred(current, blurs[s], ((1,), (0,)))
            corrections.append(blurred(ratio, blurs[s], ((1,), (1,))))
        return jnp.sqrt(corrections[0] * corrections[1])

    def swapped_over(step, begin, size):
        copy = pltpu.make_async_remote_copy(
            src_ref=outgoing.at[step, pl.ds(begin, size)],
            dst_ref=incoming.at[step, pl.ds(begin, size)],
            send_sem=send,
            recv_sem=swap_sem.at[step],
            device_id=across,
            device_id_type=mesh_id,
        )
        copy.start()
        return copy

    paired = paired_of(range(width), None)
    for g, piece in enumerate(transposed(paired, range(width))):
        outgoing[0, g] = piece
    swap = swapped_over(0, 0, width)
    whole(held_labels, label_sem)
    for s in range(2):
        found = weights([held_labels[s, g] for g in range(width)], sub < cells - 1, first)
        for g in range(width):
            for i in range(len(found[g])):
                coef[i, s, g] = found[g][i]
    swap.wait_recv()
    joined = [
        jnp.sqrt(paired[cells * g : cells * (g + 1)] * incoming[0, g]) for g in range(width)
    ]
    fields = [[held[s, g] * joined[g] for g in range(width)] for s in range(2)]
    inner = range(1, width - 1)
    for sweep in range(SWEEPS):
        kept = inner if sweep == SWEEPS - 1 else range(width)
        fresh = [list(fields[s]) for s in range(2)]
        for s in range(2):
            for g in kept:
                factors = [coef[i, s, g] for i in range(coef.shape[0])]
                fresh[s][g] = swept(fields[s], factors, g)
        fields = fresh

    currents = [[fields[s][g] for g in inner] for s in range(2)]
    paired = paired_of(inner, currents)
    for s in range(2):
        for k in range(len(inner)):
            est[s, k] = currents[s][k]
    turned = transposed(jnp.concatenate([paired, paired], axis=0), range(len(inner)))
    for k, piece in enumerate(turned):
        outgoing[1, k] = piece
    swap = swapped_over(1, 0, len(inner))
    swap.wait_recv()
    for k in range(len(inner)):
        joined = jnp.sqrt(paired[cells * k : cells * (k + 1)] * incoming[1, k])
        for s in range(2):
            leave[s, k, pad : pad + cells] = est[s, k] * joined

    def window(h, t):
        flipped = core == 1 - h
        return pl.ds(pl.multiple_of(jnp.where(flipped, tiles - 1 - t, t) * slab, 8), span)

    own = pl.ds(per_tile * tile + role, len(inner))
    single = pl.ds(per_tile * tile + 2 * role, 1)
    for d in range(tiles - 1, -1, -1):
        t = toggled(d)
        pltpu.make_async_remote_copy(
            src_ref=leave.at[1 - half, pl.ds(role, 1), window(1 - half, t), :],
            dst_ref=back.at[single],
            send_sem=send,
            recv_sem=back_sem,
            device_id=(part, 2 * (1 - half) + core, t),
            device_id_type=mesh_id,
        ).start()
        mine = leave.at[half, :, window(half, t), :]
        if d == 0:
            pltpu.make_async_copy(mine, back.at[own], back_sem).start()
        else:
            pltpu.make_async_remote_copy(
                src_ref=mine,
                dst_ref=back.at[own],
                send_sem=send,
                recv_sem=back_sem,
                device_id=(part, 2 * half + core, t),
                device_id_type=mesh_id,
            ).start()

    @pl.when(has_below)
    def _():
        beside(0).wait_recv()

    @pl.when(has_above)
    def _():
        beside(1).wait_recv()

    x_at = place * slab - pad + sub[:span]
    x_inside = (x_at >= 0) & (x_at < cells - 1) & (sub[:span] < span - 1)
    found = weights([around[g, slab - pad : 2 * slab + pad] for g in range(groups)], x_inside, 0)
    for g in range(groups):
        for i in range(len(found[g])):
            slab_coef[i, g] = found[g][i]

    @pl.when(has_above)
    def _():
        beside(0).wait_send()

    @pl.when(has_below)
    def _():
        beside(1).wait_send()

    whole(sent, send)
    whole(back, back_sem)
    fields = [back[g] for g in range(groups)]
    for sweep in range(SWEEPS):
        fields = [
            swept(fields, [slab_coef[i, g] for i in range(slab_coef.shape[0])], g)
            for g in range(groups)
        ]
    for g in range(groups):
        settled[g] = fields[g][pad : pad + slab]
    for j in range(blocks):
        parts = []
        for k in range(fold):
            line = settled[:, fold * j + k, :]
            parts.append(
                jnp.concatenate(
                    [line, jnp.zeros((mixed.shape[1] // fold - groups, lanes), jnp.float32)], axis=0
                )
            )
        for b in range(fold):
            mixed[j, pl.ds(b, mixed.shape[1] // fold, stride=fold), :] = gathered(
                parts, [b] * fold, slot, depth
            )
        lined = permuted(mixed[j, 0:rows], turn).T
        for k in range(fold):
            x = fold * j + k
            at = jnp.where(flip_x, slab - 1 - x, x)
            unpacked[pl.ds(at, 1)] = lined[depth * k : depth * (k + 1)][None]


def by_rows(data, labels, kernel, offsets):
    tiles = lax.axis_size("tile")
    _, slab, rows, depth = data.shape
    fold = 128 // depth
    tall = -(-rows // (8 * fold)) * 8 * fold
    groups = rows // fold
    cells = slab * tiles
    width = 4
    kept = width - 2
    span = slab + 2 * SWEEPS
    flat = (slab * depth, rows)
    wide = (2, width, cells, 128)
    strips = (groups + 2, slab, 128)
    sent = (2 * (2 * tiles - 1) * width * slab + depth + (width + kept) * cells
            + ((tiles - 1) * kept + tiles) * span)
    dma = pltpu.SemaphoreType.DMA
    taps = kernel.transpose(2, 0, 1)
    ready = pl.pallas_call(
        functools.partial(fused, tiles),
        out_shape=pltpu.VMEM((slab, depth, rows), jnp.float32),
        in_specs=[pl.BlockSpec(memory_space=pltpu.HBM)] * 4,
        out_specs=pl.BlockSpec(memory_space=pltpu.VMEM),
        scratch_shapes=[
            pltpu.VMEM(flat, jnp.float32),
            pltpu.VMEM(flat, jnp.int32),
            pltpu.VMEM(taps.shape, jnp.float32),
            pltpu.VMEM(offsets.shape, jnp.int32),
            pltpu.VMEM((slab * depth // 128, tall, 128), jnp.float32),
            pltpu.VMEM(strips, jnp.float32),
            pltpu.VMEM(strips, jnp.float32),
            pltpu.VMEM(wide, jnp.float32),
            pltpu.VMEM(wide, jnp.float32),
            pltpu.VMEM((2, depth, 128), jnp.float32),
            pltpu.VMEM((2, kept, cells, 128), jnp.float32),
            pltpu.VMEM((7,) + wide, jnp.float32),
            pltpu.VMEM((ITERS,) + wide[1:], jnp.float32),
            pltpu.VMEM((ITERS,) + wide[1:], jnp.float32),
            pltpu.VMEM((2, kept, cells + span - slab, 128), jnp.float32),
            pltpu.VMEM((groups, span, 128), jnp.float32),
            pltpu.VMEM((groups, 3 * slab, 128), jnp.float32),
            pltpu.VMEM((7, groups, span, 128), jnp.float32),
            pltpu.VMEM((groups, slab, 128), jnp.float32),
            pltpu.VMEM((sent, 128), jnp.float32),
            dma((4,)),
            dma(()),
            dma(()),
            dma(()),
            dma((ITERS,)),
            dma(()),
            dma((2,)),
            dma(()),
            dma((2,)),
        ],
        compiler_params=pltpu.CompilerParams(
            collective_id=0, has_side_effects=True
        ),
    )(data.transpose(0, 1, 3, 2), labels.transpose(0, 1, 3, 2), taps, offsets)
    return ready[None].transpose(0, 1, 3, 2)


def fits(data, tiles, views):
    _, slab, rows, depth = data.shape
    return (
        views == 4
        and depth * 4 == 128
        and slab * tiles == depth
        and slab == 8
        and rows == 12 * tiles
    )


def program(data, labels, kernel, offsets):
    if fits(data, lax.axis_size("tile"), lax.axis_size("view")):
        return by_rows(data, labels, kernel, offsets)
    return on_device(data, labels, kernel, offsets)


def solution(mesh):
    placed = (
        P(("parts", "view"), "tile", None, None),
        P(("parts", "view"), "tile", None, None),
        P("view", None, None),
        P("view", None),
    )
    return jax.shard_map(
        program,
        mesh=mesh,
        in_specs=placed,
        out_specs=P(("parts", "view"), "tile", None, None),
        check_vma=False,
    )
```

```python
import functools

import jax
import jax.numpy as jnp
from jax import lax
from jax.experimental import pallas as pl
from jax.experimental.pallas import tpu as pltpu
from jax.sharding import PartitionSpec as P

ITERS = 2
SWEEPS = 4


WEAK = 0.2
TAU = 0.15


def extended(cells, sides, width):
    for axis, dim in sides:
        count = lax.axis_size(axis)
        ends = count - 1
        head = lax.slice_in_dim(cells, 0, width, axis=dim)
        tail = lax.slice_in_dim(cells, cells.shape[dim] - width, cells.shape[dim], axis=dim)
        cells = jnp.concatenate(
            [
                lax.ppermute(tail, axis, [(i, (i + 1) % count) for i in range(ends)]),
                cells,
                lax.ppermute(head, axis, [((i + 1) % count, i) for i in range(ends)]),
            ],
            axis=dim,
        )
    return cells


def swapped(block, axis, stride):
    count = lax.axis_size(axis)
    route = []
    for low in range(count):
        high = low | 1 << stride
        if high != low and high < count:
            route += [(low, high), (high, low)]
    return lax.ppermute(block, axis, route)


def band(kernel, offsets):
    depth_cells = kernel.shape[0]
    taps = jnp.arange(kernel.shape[1], dtype=jnp.int32) - 4
    depth = jnp.arange(depth_cells, dtype=jnp.int32)
    index = jnp.clip(depth[:, None] + taps[None, :] + offsets[:, None], 0, depth_cells - 1)
    weight = kernel / jnp.sum(kernel, axis=1, keepdims=True)
    return (index, weight)


def axis_term(field, region, axis):
    count = field.shape[axis]
    upper = lax.slice_in_dim(field, 1, count, axis=axis)
    lower = lax.slice_in_dim(field, 0, count - 1, axis=axis)
    same = jnp.where(
        lax.slice_in_dim(region, 1, count, axis=axis)
        == lax.slice_in_dim(region, 0, count - 1, axis=axis),
        1.0,
        WEAK,
    )
    flux = same * (upper - lower)
    after = [(0, 0)] * 3
    before = [(0, 0)] * 3
    after[axis] = (0, 1)
    before[axis] = (1, 0)
    return jnp.pad(flux, after) - jnp.pad(flux, before)


def sweep_rows(field, region, first_row, total_rows):
    extent = field.shape[0]
    global_rows = first_row + jnp.arange(extent, dtype=jnp.int32)
    inside = ((global_rows >= 0) & (global_rows < total_rows)).astype(field.dtype)[:, None, None]
    same = jnp.where(region[1:] == region[:-1], 1.0, WEAK) * inside[1:] * inside[:-1]
    flux = same * (field[1:] - field[:-1])
    inner = field[1:-1]
    inner_labels = region[1:-1]
    total = (
        flux[1:] - flux[:-1] + axis_term(inner, inner_labels, 1) + axis_term(inner, inner_labels, 2)
    )
    return inner + TAU * total


def regroup(received, tiles):
    slab, rows, depth_cells = received.shape
    blocks = received.reshape(slab, rows, tiles, depth_cells // tiles)
    return blocks.transpose(3, 1, 2, 0).reshape(depth_cells // tiles, rows, depth_cells)


def on_device(data, labels, kernel, offsets):
    recorded = data[0]
    region = labels[0]
    index, weight = band(kernel[0], offsets[0])
    tiles = lax.axis_size("tile")
    slab, rows, depth_cells = recorded.shape
    total_rows = slab * tiles
    start = lax.axis_index("tile") * slab
    parity = lax.axis_index("view") % 2
    columns = jnp.arange(depth_cells, dtype=jnp.int32)
    matrix = jnp.sum(weight[:, :, None] * (index[:, :, None] == columns[None, None, :]), axis=1)
    label_ext = extended(region, (("tile", 0),), 4)
    current = recorded
    for step in range(ITERS):
        forward_flat = jnp.dot(
            current.reshape(-1, depth_cells), matrix.T, precision=lax.Precision.HIGHEST
        )
        field = recorded / forward_flat.reshape(current.shape)
        flat = jnp.dot(field.reshape(-1, depth_cells), matrix, precision=lax.Precision.HIGHEST)
        correction = flat.reshape(field.shape)
        turned = correction
        for repeat in range(2):
            turned = regroup(
                lax.all_to_all(
                    jnp.flip(turned, 2), "tile", split_axis=2, concat_axis=2, tiled=True
                ),
                tiles,
            )
        turned = swapped(turned, "view", 1)
        paired = jnp.sqrt(correction * turned)
        outgoing = jnp.where(parity == 0, jnp.flip(paired, 2), paired)
        rotated = regroup(
            lax.all_to_all(outgoing, "tile", split_axis=2, concat_axis=2, tiled=True), tiles
        )
        rotated = jnp.where(parity == 1, jnp.flip(rotated, 2), rotated)
        partner = swapped(rotated, "view", 0)
        current = current * jnp.sqrt(paired * partner)
        widened = extended(current, (("tile", 0),), 4)
        for sweep in range(SWEEPS):
            extent = widened.shape[0]
            widened = sweep_rows(
                widened, label_ext[sweep : sweep + extent], start - 4 + sweep, total_rows
            )
        current = widened
    return current[None]


def gathered(parts, b_of, slot, depth):
    fold = len(parts)
    lanes = parts[0].shape[1]
    total = None
    for k in range(fold):
        amount = (depth * (k - b_of[k])) % lanes
        piece = pltpu.roll(parts[k], amount, 1) if amount else parts[k]
        total = piece if total is None else jnp.where(slot == k, piece, total)
    return total


def turning(lanes, depth, flip_z):
    row_ids = lax.broadcasted_iota(jnp.int32, (lanes, lanes), 0)
    lane_ids = lax.broadcasted_iota(jnp.int32, (lanes, lanes), 1)
    same_block = (row_ids // depth) == (lane_ids // depth)
    aim = jnp.where(flip_z, depth - 1 - lane_ids % depth, lane_ids % depth)
    return same_block, jnp.where(same_block & (row_ids % depth == aim), 1.0, 0.0).astype(jnp.float32)


def exact(a, b):
    return jnp.dot(a, b, precision=lax.Precision.HIGHEST, preferred_element_type=jnp.float32)


def product(a, b, contract):
    return lax.dot_general(a, b, (contract, ((), ())), preferred_element_type=jnp.float32)


def halves(a):
    high = a.astype(jnp.bfloat16)
    return high, (a - high.astype(jnp.float32)).astype(jnp.bfloat16)


def permuted(a, turn):
    high, low = halves(a)
    turn = turn.astype(jnp.bfloat16)
    return product(high, turn, ((1,), (0,))) + product(low, turn, ((1,), (0,)))


def blurred(a, matrix, contract):
    high, low = halves(a)
    return product(high, matrix[0], contract) + (
        product(low, matrix[0], contract) + product(high, matrix[1], contract)
    )


def fused(tiles, data_ref, labels_ref, taps_ref, shift_ref, unpacked, raw, raw_labels, taps_buf, shift_buf, mixed, packed, packed_labels, held, held_labels, mats, est, coef, outgoing, incoming, leave, back, around, slab_coef, settled, sent, in_sem, data_sem, label_sem, mat_sem, swap_sem, back_sem, side_sem, send, send_side, late_sem):
    mesh_id = pl.DeviceIdType.MESH
    slab, depth, rows = data_ref.shape[1:]
    lanes = packed.shape[2]
    fold = lanes // depth
    groups = rows // fold
    width = held.shape[1]
    keep = width - 2
    cells = held.shape[2]
    span = back.shape[1]
    pad = (span - slab) // 2
    view = lax.axis_index("view")
    tile = lax.axis_index("tile")
    part = lax.axis_index("parts")
    half = view // 2
    core = view % 2
    workers = tiles - 1
    works = tile < workers
    idle = tile >= workers
    flip_x = (view == 1) | (view == 2)
    flip_z = view >= 2

    def at_device(h, t):
        return (part, 2 * h + core, t)

    across = (part, 2 * half + 1 - core, tile)

    barrier = pltpu.get_barrier_semaphore()

    @pl.when(works)
    def _():
        for d in range(1, tiles):
            for h in (1 - half, half):
                pl.semaphore_signal(
                    barrier,
                    inc=1,
                    device_id=at_device(h, (tile + d) % tiles),
                    device_id_type=mesh_id,
                )
        pl.semaphore_signal(
            barrier, inc=1, device_id=at_device(1 - half, tile), device_id_type=mesh_id
        )

    pl.semaphore_signal(barrier, inc=1, device_id=across, device_id_type=mesh_id)

    for source, target, sem in ((data_ref, raw, 0), (labels_ref, raw_labels, 1)):
        for x in range(slab):
            at = jnp.where(flip_x, slab - 1 - x, x)
            pltpu.make_async_copy(
                source.at[0, x],
                target.at[pl.ds(pl.multiple_of(at * depth, 8), depth)],
                in_sem.at[sem],
            ).start()
    small = [
        pltpu.make_async_copy(taps_ref, taps_buf, in_sem.at[2]),
        pltpu.make_async_copy(shift_ref, shift_buf, in_sem.at[3]),
    ]
    for copy in small:
        copy.start()

    def whole(ref, sem):
        pltpu.make_async_copy(ref, ref, sem).wait()

    same_block, turn = turning(lanes, depth, flip_z)
    slot = lax.broadcasted_iota(jnp.int32, (mixed.shape[1] // fold, lanes), 1) // depth
    blocks = slab * depth // lanes

    def pack(source, target, fill, turner):
        edge = jnp.full((1, slab, lanes), fill, jnp.float32)
        target[0:1] = edge
        target[groups + 1 : groups + 2] = edge
        for j in range(blocks):
            mixed[j, 0:rows] = turner(source[lanes * j : lanes * (j + 1), :])
        for j in range(blocks):
            parts = [
                mixed[j, pl.ds(b, mixed.shape[1] // fold, stride=fold), :] for b in range(fold)
            ]
            for k in range(fold):
                line = gathered(parts, [k] * fold, slot, depth)
                target[1 : groups + 1, fold * j + k, :] = line[:groups]

    def turned_labels(block):
        block = block.astype(jnp.float32).T.astype(jnp.bfloat16)
        return product(block, turn.astype(jnp.bfloat16), ((1,), (0,)))

    place = jnp.where(flip_x, tiles - 1 - tile, tile)
    spot = pl.ds(pl.multiple_of(place * slab, 8), slab)

    def scatter(source, target, sem):
        def piece(h, t):
            return source.at[pl.ds(keep * (2 * t + h), width)]

        dst = target.at[half, :, spot, :]

        def over(h, t):
            pltpu.make_async_remote_copy(
                src_ref=piece(h, t),
                dst_ref=dst,
                send_sem=send,
                recv_sem=sem,
                device_id=at_device(h, t),
                device_id_type=mesh_id,
            ).start()

        @pl.when(idle)
        def _():
            over(1 - half, 0)
            over(half, 0)

        for d in range(1, workers):
            over(1 - half, (tile + d) % workers)
            over(half, (tile + d) % workers)

        @pl.when(works)
        def _():
            over(1 - half, tile)
            pltpu.make_async_copy(piece(half, tile), dst, sem).start()

    whole(raw, in_sem.at[0])
    pack(raw, packed, 1.0, lambda v: permuted(v.T, turn))
    pl.semaphore_wait(barrier, jnp.where(works, 2 * workers, 2 * workers + 1))

    @pl.when(idle)
    def _():
        for d in range(workers):
            for h in (1 - half, half):
                pl.semaphore_signal(
                    late_sem, inc=1, device_id=at_device(h, d), device_id_type=mesh_id
                )

    scatter(packed, held, data_sem)

    for copy in small:
        copy.wait()
    count = taps_buf.shape[0]
    taps = [jnp.concatenate([taps_buf[k]] * fold, axis=1) for k in range(count)]
    scale = taps[0]
    for k in range(1, count):
        scale = scale + taps[k]
    shift = jnp.concatenate([shift_buf[...]] * fold, axis=1)
    level = lax.broadcasted_iota(jnp.int32, (1, lanes), 1) % depth
    strip_row = lax.broadcasted_iota(jnp.int32, (depth, lanes), 0)
    strip_aim = jnp.where(flip_z, depth - 1 - strip_row, strip_row)
    strip = jnp.zeros((depth, lanes), jnp.float32)
    for k in range(count):
        index = jnp.clip(level + (k - 4) + shift, 0, depth - 1)
        strip = strip + jnp.where(index == strip_aim, taps[k] / scale, 0.0)
    strip = exact(strip, turn)
    mats[pl.ds(half, 1)] = strip[None]
    mat_copy = pltpu.make_async_remote_copy(
        src_ref=mats.at[half],
        dst_ref=mats.at[half],
        send_sem=send,
        recv_sem=mat_sem,
        device_id=at_device(1 - half, tile),
        device_id_type=mesh_id,
    )
    pl.when(works)(mat_copy.start)

    whole(raw_labels, in_sem.at[1])
    pack(raw_labels, packed_labels, 0.0, turned_labels)
    scatter(packed_labels, held_labels, label_sem)

    inner_labels = packed_labels.at[pl.ds(1, groups)]

    def beside(side):
        onto = place + 1 - 2 * side
        t = jnp.where(flip_x, tiles - 1 - onto, onto)
        return pltpu.make_async_remote_copy(
            src_ref=inner_labels,
            dst_ref=around.at[:, pl.ds(2 * slab * side, slab), :],
            send_sem=send_side.at[side],
            recv_sem=side_sem.at[side],
            device_id=(part, view, jnp.clip(t, 0, tiles - 1)),
            device_id_type=mesh_id,
        )

    has_above = place < tiles - 1
    has_below = place > 0

    def start_sides():
        @pl.when(has_above)
        def _():
            beside(0).start()

        @pl.when(has_below)
        def _():
            beside(1).start()

    @pl.when(jnp.logical_not(has_below))
    def _():
        around[:, 0:slab, :] = jnp.zeros((groups, slab, lanes), jnp.float32)

    @pl.when(jnp.logical_not(has_above))
    def _():
        around[:, 2 * slab : 3 * slab, :] = jnp.zeros((groups, slab, lanes), jnp.float32)

    around[:, slab : 2 * slab, :] = packed_labels[1 : groups + 1]
    for s in range(2):
        for k in range(leave.shape[1]):
            leave[s, k, 0:pad] = jnp.zeros((pad, lanes), jnp.float32)
            leave[s, k, pad + cells : 2 * pad + cells] = jnp.zeros((pad, lanes), jnp.float32)

    lane = lax.broadcasted_iota(jnp.int32, (cells, lanes), 1)
    sub = lax.broadcasted_iota(jnp.int32, (cells, lanes), 0)
    block = 2 * tile + half
    first = keep * block - 1

    def lanes_of(field):
        return lane[: field.shape[0]]

    def ahead_y(fields, g):
        after = fields[(g + 1) % len(fields)]
        return jnp.where(
            lanes_of(fields[g]) < lanes - depth,
            pltpu.roll(fields[g], lanes - depth, 1),
            pltpu.roll(after, lanes - depth, 1),
        )

    def behind_y(fields, g):
        return jnp.where(
            lanes_of(fields[g]) < depth,
            pltpu.roll(fields[g - 1], depth, 1),
            pltpu.roll(fields[g], depth, 1),
        )

    def weights(regions, x_inside, y_first):
        strong, weak = TAU, TAU * WEAK
        high = regions[0].shape[0]
        count = len(regions)
        lane_of = lanes_of(regions[0])
        up_y = []
        for g in range(count):
            e_y = jnp.where(ahead_y(regions, g) == regions[g], strong, weak)
            y = fold * (y_first + g) + lane_of // depth
            up_y.append(jnp.where((y >= 0) & (y < rows - 1), e_y, 0.0))
        result = []
        for g in range(count):
            mine = regions[g]
            up_x = jnp.where(pltpu.roll(mine, high - 1, 0) == mine, strong, weak)
            up_x = jnp.where(x_inside, up_x, 0.0)
            up_z = jnp.where(pltpu.roll(mine, lanes - 1, 1) == mine, strong, weak)
            up_z = jnp.where(lane_of % depth == depth - 1, 0.0, up_z)
            down_x = pltpu.roll(up_x, 1, 0)
            down_z = pltpu.roll(up_z, 1, 1)
            down_y = behind_y(up_y, g)
            middle = 1.0 - (((up_x + down_x) + (up_z + down_z)) + (up_y[g] + down_y))
            result.append((middle, up_x, down_x, up_y[g], down_y, up_z, down_z))
        return result

    def swept(fields, factors, g):
        f = fields[g]
        high = f.shape[0]
        middle, up_x, down_x, up_y, down_y, up_z, down_z = factors
        return (
            (middle * f + up_x * pltpu.roll(f, high - 1, 0))
            + (down_x * pltpu.roll(f, 1, 0) + up_z * pltpu.roll(f, lanes - 1, 1))
        ) + (
            down_z * pltpu.roll(f, 1, 1)
            + (up_y * ahead_y(fields, g) + down_y * behind_y(fields, g))
        )

    def transposed(p, chosen):
        flipped = p.T
        result = []
        for g in chosen:
            piece = flipped[0:depth]
            if g:
                piece = pltpu.roll(piece, (lanes - depth * g) % lanes, 1)
            for b in range(1, fold):
                part_b = flipped[depth * b : depth * (b + 1)]
                amount = (depth * (b - g)) % lanes
                if amount:
                    part_b = pltpu.roll(part_b, amount, 1)
                piece = jnp.where(lane // depth == b, part_b, piece)
            result.append(piece)
        return result

    @pl.when(works)
    def _():
        whole(held, data_sem)
        mat_copy.wait_recv()
        blurs = [
            halves(jnp.where(same_block, jnp.concatenate([mats[s]] * fold, axis=0), 0.0))
            for s in range(2)
        ]

        def paired_of(chosen, currents):
            corrections = []
            for s in range(2):
                recorded = jnp.concatenate([held[s, g] for g in chosen], axis=0)
                current = recorded if currents is None else jnp.concatenate(currents[s], axis=0)
                ratio = recorded / blurred(current, blurs[s], ((1,), (0,)))
                corrections.append(blurred(ratio, blurs[s], ((1,), (1,))))
            return jnp.sqrt(corrections[0] * corrections[1])

        def swapped_over(step, begin, size):
            copy = pltpu.make_async_remote_copy(
                src_ref=outgoing.at[step, pl.ds(begin, size)],
                dst_ref=incoming.at[step, pl.ds(begin, size)],
                send_sem=send,
                recv_sem=swap_sem.at[step],
                device_id=across,
                device_id_type=mesh_id,
            )
            copy.start()
            return copy

        paired = paired_of(range(width), None)
        for g, piece in enumerate(transposed(paired, range(width))):
            outgoing[0, g] = piece
        swap = swapped_over(0, 0, width)
        pl.semaphore_wait(late_sem, 2)
        start_sides()
        whole(held_labels, label_sem)
        for s in range(2):
            found = weights([held_labels[s, g] for g in range(width)], sub < cells - 1, first)
            for g in range(width):
                for i in range(len(found[g])):
                    coef[i, s, g] = found[g][i]
        swap.wait_recv()
        joined = [
            jnp.sqrt(paired[cells * g : cells * (g + 1)] * incoming[0, g]) for g in range(width)
        ]
        fields = [[held[s, g] * joined[g] for g in range(width)] for s in range(2)]
        inner = range(1, width - 1)
        for sweep in range(SWEEPS):
            kept = inner if sweep == SWEEPS - 1 else range(width)
            fresh = [list(fields[s]) for s in range(2)]
            for s in range(2):
                for g in kept:
                    factors = [coef[i, s, g] for i in range(coef.shape[0])]
                    fresh[s][g] = swept(fields[s], factors, g)
            fields = fresh

        currents = [[fields[s][g] for g in inner] for s in range(2)]
        paired = paired_of(inner, currents)
        for s in range(2):
            for k in range(len(inner)):
                est[s, k] = currents[s][k]
        turned = transposed(jnp.concatenate([paired, paired], axis=0), range(len(inner)))
        for k, piece in enumerate(turned):
            outgoing[1, k] = piece
        swap = swapped_over(1, 0, len(inner))
        swap.wait_recv()
        for k in range(len(inner)):
            joined = jnp.sqrt(paired[cells * k : cells * (k + 1)] * incoming[1, k])
            for s in range(2):
                leave[s, k, pad : pad + cells] = est[s, k] * joined

        def window(h, t):
            flipped = core == 1 - h
            return pl.ds(pl.multiple_of(jnp.where(flipped, tiles - 1 - t, t) * slab, 8), span)

        def returned(h, t):
            return pltpu.make_async_remote_copy(
                src_ref=leave.at[h, :, window(h, t), :],
                dst_ref=back.at[own],
                send_sem=send,
                recv_sem=back_sem,
                device_id=at_device(h, t),
                device_id_type=mesh_id,
            )

        own = pl.ds(keep * block, keep)
        for t in range(tiles):
            returned(1 - half, t).start()

            @pl.when(tile == t)
            def _():
                pltpu.make_async_copy(
                    leave.at[half, :, window(half, t), :], back.at[own], back_sem
                ).start()

            @pl.when(tile != t)
            def _():
                returned(half, t).start()

    pl.when(idle)(start_sides)

    @pl.when(has_below)
    def _():
        beside(0).wait_recv()

    @pl.when(has_above)
    def _():
        beside(1).wait_recv()

    x_at = place * slab - pad + sub[:span]
    x_inside = (x_at >= 0) & (x_at < cells - 1) & (sub[:span] < span - 1)
    found = weights([around[g, slab - pad : 2 * slab + pad] for g in range(groups)], x_inside, 0)
    for g in range(groups):
        for i in range(len(found[g])):
            slab_coef[i, g] = found[g][i]

    @pl.when(has_above)
    def _():
        beside(0).wait_send()

    @pl.when(has_below)
    def _():
        beside(1).wait_send()

    share = width * slab
    swaps = (width + keep) * cells
    busy = 2 * (2 * workers - 1) * share + depth + swaps + (2 * tiles - 1) * keep * span

    @pl.when(works)
    def _():
        whole(sent.at[pl.ds(0, busy)], send)

    @pl.when(idle)
    def _():
        whole(sent.at[pl.ds(0, 4 * workers * share)], send)

    whole(back, back_sem)
    fields = [back[g] for g in range(groups)]
    for sweep in range(SWEEPS):
        fields = [
            swept(fields, [slab_coef[i, g] for i in range(slab_coef.shape[0])], g)
            for g in range(groups)
        ]
    for g in range(groups):
        settled[g] = fields[g][pad : pad + slab]
    for j in range(blocks):
        parts = []
        for k in range(fold):
            line = settled[:, fold * j + k, :]
            parts.append(
                jnp.concatenate(
                    [line, jnp.zeros((mixed.shape[1] // fold - groups, lanes), jnp.float32)], axis=0
                )
            )
        for b in range(fold):
            mixed[j, pl.ds(b, mixed.shape[1] // fold, stride=fold), :] = gathered(
                parts, [b] * fold, slot, depth
            )
        lined = permuted(mixed[j, 0:rows], turn).T
        for k in range(fold):
            x = fold * j + k
            at = jnp.where(flip_x, slab - 1 - x, x)
            unpacked[pl.ds(at, 1)] = lined[depth * k : depth * (k + 1)][None]


def by_rows(data, labels, kernel, offsets):
    tiles = lax.axis_size("tile")
    _, slab, rows, depth = data.shape
    fold = 128 // depth
    tall = -(-rows // (8 * fold)) * 8 * fold
    groups = rows // fold
    cells = slab * tiles
    width = 4
    kept = width - 2
    span = slab + 2 * SWEEPS
    flat = (slab * depth, rows)
    wide = (2, width, cells, 128)
    strips = (groups + 2, slab, 128)
    sent = 4 * tiles * width * slab + depth + (width + kept) * cells + 2 * tiles * kept * span
    dma = pltpu.SemaphoreType.DMA
    taps = kernel.transpose(2, 0, 1)
    ready = pl.pallas_call(
        functools.partial(fused, tiles),
        out_shape=pltpu.VMEM((slab, depth, rows), jnp.float32),
        in_specs=[pl.BlockSpec(memory_space=pltpu.HBM)] * 4,
        out_specs=pl.BlockSpec(memory_space=pltpu.VMEM),
        scratch_shapes=[
            pltpu.VMEM(flat, jnp.float32),
            pltpu.VMEM(flat, jnp.int32),
            pltpu.VMEM(taps.shape, jnp.float32),
            pltpu.VMEM(offsets.shape, jnp.int32),
            pltpu.VMEM((slab * depth // 128, tall, 128), jnp.float32),
            pltpu.VMEM(strips, jnp.float32),
            pltpu.VMEM(strips, jnp.float32),
            pltpu.VMEM(wide, jnp.float32),
            pltpu.VMEM(wide, jnp.float32),
            pltpu.VMEM((2, depth, 128), jnp.float32),
            pltpu.VMEM((2, kept, cells, 128), jnp.float32),
            pltpu.VMEM((7,) + wide, jnp.float32),
            pltpu.VMEM((ITERS,) + wide[1:], jnp.float32),
            pltpu.VMEM((ITERS,) + wide[1:], jnp.float32),
            pltpu.VMEM((2, kept, cells + span - slab, 128), jnp.float32),
            pltpu.VMEM((groups, span, 128), jnp.float32),
            pltpu.VMEM((groups, 3 * slab, 128), jnp.float32),
            pltpu.VMEM((7, groups, span, 128), jnp.float32),
            pltpu.VMEM((groups, slab, 128), jnp.float32),
            pltpu.VMEM((sent, 128), jnp.float32),
            dma((4,)),
            dma(()),
            dma(()),
            dma(()),
            dma((ITERS,)),
            dma(()),
            dma((2,)),
            dma(()),
            dma((2,)),
            pltpu.SemaphoreType.REGULAR,
        ],
        compiler_params=pltpu.CompilerParams(
            collective_id=0, has_side_effects=True
        ),
    )(data.transpose(0, 1, 3, 2), labels.transpose(0, 1, 3, 2), taps, offsets)
    return ready[None].transpose(0, 1, 3, 2)


def fits(data, tiles, views):
    _, slab, rows, depth = data.shape
    return (
        views == 4
        and depth * 4 == 128
        and slab * tiles == depth
        and slab == 8
        and tiles > 1
        and rows == 16 * (tiles - 1)
    )


def program(data, labels, kernel, offsets):
    if fits(data, lax.axis_size("tile"), lax.axis_size("view")):
        return by_rows(data, labels, kernel, offsets)
    return on_device(data, labels, kernel, offsets)


def solution(mesh):
    placed = (
        P(("parts", "view"), "tile", None, None),
        P(("parts", "view"), "tile", None, None),
        P("view", None, None),
        P("view", None),
    )
    return jax.shard_map(
        program,
        mesh=mesh,
        in_specs=placed,
        out_specs=P(("parts", "view"), "tile", None, None),
        check_vma=False,
    )
```

```python
import functools

import jax
import jax.numpy as jnp
from jax import lax
from jax.experimental import pallas as pl
from jax.experimental.pallas import tpu as pltpu
from jax.sharding import PartitionSpec as P

ITERS = 2
SWEEPS = 4


WEAK = 0.2
TAU = 0.15


def extended(cells, sides, width):
    for axis, dim in sides:
        count = lax.axis_size(axis)
        ends = count - 1
        head = lax.slice_in_dim(cells, 0, width, axis=dim)
        tail = lax.slice_in_dim(cells, cells.shape[dim] - width, cells.shape[dim], axis=dim)
        cells = jnp.concatenate(
            [
                lax.ppermute(tail, axis, [(i, (i + 1) % count) for i in range(ends)]),
                cells,
                lax.ppermute(head, axis, [((i + 1) % count, i) for i in range(ends)]),
            ],
            axis=dim,
        )
    return cells


def swapped(block, axis, stride):
    count = lax.axis_size(axis)
    route = []
    for low in range(count):
        high = low | 1 << stride
        if high != low and high < count:
            route += [(low, high), (high, low)]
    return lax.ppermute(block, axis, route)


def band(kernel, offsets):
    depth_cells = kernel.shape[0]
    taps = jnp.arange(kernel.shape[1], dtype=jnp.int32) - 4
    depth = jnp.arange(depth_cells, dtype=jnp.int32)
    index = jnp.clip(depth[:, None] + taps[None, :] + offsets[:, None], 0, depth_cells - 1)
    weight = kernel / jnp.sum(kernel, axis=1, keepdims=True)
    return (index, weight)


def axis_term(field, region, axis):
    count = field.shape[axis]
    upper = lax.slice_in_dim(field, 1, count, axis=axis)
    lower = lax.slice_in_dim(field, 0, count - 1, axis=axis)
    same = jnp.where(
        lax.slice_in_dim(region, 1, count, axis=axis)
        == lax.slice_in_dim(region, 0, count - 1, axis=axis),
        1.0,
        WEAK,
    )
    flux = same * (upper - lower)
    after = [(0, 0)] * 3
    before = [(0, 0)] * 3
    after[axis] = (0, 1)
    before[axis] = (1, 0)
    return jnp.pad(flux, after) - jnp.pad(flux, before)


def sweep_rows(field, region, first_row, total_rows):
    extent = field.shape[0]
    global_rows = first_row + jnp.arange(extent, dtype=jnp.int32)
    inside = ((global_rows >= 0) & (global_rows < total_rows)).astype(field.dtype)[:, None, None]
    same = jnp.where(region[1:] == region[:-1], 1.0, WEAK) * inside[1:] * inside[:-1]
    flux = same * (field[1:] - field[:-1])
    inner = field[1:-1]
    inner_labels = region[1:-1]
    total = (
        flux[1:] - flux[:-1] + axis_term(inner, inner_labels, 1) + axis_term(inner, inner_labels, 2)
    )
    return inner + TAU * total


def regroup(received, tiles):
    slab, rows, depth_cells = received.shape
    blocks = received.reshape(slab, rows, tiles, depth_cells // tiles)
    return blocks.transpose(3, 1, 2, 0).reshape(depth_cells // tiles, rows, depth_cells)


def on_device(data, labels, kernel, offsets):
    recorded = data[0]
    region = labels[0]
    index, weight = band(kernel[0], offsets[0])
    tiles = lax.axis_size("tile")
    slab, rows, depth_cells = recorded.shape
    total_rows = slab * tiles
    start = lax.axis_index("tile") * slab
    parity = lax.axis_index("view") % 2
    columns = jnp.arange(depth_cells, dtype=jnp.int32)
    matrix = jnp.sum(weight[:, :, None] * (index[:, :, None] == columns[None, None, :]), axis=1)
    label_ext = extended(region, (("tile", 0),), 4)
    current = recorded
    for step in range(ITERS):
        forward_flat = jnp.dot(
            current.reshape(-1, depth_cells), matrix.T, precision=lax.Precision.HIGHEST
        )
        field = recorded / forward_flat.reshape(current.shape)
        flat = jnp.dot(field.reshape(-1, depth_cells), matrix, precision=lax.Precision.HIGHEST)
        correction = flat.reshape(field.shape)
        turned = correction
        for repeat in range(2):
            turned = regroup(
                lax.all_to_all(
                    jnp.flip(turned, 2), "tile", split_axis=2, concat_axis=2, tiled=True
                ),
                tiles,
            )
        turned = swapped(turned, "view", 1)
        paired = jnp.sqrt(correction * turned)
        outgoing = jnp.where(parity == 0, jnp.flip(paired, 2), paired)
        rotated = regroup(
            lax.all_to_all(outgoing, "tile", split_axis=2, concat_axis=2, tiled=True), tiles
        )
        rotated = jnp.where(parity == 1, jnp.flip(rotated, 2), rotated)
        partner = swapped(rotated, "view", 0)
        current = current * jnp.sqrt(paired * partner)
        widened = extended(current, (("tile", 0),), 4)
        for sweep in range(SWEEPS):
            extent = widened.shape[0]
            widened = sweep_rows(
                widened, label_ext[sweep : sweep + extent], start - 4 + sweep, total_rows
            )
        current = widened
    return current[None]


def gathered(parts, b_of, slot, depth):
    fold = len(parts)
    lanes = parts[0].shape[1]
    total = None
    for k in range(fold):
        amount = (depth * (k - b_of[k])) % lanes
        piece = pltpu.roll(parts[k], amount, 1) if amount else parts[k]
        total = piece if total is None else jnp.where(slot == k, piece, total)
    return total


def turning(lanes, depth, flip_z):
    row_ids = lax.broadcasted_iota(jnp.int32, (lanes, lanes), 0)
    lane_ids = lax.broadcasted_iota(jnp.int32, (lanes, lanes), 1)
    same_block = (row_ids // depth) == (lane_ids // depth)
    aim = jnp.where(flip_z, depth - 1 - lane_ids % depth, lane_ids % depth)
    return same_block, jnp.where(same_block & (row_ids % depth == aim), 1.0, 0.0).astype(jnp.float32)


def exact(a, b):
    return jnp.dot(a, b, precision=lax.Precision.HIGHEST, preferred_element_type=jnp.float32)


def product(a, b, contract):
    return lax.dot_general(a, b, (contract, ((), ())), preferred_element_type=jnp.float32)


def halves(a):
    high = a.astype(jnp.bfloat16)
    return high, (a - high.astype(jnp.float32)).astype(jnp.bfloat16)


def permuted(a, turn):
    high, low = halves(a)
    turn = turn.astype(jnp.bfloat16)
    return product(high, turn, ((1,), (0,))) + product(low, turn, ((1,), (0,)))


def blurred(a, matrix, contract):
    high, low = halves(a)
    return product(high, matrix[0], contract) + (
        product(low, matrix[0], contract) + product(high, matrix[1], contract)
    )


def fused(tiles, data_ref, labels_ref, taps_ref, shift_ref, unpacked, raw, raw_labels, taps_buf, shift_buf, mixed, packed, packed_labels, held, held_labels, mats, est, coef, outgoing, incoming, leave, back, around, slab_coef, settled, sent, in_sem, data_sem, label_sem, mat_sem, swap_sem, back_sem, side_sem, send, send_side, late_sem):
    mesh_id = pl.DeviceIdType.MESH
    slab, depth, rows = data_ref.shape[1:]
    lanes = packed.shape[2]
    fold = lanes // depth
    groups = rows // fold
    width = held.shape[1]
    keep = width - 2
    cells = held.shape[2]
    span = back.shape[1]
    pad = (span - slab) // 2
    view = lax.axis_index("view")
    tile = lax.axis_index("tile")
    part = lax.axis_index("parts")
    half = view // 2
    core = view % 2
    workers = tiles - 2
    ends = tiles - workers
    works = (tile > 0) & (tile <= workers)
    idle = (tile == 0) | (tile > workers)
    flip_x = (view == 1) | (view == 2)
    flip_z = view >= 2

    def at_device(h, t):
        return (part, 2 * h + core, t)

    across = (part, 2 * half + 1 - core, tile)

    barrier = pltpu.get_barrier_semaphore()

    @pl.when(works)
    def _():
        for d in range(1, tiles):
            for h in (1 - half, half):
                pl.semaphore_signal(
                    barrier,
                    inc=1,
                    device_id=at_device(h, (tile + d) % tiles),
                    device_id_type=mesh_id,
                )
        pl.semaphore_signal(
            barrier, inc=1, device_id=at_device(1 - half, tile), device_id_type=mesh_id
        )

    pl.semaphore_signal(barrier, inc=1, device_id=across, device_id_type=mesh_id)

    for source, target, sem in ((data_ref, raw, 0), (labels_ref, raw_labels, 1)):
        for x in range(slab):
            at = jnp.where(flip_x, slab - 1 - x, x)
            pltpu.make_async_copy(
                source.at[0, x],
                target.at[pl.ds(pl.multiple_of(at * depth, 8), depth)],
                in_sem.at[sem],
            ).start()
    small = [
        pltpu.make_async_copy(taps_ref, taps_buf, in_sem.at[2]),
        pltpu.make_async_copy(shift_ref, shift_buf, in_sem.at[3]),
    ]
    for copy in small:
        copy.start()

    def whole(ref, sem):
        pltpu.make_async_copy(ref, ref, sem).wait()

    same_block, turn = turning(lanes, depth, flip_z)
    slot = lax.broadcasted_iota(jnp.int32, (mixed.shape[1] // fold, lanes), 1) // depth
    blocks = slab * depth // lanes

    def pack(source, target, fill, turner):
        edge = jnp.full((1, slab, lanes), fill, jnp.float32)
        target[0:1] = edge
        target[groups + 1 : groups + 2] = edge
        for j in range(blocks):
            mixed[j, 0:rows] = turner(source[lanes * j : lanes * (j + 1), :])
        for j in range(blocks):
            parts = [
                mixed[j, pl.ds(b, mixed.shape[1] // fold, stride=fold), :] for b in range(fold)
            ]
            for k in range(fold):
                line = gathered(parts, [k] * fold, slot, depth)
                target[1 : groups + 1, fold * j + k, :] = line[:groups]

    def turned_labels(block):
        block = block.astype(jnp.float32).T.astype(jnp.bfloat16)
        return product(block, turn.astype(jnp.bfloat16), ((1,), (0,)))

    place = jnp.where(flip_x, tiles - 1 - tile, tile)
    spot = pl.ds(pl.multiple_of(place * slab, 8), slab)

    def scatter(source, target, sem):
        def piece(h, t):
            return source.at[pl.ds(keep * (2 * (t - 1) + h), width)]

        dst = target.at[half, :, spot, :]

        def over(h, t):
            pltpu.make_async_remote_copy(
                src_ref=piece(h, t),
                dst_ref=dst,
                send_sem=send,
                recv_sem=sem,
                device_id=at_device(h, t),
                device_id_type=mesh_id,
            ).start()

        @pl.when(idle)
        def _():
            for d in range(workers):
                t = jnp.where(tile == 0, workers - d, 1 + d)
                over(1 - half, t)
                over(half, t)

        @pl.when(works)
        def _():
            for d in range(1, workers):
                t = 1 + (tile - 1 + d) % workers
                over(1 - half, t)
                over(half, t)
            over(1 - half, tile)
            pltpu.make_async_copy(piece(half, tile), dst, sem).start()

    whole(raw, in_sem.at[0])
    pack(raw, packed, 1.0, lambda v: permuted(v.T, turn))
    pl.semaphore_wait(barrier, jnp.where(works, 2 * workers, 2 * workers + 1))

    @pl.when(idle)
    def _():
        for t in range(1, workers + 1):
            for h in (1 - half, half):
                pl.semaphore_signal(
                    late_sem, inc=1, device_id=at_device(h, t), device_id_type=mesh_id
                )

    scatter(packed, held, data_sem)

    for copy in small:
        copy.wait()
    count = taps_buf.shape[0]
    taps = [jnp.concatenate([taps_buf[k]] * fold, axis=1) for k in range(count)]
    scale = taps[0]
    for k in range(1, count):
        scale = scale + taps[k]
    shift = jnp.concatenate([shift_buf[...]] * fold, axis=1)
    level = lax.broadcasted_iota(jnp.int32, (1, lanes), 1) % depth
    strip_row = lax.broadcasted_iota(jnp.int32, (depth, lanes), 0)
    strip_aim = jnp.where(flip_z, depth - 1 - strip_row, strip_row)
    strip = jnp.zeros((depth, lanes), jnp.float32)
    for k in range(count):
        index = jnp.clip(level + (k - 4) + shift, 0, depth - 1)
        strip = strip + jnp.where(index == strip_aim, taps[k] / scale, 0.0)
    strip = exact(strip, turn)
    mats[pl.ds(half, 1)] = strip[None]
    mat_copy = pltpu.make_async_remote_copy(
        src_ref=mats.at[half],
        dst_ref=mats.at[half],
        send_sem=send,
        recv_sem=mat_sem,
        device_id=at_device(1 - half, tile),
        device_id_type=mesh_id,
    )
    pl.when(works)(mat_copy.start)

    whole(raw_labels, in_sem.at[1])
    pack(raw_labels, packed_labels, 0.0, turned_labels)
    pl.when((core == 1) & idle)(lambda: pl.delay(1200))
    scatter(packed_labels, held_labels, label_sem)

    inner_labels = packed_labels.at[pl.ds(1, groups)]

    def beside(side):
        onto = place + 1 - 2 * side
        t = jnp.where(flip_x, tiles - 1 - onto, onto)
        return pltpu.make_async_remote_copy(
            src_ref=inner_labels,
            dst_ref=around.at[:, pl.ds(2 * slab * side, slab), :],
            send_sem=send_side.at[side],
            recv_sem=side_sem.at[side],
            device_id=(part, view, jnp.clip(t, 0, tiles - 1)),
            device_id_type=mesh_id,
        )

    has_above = place < tiles - 1
    has_below = place > 0

    def start_sides():
        @pl.when(has_above)
        def _():
            beside(0).start()

        @pl.when(has_below)
        def _():
            beside(1).start()

    @pl.when(jnp.logical_not(has_below))
    def _():
        around[:, 0:slab, :] = jnp.zeros((groups, slab, lanes), jnp.float32)

    @pl.when(jnp.logical_not(has_above))
    def _():
        around[:, 2 * slab : 3 * slab, :] = jnp.zeros((groups, slab, lanes), jnp.float32)

    around[:, slab : 2 * slab, :] = packed_labels[1 : groups + 1]
    for s in range(2):
        for k in range(leave.shape[1]):
            leave[s, k, 0:pad] = jnp.zeros((pad, lanes), jnp.float32)
            leave[s, k, pad + cells : 2 * pad + cells] = jnp.zeros((pad, lanes), jnp.float32)

    lane = lax.broadcasted_iota(jnp.int32, (cells, lanes), 1)
    sub = lax.broadcasted_iota(jnp.int32, (cells, lanes), 0)
    block = 2 * (tile - 1) + half
    first = keep * block - 1

    def lanes_of(field):
        return lane[: field.shape[0]]

    def ahead_y(fields, g):
        after = fields[(g + 1) % len(fields)]
        return jnp.where(
            lanes_of(fields[g]) < lanes - depth,
            pltpu.roll(fields[g], lanes - depth, 1),
            pltpu.roll(after, lanes - depth, 1),
        )

    def behind_y(fields, g):
        return jnp.where(
            lanes_of(fields[g]) < depth,
            pltpu.roll(fields[g - 1], depth, 1),
            pltpu.roll(fields[g], depth, 1),
        )

    def weights(regions, x_inside, y_first):
        strong, weak = TAU, TAU * WEAK
        high = regions[0].shape[0]
        count = len(regions)
        lane_of = lanes_of(regions[0])
        up_y = []
        for g in range(count):
            e_y = jnp.where(ahead_y(regions, g) == regions[g], strong, weak)
            y = fold * (y_first + g) + lane_of // depth
            up_y.append(jnp.where((y >= 0) & (y < rows - 1), e_y, 0.0))
        result = []
        for g in range(count):
            mine = regions[g]
            up_x = jnp.where(pltpu.roll(mine, high - 1, 0) == mine, strong, weak)
            up_x = jnp.where(x_inside, up_x, 0.0)
            up_z = jnp.where(pltpu.roll(mine, lanes - 1, 1) == mine, strong, weak)
            up_z = jnp.where(lane_of % depth == depth - 1, 0.0, up_z)
            down_x = pltpu.roll(up_x, 1, 0)
            down_z = pltpu.roll(up_z, 1, 1)
            down_y = behind_y(up_y, g)
            middle = 1.0 - (((up_x + down_x) + (up_z + down_z)) + (up_y[g] + down_y))
            result.append((middle, up_x, down_x, up_y[g], down_y, up_z, down_z))
        return result

    def swept(fields, factors, g):
        f = fields[g]
        high = f.shape[0]
        middle, up_x, down_x, up_y, down_y, up_z, down_z = factors
        return (
            (middle * f + up_x * pltpu.roll(f, high - 1, 0))
            + (down_x * pltpu.roll(f, 1, 0) + up_z * pltpu.roll(f, lanes - 1, 1))
        ) + (
            down_z * pltpu.roll(f, 1, 1)
            + (up_y * ahead_y(fields, g) + down_y * behind_y(fields, g))
        )

    def transposed(p):
        result = []
        for start in range(0, p.shape[0] // cells, fold):
            chunk = p[cells * start : cells * (start + fold)]
            found = chunk.shape[0] // cells
            flipped = jnp.concatenate([chunk] + [chunk[:cells]] * (fold - found), axis=0).T
            for g in range(found):
                piece = flipped[0:depth]
                if g:
                    piece = pltpu.roll(piece, (lanes - depth * g) % lanes, 1)
                for b in range(1, fold):
                    part_b = flipped[depth * b : depth * (b + 1)]
                    amount = (depth * (b - g)) % lanes
                    if amount:
                        part_b = pltpu.roll(part_b, amount, 1)
                    piece = jnp.where(lane // depth == b, part_b, piece)
                result.append(piece)
        return result

    @pl.when(works)
    def _():
        whole(held, data_sem)
        mat_copy.wait_recv()
        blurs = [
            halves(jnp.where(same_block, jnp.concatenate([mats[s]] * fold, axis=0), 0.0))
            for s in range(2)
        ]

        def paired_of(chosen, currents):
            corrections = []
            for s in range(2):
                recorded = jnp.concatenate([held[s, g] for g in chosen], axis=0)
                current = recorded if currents is None else jnp.concatenate(currents[s], axis=0)
                ratio = recorded / blurred(current, blurs[s], ((1,), (0,)))
                corrections.append(blurred(ratio, blurs[s], ((1,), (1,))))
            return jnp.sqrt(corrections[0] * corrections[1])

        def swapped_over(step, begin, size):
            copy = pltpu.make_async_remote_copy(
                src_ref=outgoing.at[step, pl.ds(begin, size)],
                dst_ref=incoming.at[step, pl.ds(begin, size)],
                send_sem=send,
                recv_sem=swap_sem.at[step],
                device_id=across,
                device_id_type=mesh_id,
            )
            copy.start()
            return copy

        paired = paired_of(range(width), None)
        for g, piece in enumerate(transposed(paired)):
            outgoing[0, g] = piece
        swap = swapped_over(0, 0, width)
        pl.semaphore_wait(late_sem, 2 * ends)
        start_sides()
        whole(held_labels, label_sem)
        for s in range(2):
            found = weights([held_labels[s, g] for g in range(width)], sub < cells - 1, first)
            for g in range(width):
                for i in range(len(found[g])):
                    coef[i, s, g] = found[g][i]
        swap.wait_recv()
        joined = [
            jnp.sqrt(paired[cells * g : cells * (g + 1)] * incoming[0, g]) for g in range(width)
        ]
        fields = [[held[s, g] * joined[g] for g in range(width)] for s in range(2)]
        inner = range(1, width - 1)
        for sweep in range(SWEEPS):
            kept = inner if sweep == SWEEPS - 1 else range(width)
            fresh = [list(fields[s]) for s in range(2)]
            for s in range(2):
                for g in kept:
                    factors = [coef[i, s, g] for i in range(coef.shape[0])]
                    fresh[s][g] = swept(fields[s], factors, g)
            fields = fresh

        currents = [[fields[s][g] for g in inner] for s in range(2)]
        paired = paired_of(inner, currents)
        for s in range(2):
            for k in range(len(inner)):
                est[s, k] = currents[s][k]
        for k, piece in enumerate(transposed(paired)):
            outgoing[1, k] = piece
        swap = swapped_over(1, 0, len(inner))
        swap.wait_recv()
        for k in range(len(inner)):
            joined = jnp.sqrt(paired[cells * k : cells * (k + 1)] * incoming[1, k])
            for s in range(2):
                leave[s, k, pad : pad + cells] = est[s, k] * joined

        def window(h, t):
            flipped = core == 1 - h
            return pl.ds(pl.multiple_of(jnp.where(flipped, tiles - 1 - t, t) * slab, 8), span)

        def returned(h, t):
            return pltpu.make_async_remote_copy(
                src_ref=leave.at[h, :, window(h, t), :],
                dst_ref=back.at[own],
                send_sem=send,
                recv_sem=back_sem,
                device_id=at_device(h, t),
                device_id_type=mesh_id,
            )

        own = pl.ds(keep * block, keep)
        for t in [0, tiles - 1] + list(range(1, tiles - 1)):
            returned(1 - half, t).start()

            @pl.when(tile == t)
            def _():
                pltpu.make_async_copy(
                    leave.at[half, :, window(half, t), :], back.at[own], back_sem
                ).start()

            @pl.when(tile != t)
            def _():
                returned(half, t).start()

    pl.when(idle)(start_sides)

    @pl.when(has_below)
    def _():
        beside(0).wait_recv()

    @pl.when(has_above)
    def _():
        beside(1).wait_recv()

    x_at = place * slab - pad + sub[:span]
    x_inside = (x_at >= 0) & (x_at < cells - 1) & (sub[:span] < span - 1)
    found = weights([around[g, slab - pad : 2 * slab + pad] for g in range(groups)], x_inside, 0)
    for g in range(groups):
        for i in range(len(found[g])):
            slab_coef[i, g] = found[g][i]

    @pl.when(has_above)
    def _():
        beside(0).wait_send()

    @pl.when(has_below)
    def _():
        beside(1).wait_send()

    share = width * slab
    swaps = (width + keep) * cells
    busy = 2 * (2 * workers - 1) * share + depth + swaps + (2 * tiles - 1) * keep * span

    @pl.when(works)
    def _():
        whole(sent.at[pl.ds(0, busy)], send)

    @pl.when(idle)
    def _():
        whole(sent.at[pl.ds(0, 4 * workers * share)], send)

    whole(back, back_sem)
    fields = [back[g] for g in range(groups)]
    for sweep in range(SWEEPS):
        fields = [
            swept(fields, [slab_coef[i, g] for i in range(slab_coef.shape[0])], g)
            for g in range(groups)
        ]
    for g in range(groups):
        settled[g] = fields[g][pad : pad + slab]
    for j in range(blocks):
        parts = []
        for k in range(fold):
            line = settled[:, fold * j + k, :]
            parts.append(
                jnp.concatenate(
                    [line, jnp.zeros((mixed.shape[1] // fold - groups, lanes), jnp.float32)], axis=0
                )
            )
        for b in range(fold):
            mixed[j, pl.ds(b, mixed.shape[1] // fold, stride=fold), :] = gathered(
                parts, [b] * fold, slot, depth
            )
        lined = permuted(mixed[j, 0:rows], turn).T
        for k in range(fold):
            x = fold * j + k
            at = jnp.where(flip_x, slab - 1 - x, x)
            unpacked[pl.ds(at, 1)] = lined[depth * k : depth * (k + 1)][None]


def by_rows(data, labels, kernel, offsets):
    tiles = lax.axis_size("tile")
    _, slab, rows, depth = data.shape
    fold = 128 // depth
    tall = -(-rows // (8 * fold)) * 8 * fold
    groups = rows // fold
    cells = slab * tiles
    kept = groups // (2 * (tiles - 2))
    width = kept + 2
    span = slab + 2 * SWEEPS
    flat = (slab * depth, rows)
    wide = (2, width, cells, 128)
    strips = (groups + 2, slab, 128)
    sent = 4 * tiles * width * slab + depth + (width + kept) * cells + 2 * tiles * kept * span
    dma = pltpu.SemaphoreType.DMA
    taps = kernel.transpose(2, 0, 1)
    ready = pl.pallas_call(
        functools.partial(fused, tiles),
        out_shape=pltpu.VMEM((slab, depth, rows), jnp.float32),
        in_specs=[pl.BlockSpec(memory_space=pltpu.HBM)] * 4,
        out_specs=pl.BlockSpec(memory_space=pltpu.VMEM),
        scratch_shapes=[
            pltpu.VMEM(flat, jnp.float32),
            pltpu.VMEM(flat, jnp.int32),
            pltpu.VMEM(taps.shape, jnp.float32),
            pltpu.VMEM(offsets.shape, jnp.int32),
            pltpu.VMEM((slab * depth // 128, tall, 128), jnp.float32),
            pltpu.VMEM(strips, jnp.float32),
            pltpu.VMEM(strips, jnp.float32),
            pltpu.VMEM(wide, jnp.float32),
            pltpu.VMEM(wide, jnp.float32),
            pltpu.VMEM((2, depth, 128), jnp.float32),
            pltpu.VMEM((2, kept, cells, 128), jnp.float32),
            pltpu.VMEM((7,) + wide, jnp.float32),
            pltpu.VMEM((ITERS,) + wide[1:], jnp.float32),
            pltpu.VMEM((ITERS,) + wide[1:], jnp.float32),
            pltpu.VMEM((2, kept, cells + span - slab, 128), jnp.float32),
            pltpu.VMEM((groups, span, 128), jnp.float32),
            pltpu.VMEM((groups, 3 * slab, 128), jnp.float32),
            pltpu.VMEM((7, groups, span, 128), jnp.float32),
            pltpu.VMEM((groups, slab, 128), jnp.float32),
            pltpu.VMEM((sent, 128), jnp.float32),
            dma((4,)),
            dma(()),
            dma(()),
            dma(()),
            dma((ITERS,)),
            dma(()),
            dma((2,)),
            dma(()),
            dma((2,)),
            pltpu.SemaphoreType.REGULAR,
        ],
        compiler_params=pltpu.CompilerParams(
            collective_id=0, has_side_effects=True
        ),
    )(data.transpose(0, 1, 3, 2), labels.transpose(0, 1, 3, 2), taps, offsets)
    return ready[None].transpose(0, 1, 3, 2)


def fits(data, tiles, views):
    _, slab, rows, depth = data.shape
    return (
        views == 4
        and depth * 4 == 128
        and slab * tiles == depth
        and slab == 8
        and tiles > 2
        and rows % (8 * (tiles - 2)) == 0
    )


def program(data, labels, kernel, offsets):
    if fits(data, lax.axis_size("tile"), lax.axis_size("view")):
        return by_rows(data, labels, kernel, offsets)
    return on_device(data, labels, kernel, offsets)


def solution(mesh):
    placed = (
        P(("parts", "view"), "tile", None, None),
        P(("parts", "view"), "tile", None, None),
        P("view", None, None),
        P("view", None),
    )
    return jax.shard_map(
        program,
        mesh=mesh,
        in_specs=placed,
        out_specs=P(("parts", "view"), "tile", None, None),
        check_vma=False,
    )
```

```python
import functools

import jax
import jax.numpy as jnp
from jax import lax
from jax.experimental import pallas as pl
from jax.experimental.pallas import tpu as pltpu
from jax.sharding import PartitionSpec as P

ITERS = 2
SWEEPS = 4


WEAK = 0.2
TAU = 0.15


def extended(cells, sides, width):
    for axis, dim in sides:
        count = lax.axis_size(axis)
        ends = count - 1
        head = lax.slice_in_dim(cells, 0, width, axis=dim)
        tail = lax.slice_in_dim(cells, cells.shape[dim] - width, cells.shape[dim], axis=dim)
        cells = jnp.concatenate(
            [
                lax.ppermute(tail, axis, [(i, (i + 1) % count) for i in range(ends)]),
                cells,
                lax.ppermute(head, axis, [((i + 1) % count, i) for i in range(ends)]),
            ],
            axis=dim,
        )
    return cells


def swapped(block, axis, stride):
    count = lax.axis_size(axis)
    route = []
    for low in range(count):
        high = low | 1 << stride
        if high != low and high < count:
            route += [(low, high), (high, low)]
    return lax.ppermute(block, axis, route)


def band(kernel, offsets):
    depth_cells = kernel.shape[0]
    taps = jnp.arange(kernel.shape[1], dtype=jnp.int32) - 4
    depth = jnp.arange(depth_cells, dtype=jnp.int32)
    index = jnp.clip(depth[:, None] + taps[None, :] + offsets[:, None], 0, depth_cells - 1)
    weight = kernel / jnp.sum(kernel, axis=1, keepdims=True)
    return (index, weight)


def axis_term(field, region, axis):
    count = field.shape[axis]
    upper = lax.slice_in_dim(field, 1, count, axis=axis)
    lower = lax.slice_in_dim(field, 0, count - 1, axis=axis)
    same = jnp.where(
        lax.slice_in_dim(region, 1, count, axis=axis)
        == lax.slice_in_dim(region, 0, count - 1, axis=axis),
        1.0,
        WEAK,
    )
    flux = same * (upper - lower)
    after = [(0, 0)] * 3
    before = [(0, 0)] * 3
    after[axis] = (0, 1)
    before[axis] = (1, 0)
    return jnp.pad(flux, after) - jnp.pad(flux, before)


def sweep_rows(field, region, first_row, total_rows):
    extent = field.shape[0]
    global_rows = first_row + jnp.arange(extent, dtype=jnp.int32)
    inside = ((global_rows >= 0) & (global_rows < total_rows)).astype(field.dtype)[:, None, None]
    same = jnp.where(region[1:] == region[:-1], 1.0, WEAK) * inside[1:] * inside[:-1]
    flux = same * (field[1:] - field[:-1])
    inner = field[1:-1]
    inner_labels = region[1:-1]
    total = (
        flux[1:] - flux[:-1] + axis_term(inner, inner_labels, 1) + axis_term(inner, inner_labels, 2)
    )
    return inner + TAU * total


def regroup(received, tiles):
    slab, rows, depth_cells = received.shape
    blocks = received.reshape(slab, rows, tiles, depth_cells // tiles)
    return blocks.transpose(3, 1, 2, 0).reshape(depth_cells // tiles, rows, depth_cells)


def on_device(data, labels, kernel, offsets):
    recorded = data[0]
    region = labels[0]
    index, weight = band(kernel[0], offsets[0])
    tiles = lax.axis_size("tile")
    slab, rows, depth_cells = recorded.shape
    total_rows = slab * tiles
    start = lax.axis_index("tile") * slab
    parity = lax.axis_index("view") % 2
    columns = jnp.arange(depth_cells, dtype=jnp.int32)
    matrix = jnp.sum(weight[:, :, None] * (index[:, :, None] == columns[None, None, :]), axis=1)
    label_ext = extended(region, (("tile", 0),), 4)
    current = recorded
    for step in range(ITERS):
        forward_flat = jnp.dot(
            current.reshape(-1, depth_cells), matrix.T, precision=lax.Precision.HIGHEST
        )
        field = recorded / forward_flat.reshape(current.shape)
        flat = jnp.dot(field.reshape(-1, depth_cells), matrix, precision=lax.Precision.HIGHEST)
        correction = flat.reshape(field.shape)
        turned = correction
        for repeat in range(2):
            turned = regroup(
                lax.all_to_all(
                    jnp.flip(turned, 2), "tile", split_axis=2, concat_axis=2, tiled=True
                ),
                tiles,
            )
        turned = swapped(turned, "view", 1)
        paired = jnp.sqrt(correction * turned)
        outgoing = jnp.where(parity == 0, jnp.flip(paired, 2), paired)
        rotated = regroup(
            lax.all_to_all(outgoing, "tile", split_axis=2, concat_axis=2, tiled=True), tiles
        )
        rotated = jnp.where(parity == 1, jnp.flip(rotated, 2), rotated)
        partner = swapped(rotated, "view", 0)
        current = current * jnp.sqrt(paired * partner)
        widened = extended(current, (("tile", 0),), 4)
        for sweep in range(SWEEPS):
            extent = widened.shape[0]
            widened = sweep_rows(
                widened, label_ext[sweep : sweep + extent], start - 4 + sweep, total_rows
            )
        current = widened
    return current[None]


def gathered(parts, b_of, slot, depth):
    fold = len(parts)
    lanes = parts[0].shape[1]
    total = None
    for k in range(fold):
        amount = (depth * (k - b_of[k])) % lanes
        piece = pltpu.roll(parts[k], amount, 1) if amount else parts[k]
        total = piece if total is None else jnp.where(slot == k, piece, total)
    return total


def turning(lanes, depth, flip_z):
    row_ids = lax.broadcasted_iota(jnp.int32, (lanes, lanes), 0)
    lane_ids = lax.broadcasted_iota(jnp.int32, (lanes, lanes), 1)
    same_block = (row_ids // depth) == (lane_ids // depth)
    aim = jnp.where(flip_z, depth - 1 - lane_ids % depth, lane_ids % depth)
    return same_block, jnp.where(same_block & (row_ids % depth == aim), 1.0, 0.0).astype(jnp.float32)


def exact(a, b):
    return jnp.dot(a, b, precision=lax.Precision.HIGHEST, preferred_element_type=jnp.float32)


def product(a, b, contract):
    return lax.dot_general(a, b, (contract, ((), ())), preferred_element_type=jnp.float32)


def halves(a):
    high = a.astype(jnp.bfloat16)
    return high, (a - high.astype(jnp.float32)).astype(jnp.bfloat16)


def permuted(a, turn):
    high, low = halves(a)
    turn = turn.astype(jnp.bfloat16)
    return product(high, turn, ((1,), (0,))) + product(low, turn, ((1,), (0,)))


def widened(matrix):
    high, low = halves(matrix)
    none = jnp.zeros_like(high)
    return jnp.concatenate(
        [jnp.concatenate([high, low], axis=1), jnp.concatenate([high, none], axis=1)], axis=0
    )


def blurred(a, wide):
    both = product(jnp.concatenate(halves(a), axis=1), wide, ((1,), (0,)))
    lanes = a.shape[1]
    return both[:, :lanes] + both[:, lanes:]


def fused(tiles, data_ref, labels_ref, taps_ref, shift_ref, unpacked, raw, raw_labels, taps_buf, shift_buf, mixed, packed, packed_labels, held, held_labels, mats, est, coef, outgoing, incoming, leave, back, around, slab_coef, settled, sent, in_sem, data_sem, label_sem, mat_sem, swap_sem, back_sem, side_sem, send, send_side, late_sem):
    mesh_id = pl.DeviceIdType.MESH
    slab, depth, rows = data_ref.shape[1:]
    lanes = packed.shape[2]
    fold = lanes // depth
    groups = rows // fold
    width = held.shape[1]
    keep = width - 2
    cells = held.shape[2]
    span = back.shape[1]
    pad = (span - slab) // 2
    view = lax.axis_index("view")
    tile = lax.axis_index("tile")
    part = lax.axis_index("parts")
    half = view // 2
    core = view % 2
    workers = tiles - 2
    ends = tiles - workers
    works = (tile > 0) & (tile <= workers)
    idle = (tile == 0) | (tile > workers)
    flip_x = (view == 1) | (view == 2)
    flip_z = view >= 2

    def at_device(h, t):
        return (part, 2 * h + core, t)

    across = (part, 2 * half + 1 - core, tile)

    barrier = pltpu.get_barrier_semaphore()

    @pl.when(works)
    def _():
        for d in range(1, tiles):
            for h in (1 - half, half):
                pl.semaphore_signal(
                    barrier,
                    inc=1,
                    device_id=at_device(h, (tile + d) % tiles),
                    device_id_type=mesh_id,
                )
        pl.semaphore_signal(
            barrier, inc=1, device_id=at_device(1 - half, tile), device_id_type=mesh_id
        )

    pl.semaphore_signal(barrier, inc=1, device_id=across, device_id_type=mesh_id)

    for source, target, sem in ((data_ref, raw, 0), (labels_ref, raw_labels, 1)):
        for x in range(slab):
            at = jnp.where(flip_x, slab - 1 - x, x)
            pltpu.make_async_copy(
                source.at[0, x],
                target.at[pl.ds(pl.multiple_of(at * depth, 8), depth)],
                in_sem.at[sem],
            ).start()
    small = [
        pltpu.make_async_copy(taps_ref, taps_buf, in_sem.at[2]),
        pltpu.make_async_copy(shift_ref, shift_buf, in_sem.at[3]),
    ]
    for copy in small:
        copy.start()

    def whole(ref, sem):
        pltpu.make_async_copy(ref, ref, sem).wait()

    same_block, turn = turning(lanes, depth, flip_z)
    slot = lax.broadcasted_iota(jnp.int32, (mixed.shape[1] // fold, lanes), 1) // depth
    blocks = slab * depth // lanes

    def pack(source, target, fill, turner):
        edge = jnp.full((1, slab, lanes), fill, jnp.float32)
        target[0:1] = edge
        target[groups + 1 : groups + 2] = edge
        for j in range(blocks):
            mixed[j, 0:rows] = turner(source[lanes * j : lanes * (j + 1), :])
        for j in range(blocks):
            parts = [
                mixed[j, pl.ds(b, mixed.shape[1] // fold, stride=fold), :] for b in range(fold)
            ]
            for k in range(fold):
                line = gathered(parts, [k] * fold, slot, depth)
                target[1 : groups + 1, fold * j + k, :] = line[:groups]

    def turned_labels(block):
        block = block.astype(jnp.float32).T.astype(jnp.bfloat16)
        return product(block, turn.astype(jnp.bfloat16), ((1,), (0,)))

    place = jnp.where(flip_x, tiles - 1 - tile, tile)
    spot = pl.ds(pl.multiple_of(place * slab, 8), slab)

    def scatter(source, target, sem):
        def piece(h, t):
            return source.at[pl.ds(keep * (2 * (t - 1) + h), width)]

        dst = target.at[half, :, spot, :]

        def over(h, t):
            pltpu.make_async_remote_copy(
                src_ref=piece(h, t),
                dst_ref=dst,
                send_sem=send,
                recv_sem=sem,
                device_id=at_device(h, t),
                device_id_type=mesh_id,
            ).start()

        @pl.when(idle)
        def _():
            for d in range(workers):
                t = jnp.where(tile == 0, workers - d, 1 + d)
                over(1 - half, t)
                over(half, t)

        @pl.when(works)
        def _():
            for d in range(1, workers):
                t = 1 + (tile - 1 + d) % workers
                over(1 - half, t)
                over(half, t)
            over(1 - half, tile)
            pltpu.make_async_copy(piece(half, tile), dst, sem).start()

    whole(raw, in_sem.at[0])
    pack(raw, packed, 1.0, lambda v: permuted(v.T, turn))
    pl.semaphore_wait(barrier, jnp.where(works, 2 * workers, 2 * workers + 1))

    @pl.when(idle)
    def _():
        for t in range(1, workers + 1):
            for h in (1 - half, half):
                pl.semaphore_signal(
                    late_sem, inc=1, device_id=at_device(h, t), device_id_type=mesh_id
                )

    scatter(packed, held, data_sem)

    for copy in small:
        copy.wait()
    count = taps_buf.shape[0]
    taps = [jnp.concatenate([taps_buf[k]] * fold, axis=1) for k in range(count)]
    scale = taps[0]
    for k in range(1, count):
        scale = scale + taps[k]
    shift = jnp.concatenate([shift_buf[...]] * fold, axis=1)
    level = lax.broadcasted_iota(jnp.int32, (1, lanes), 1) % depth
    strip_row = lax.broadcasted_iota(jnp.int32, (depth, lanes), 0)
    strip_aim = jnp.where(flip_z, depth - 1 - strip_row, strip_row)
    strip = jnp.zeros((depth, lanes), jnp.float32)
    for k in range(count):
        index = jnp.clip(level + (k - 4) + shift, 0, depth - 1)
        strip = strip + jnp.where(index == strip_aim, taps[k] / scale, 0.0)
    strip = exact(strip, turn)
    mats[pl.ds(half, 1)] = strip[None]
    mat_copy = pltpu.make_async_remote_copy(
        src_ref=mats.at[half],
        dst_ref=mats.at[half],
        send_sem=send,
        recv_sem=mat_sem,
        device_id=at_device(1 - half, tile),
        device_id_type=mesh_id,
    )
    pl.when(works)(mat_copy.start)

    whole(raw_labels, in_sem.at[1])
    pack(raw_labels, packed_labels, 0.0, turned_labels)
    pl.when((core == 1) & idle)(lambda: pl.delay(2000))
    scatter(packed_labels, held_labels, label_sem)

    inner_labels = packed_labels.at[pl.ds(1, groups)]

    def beside(side):
        onto = place + 1 - 2 * side
        t = jnp.where(flip_x, tiles - 1 - onto, onto)
        return pltpu.make_async_remote_copy(
            src_ref=inner_labels,
            dst_ref=around.at[:, pl.ds(2 * slab * side, slab), :],
            send_sem=send_side.at[side],
            recv_sem=side_sem.at[side],
            device_id=(part, view, jnp.clip(t, 0, tiles - 1)),
            device_id_type=mesh_id,
        )

    has_above = place < tiles - 1
    has_below = place > 0

    def start_sides():
        @pl.when(has_above)
        def _():
            beside(0).start()

        @pl.when(has_below)
        def _():
            beside(1).start()

    @pl.when(jnp.logical_not(has_below))
    def _():
        around[:, 0:slab, :] = jnp.zeros((groups, slab, lanes), jnp.float32)

    @pl.when(jnp.logical_not(has_above))
    def _():
        around[:, 2 * slab : 3 * slab, :] = jnp.zeros((groups, slab, lanes), jnp.float32)

    around[:, slab : 2 * slab, :] = packed_labels[1 : groups + 1]
    for s in range(2):
        for k in range(leave.shape[1]):
            leave[s, k, 0:pad] = jnp.zeros((pad, lanes), jnp.float32)
            leave[s, k, pad + cells : 2 * pad + cells] = jnp.zeros((pad, lanes), jnp.float32)

    lane = lax.broadcasted_iota(jnp.int32, (cells, lanes), 1)
    sub = lax.broadcasted_iota(jnp.int32, (cells, lanes), 0)
    block = 2 * (tile - 1) + half
    first = keep * block - 1

    def lanes_of(field):
        return lane[: field.shape[0]]

    def ahead_y(fields, g):
        after = fields[(g + 1) % len(fields)]
        return jnp.where(
            lanes_of(fields[g]) < lanes - depth,
            pltpu.roll(fields[g], lanes - depth, 1),
            pltpu.roll(after, lanes - depth, 1),
        )

    def behind_y(fields, g):
        return jnp.where(
            lanes_of(fields[g]) < depth,
            pltpu.roll(fields[g - 1], depth, 1),
            pltpu.roll(fields[g], depth, 1),
        )

    def weights(regions, x_inside, y_first):
        strong, weak = TAU, TAU * WEAK
        high = regions[0].shape[0]
        count = len(regions)
        lane_of = lanes_of(regions[0])
        up_y = []
        for g in range(count):
            e_y = jnp.where(ahead_y(regions, g) == regions[g], strong, weak)
            y = fold * (y_first + g) + lane_of // depth
            up_y.append(jnp.where((y >= 0) & (y < rows - 1), e_y, 0.0))
        result = []
        for g in range(count):
            mine = regions[g]
            up_x = jnp.where(pltpu.roll(mine, high - 1, 0) == mine, strong, weak)
            up_x = jnp.where(x_inside, up_x, 0.0)
            up_z = jnp.where(pltpu.roll(mine, lanes - 1, 1) == mine, strong, weak)
            up_z = jnp.where(lane_of % depth == depth - 1, 0.0, up_z)
            down_x = pltpu.roll(up_x, 1, 0)
            down_z = pltpu.roll(up_z, 1, 1)
            down_y = behind_y(up_y, g)
            middle = 1.0 - (((up_x + down_x) + (up_z + down_z)) + (up_y[g] + down_y))
            result.append((middle, up_x, down_x, up_y[g], down_y, up_z, down_z))
        return result

    def swept(fields, factors, g):
        f = fields[g]
        high = f.shape[0]
        middle, up_x, down_x, up_y, down_y, up_z, down_z = factors
        return (
            (middle * f + up_x * pltpu.roll(f, high - 1, 0))
            + (down_x * pltpu.roll(f, 1, 0) + up_z * pltpu.roll(f, lanes - 1, 1))
        ) + (
            down_z * pltpu.roll(f, 1, 1)
            + (up_y * ahead_y(fields, g) + down_y * behind_y(fields, g))
        )

    def transposed(p):
        result = []
        for start in range(0, p.shape[0] // cells, fold):
            chunk = p[cells * start : cells * (start + fold)]
            found = chunk.shape[0] // cells
            flipped = jnp.concatenate([chunk] + [chunk[:cells]] * (fold - found), axis=0).T
            for g in range(found):
                piece = flipped[0:depth]
                if g:
                    piece = pltpu.roll(piece, (lanes - depth * g) % lanes, 1)
                for b in range(1, fold):
                    part_b = flipped[depth * b : depth * (b + 1)]
                    amount = (depth * (b - g)) % lanes
                    if amount:
                        part_b = pltpu.roll(part_b, amount, 1)
                    piece = jnp.where(lane // depth == b, part_b, piece)
                result.append(piece)
        return result

    @pl.when(works)
    def _():
        mat_copy.wait_recv()
        blurs = []
        for s in range(2):
            matrix = jnp.where(same_block, jnp.concatenate([mats[s]] * fold, axis=0), 0.0)
            blurs.append((widened(matrix), widened(matrix.T)))
        whole(held, data_sem)

        def paired_of(chosen, currents):
            corrections = []
            for s in range(2):
                recorded = jnp.concatenate([held[s, g] for g in chosen], axis=0)
                current = recorded if currents is None else jnp.concatenate(currents[s], axis=0)
                ratio = recorded / blurred(current, blurs[s][0])
                corrections.append(blurred(ratio, blurs[s][1]))
            return jnp.sqrt(corrections[0] * corrections[1])

        def swapped_over(step, begin, size):
            copy = pltpu.make_async_remote_copy(
                src_ref=outgoing.at[step, pl.ds(begin, size)],
                dst_ref=incoming.at[step, pl.ds(begin, size)],
                send_sem=send,
                recv_sem=swap_sem.at[step],
                device_id=across,
                device_id_type=mesh_id,
            )
            copy.start()
            return copy

        paired = paired_of(range(width), None)
        for g, piece in enumerate(transposed(paired)):
            outgoing[0, g] = piece
        swap = swapped_over(0, 0, width)
        pl.semaphore_wait(late_sem, 2 * ends)
        start_sides()
        whole(held_labels, label_sem)
        for s in range(2):
            found = weights([held_labels[s, g] for g in range(width)], sub < cells - 1, first)
            for g in range(width):
                for i in range(len(found[g])):
                    coef[i, s, g] = found[g][i]
        swap.wait_recv()
        joined = [
            jnp.sqrt(paired[cells * g : cells * (g + 1)] * incoming[0, g]) for g in range(width)
        ]
        fields = [[held[s, g] * joined[g] for g in range(width)] for s in range(2)]
        inner = range(1, width - 1)
        for sweep in range(SWEEPS):
            kept = inner if sweep == SWEEPS - 1 else range(width)
            fresh = [list(fields[s]) for s in range(2)]
            for s in range(2):
                for g in kept:
                    factors = [coef[i, s, g] for i in range(coef.shape[0])]
                    fresh[s][g] = swept(fields[s], factors, g)
            fields = fresh

        currents = [[fields[s][g] for g in inner] for s in range(2)]
        paired = paired_of(inner, currents)
        for s in range(2):
            for k in range(len(inner)):
                est[s, k] = currents[s][k]
        for k, piece in enumerate(transposed(paired)):
            outgoing[1, k] = piece
        swap = swapped_over(1, 0, len(inner))
        swap.wait_recv()
        for k in range(len(inner)):
            joined = jnp.sqrt(paired[cells * k : cells * (k + 1)] * incoming[1, k])
            for s in range(2):
                leave[s, k, pad : pad + cells] = est[s, k] * joined

        def window(h, t):
            flipped = core == 1 - h
            return pl.ds(pl.multiple_of(jnp.where(flipped, tiles - 1 - t, t) * slab, 8), span)

        def returned(h, t):
            return pltpu.make_async_remote_copy(
                src_ref=leave.at[h, :, window(h, t), :],
                dst_ref=back.at[own],
                send_sem=send,
                recv_sem=back_sem,
                device_id=at_device(h, t),
                device_id_type=mesh_id,
            )

        own = pl.ds(keep * block, keep)
        for t in (0, tiles - 1):
            returned(0, t).start()
            returned(1, t).start()
        for t in range(1, tiles - 1):
            returned(1 - half, t).start()

            @pl.when(tile == t)
            def _():
                pltpu.make_async_copy(
                    leave.at[half, :, window(half, t), :], back.at[own], back_sem
                ).start()

            @pl.when(tile != t)
            def _():
                returned(half, t).start()

    pl.when(idle)(start_sides)

    @pl.when(has_below)
    def _():
        beside(0).wait_recv()

    @pl.when(has_above)
    def _():
        beside(1).wait_recv()

    x_at = place * slab - pad + sub[:span]
    x_inside = (x_at >= 0) & (x_at < cells - 1) & (sub[:span] < span - 1)
    found = weights([around[g, slab - pad : 2 * slab + pad] for g in range(groups)], x_inside, 0)
    for g in range(groups):
        for i in range(len(found[g])):
            slab_coef[i, g] = found[g][i]

    @pl.when(has_above)
    def _():
        beside(0).wait_send()

    @pl.when(has_below)
    def _():
        beside(1).wait_send()

    share = width * slab
    swaps = (width + keep) * cells
    busy = 2 * (2 * workers - 1) * share + depth + swaps + (2 * tiles - 1) * keep * span

    @pl.when(works)
    def _():
        whole(sent.at[pl.ds(0, busy)], send)

    @pl.when(idle)
    def _():
        whole(sent.at[pl.ds(0, 4 * workers * share)], send)

    whole(back, back_sem)
    fields = [back[g] for g in range(groups)]
    for sweep in range(SWEEPS):
        fields = [
            swept(fields, [slab_coef[i, g] for i in range(slab_coef.shape[0])], g)
            for g in range(groups)
        ]
    for g in range(groups):
        settled[g] = fields[g][pad : pad + slab]
    for j in range(blocks):
        parts = []
        for k in range(fold):
            line = settled[:, fold * j + k, :]
            parts.append(
                jnp.concatenate(
                    [line, jnp.zeros((mixed.shape[1] // fold - groups, lanes), jnp.float32)], axis=0
                )
            )
        for b in range(fold):
            mixed[j, pl.ds(b, mixed.shape[1] // fold, stride=fold), :] = gathered(
                parts, [b] * fold, slot, depth
            )
        lined = permuted(mixed[j, 0:rows], turn).T
        for k in range(fold):
            x = fold * j + k
            at = jnp.where(flip_x, slab - 1 - x, x)
            unpacked[pl.ds(at, 1)] = lined[depth * k : depth * (k + 1)][None]


def by_rows(data, labels, kernel, offsets):
    tiles = lax.axis_size("tile")
    _, slab, rows, depth = data.shape
    fold = 128 // depth
    tall = -(-rows // (8 * fold)) * 8 * fold
    groups = rows // fold
    cells = slab * tiles
    kept = groups // (2 * (tiles - 2))
    width = kept + 2
    span = slab + 2 * SWEEPS
    flat = (slab * depth, rows)
    wide = (2, width, cells, 128)
    strips = (groups + 2, slab, 128)
    sent = 4 * tiles * width * slab + depth + (width + kept) * cells + 2 * tiles * kept * span
    dma = pltpu.SemaphoreType.DMA
    taps = kernel.transpose(2, 0, 1)
    ready = pl.pallas_call(
        functools.partial(fused, tiles),
        out_shape=pltpu.VMEM((slab, depth, rows), jnp.float32),
        in_specs=[pl.BlockSpec(memory_space=pltpu.HBM)] * 4,
        out_specs=pl.BlockSpec(memory_space=pltpu.VMEM),
        scratch_shapes=[
            pltpu.VMEM(flat, jnp.float32),
            pltpu.VMEM(flat, jnp.int32),
            pltpu.VMEM(taps.shape, jnp.float32),
            pltpu.VMEM(offsets.shape, jnp.int32),
            pltpu.VMEM((slab * depth // 128, tall, 128), jnp.float32),
            pltpu.VMEM(strips, jnp.float32),
            pltpu.VMEM(strips, jnp.float32),
            pltpu.VMEM(wide, jnp.float32),
            pltpu.VMEM(wide, jnp.float32),
            pltpu.VMEM((2, depth, 128), jnp.float32),
            pltpu.VMEM((2, kept, cells, 128), jnp.float32),
            pltpu.VMEM((7,) + wide, jnp.float32),
            pltpu.VMEM((ITERS,) + wide[1:], jnp.float32),
            pltpu.VMEM((ITERS,) + wide[1:], jnp.float32),
            pltpu.VMEM((2, kept, cells + span - slab, 128), jnp.float32),
            pltpu.VMEM((groups, span, 128), jnp.float32),
            pltpu.VMEM((groups, 3 * slab, 128), jnp.float32),
            pltpu.VMEM((7, groups, span, 128), jnp.float32),
            pltpu.VMEM((groups, slab, 128), jnp.float32),
            pltpu.VMEM((sent, 128), jnp.float32),
            dma((4,)),
            dma(()),
            dma(()),
            dma(()),
            dma((ITERS,)),
            dma(()),
            dma((2,)),
            dma(()),
            dma((2,)),
            pltpu.SemaphoreType.REGULAR,
        ],
        compiler_params=pltpu.CompilerParams(
            collective_id=0, has_side_effects=True
        ),
    )(data.transpose(0, 1, 3, 2), labels.transpose(0, 1, 3, 2), taps, offsets)
    return ready[None].transpose(0, 1, 3, 2)


def fits(data, tiles, views):
    _, slab, rows, depth = data.shape
    return (
        views == 4
        and depth * 4 == 128
        and slab * tiles == depth
        and slab == 8
        and tiles > 2
        and rows % (8 * (tiles - 2)) == 0
    )


def program(data, labels, kernel, offsets):
    if fits(data, lax.axis_size("tile"), lax.axis_size("view")):
        return by_rows(data, labels, kernel, offsets)
    return on_device(data, labels, kernel, offsets)


def solution(mesh):
    placed = (
        P(("parts", "view"), "tile", None, None),
        P(("parts", "view"), "tile", None, None),
        P("view", None, None),
        P("view", None),
    )
    return jax.shard_map(
        program,
        mesh=mesh,
        in_specs=placed,
        out_specs=P(("parts", "view"), "tile", None, None),
        check_vma=False,
    )
```

```python
import functools

import jax
import jax.numpy as jnp
from jax import lax
from jax.experimental import pallas as pl
from jax.experimental.pallas import tpu as pltpu
from jax.sharding import PartitionSpec as P

ITERS = 2
SWEEPS = 4


WEAK = 0.2
TAU = 0.15


def extended(cells, sides, width):
    for axis, dim in sides:
        count = lax.axis_size(axis)
        ends = count - 1
        head = lax.slice_in_dim(cells, 0, width, axis=dim)
        tail = lax.slice_in_dim(cells, cells.shape[dim] - width, cells.shape[dim], axis=dim)
        cells = jnp.concatenate(
            [
                lax.ppermute(tail, axis, [(i, (i + 1) % count) for i in range(ends)]),
                cells,
                lax.ppermute(head, axis, [((i + 1) % count, i) for i in range(ends)]),
            ],
            axis=dim,
        )
    return cells


def swapped(block, axis, stride):
    count = lax.axis_size(axis)
    route = []
    for low in range(count):
        high = low | 1 << stride
        if high != low and high < count:
            route += [(low, high), (high, low)]
    return lax.ppermute(block, axis, route)


def band(kernel, offsets):
    depth_cells = kernel.shape[0]
    taps = jnp.arange(kernel.shape[1], dtype=jnp.int32) - 4
    depth = jnp.arange(depth_cells, dtype=jnp.int32)
    index = jnp.clip(depth[:, None] + taps[None, :] + offsets[:, None], 0, depth_cells - 1)
    weight = kernel / jnp.sum(kernel, axis=1, keepdims=True)
    return (index, weight)


def axis_term(field, region, axis):
    count = field.shape[axis]
    upper = lax.slice_in_dim(field, 1, count, axis=axis)
    lower = lax.slice_in_dim(field, 0, count - 1, axis=axis)
    same = jnp.where(
        lax.slice_in_dim(region, 1, count, axis=axis)
        == lax.slice_in_dim(region, 0, count - 1, axis=axis),
        1.0,
        WEAK,
    )
    flux = same * (upper - lower)
    after = [(0, 0)] * 3
    before = [(0, 0)] * 3
    after[axis] = (0, 1)
    before[axis] = (1, 0)
    return jnp.pad(flux, after) - jnp.pad(flux, before)


def sweep_rows(field, region, first_row, total_rows):
    extent = field.shape[0]
    global_rows = first_row + jnp.arange(extent, dtype=jnp.int32)
    inside = ((global_rows >= 0) & (global_rows < total_rows)).astype(field.dtype)[:, None, None]
    same = jnp.where(region[1:] == region[:-1], 1.0, WEAK) * inside[1:] * inside[:-1]
    flux = same * (field[1:] - field[:-1])
    inner = field[1:-1]
    inner_labels = region[1:-1]
    total = (
        flux[1:] - flux[:-1] + axis_term(inner, inner_labels, 1) + axis_term(inner, inner_labels, 2)
    )
    return inner + TAU * total


def regroup(received, tiles):
    slab, rows, depth_cells = received.shape
    blocks = received.reshape(slab, rows, tiles, depth_cells // tiles)
    return blocks.transpose(3, 1, 2, 0).reshape(depth_cells // tiles, rows, depth_cells)


def on_device(data, labels, kernel, offsets):
    recorded = data[0]
    region = labels[0]
    index, weight = band(kernel[0], offsets[0])
    tiles = lax.axis_size("tile")
    slab, rows, depth_cells = recorded.shape
    total_rows = slab * tiles
    start = lax.axis_index("tile") * slab
    parity = lax.axis_index("view") % 2
    columns = jnp.arange(depth_cells, dtype=jnp.int32)
    matrix = jnp.sum(weight[:, :, None] * (index[:, :, None] == columns[None, None, :]), axis=1)
    label_ext = extended(region, (("tile", 0),), 4)
    current = recorded
    for step in range(ITERS):
        forward_flat = jnp.dot(
            current.reshape(-1, depth_cells), matrix.T, precision=lax.Precision.HIGHEST
        )
        field = recorded / forward_flat.reshape(current.shape)
        flat = jnp.dot(field.reshape(-1, depth_cells), matrix, precision=lax.Precision.HIGHEST)
        correction = flat.reshape(field.shape)
        turned = correction
        for repeat in range(2):
            turned = regroup(
                lax.all_to_all(
                    jnp.flip(turned, 2), "tile", split_axis=2, concat_axis=2, tiled=True
                ),
                tiles,
            )
        turned = swapped(turned, "view", 1)
        paired = jnp.sqrt(correction * turned)
        outgoing = jnp.where(parity == 0, jnp.flip(paired, 2), paired)
        rotated = regroup(
            lax.all_to_all(outgoing, "tile", split_axis=2, concat_axis=2, tiled=True), tiles
        )
        rotated = jnp.where(parity == 1, jnp.flip(rotated, 2), rotated)
        partner = swapped(rotated, "view", 0)
        current = current * jnp.sqrt(paired * partner)
        widened = extended(current, (("tile", 0),), 4)
        for sweep in range(SWEEPS):
            extent = widened.shape[0]
            widened = sweep_rows(
                widened, label_ext[sweep : sweep + extent], start - 4 + sweep, total_rows
            )
        current = widened
    return current[None]


def gathered(parts, b_of, slot, depth):
    fold = len(parts)
    lanes = parts[0].shape[1]
    total = None
    for k in range(fold):
        amount = (depth * (k - b_of[k])) % lanes
        piece = pltpu.roll(parts[k], amount, 1) if amount else parts[k]
        total = piece if total is None else jnp.where(slot == k, piece, total)
    return total


def turning(lanes, depth, flip_z):
    row_ids = lax.broadcasted_iota(jnp.int32, (lanes, lanes), 0)
    lane_ids = lax.broadcasted_iota(jnp.int32, (lanes, lanes), 1)
    same_block = (row_ids // depth) == (lane_ids // depth)
    aim = jnp.where(flip_z, depth - 1 - lane_ids % depth, lane_ids % depth)
    return same_block, jnp.where(same_block & (row_ids % depth == aim), 1.0, 0.0).astype(jnp.float32)


def exact(a, b):
    return jnp.dot(a, b, precision=lax.Precision.HIGHEST, preferred_element_type=jnp.float32)


def product(a, b, contract):
    return lax.dot_general(a, b, (contract, ((), ())), preferred_element_type=jnp.float32)


def halves(a):
    high = a.astype(jnp.bfloat16)
    return high, (a - high.astype(jnp.float32)).astype(jnp.bfloat16)


def permuted(a, turn):
    high, low = halves(a)
    turn = turn.astype(jnp.bfloat16)
    return product(high, turn, ((1,), (0,))) + product(low, turn, ((1,), (0,)))


def widened(matrix):
    high, low = halves(matrix)
    none = jnp.zeros_like(high)
    return jnp.concatenate(
        [jnp.concatenate([high, low], axis=1), jnp.concatenate([high, none], axis=1)], axis=0
    )


def blurred(a, wide):
    both = product(jnp.concatenate(halves(a), axis=1), wide, ((1,), (0,)))
    lanes = a.shape[1]
    return both[:, :lanes] + both[:, lanes:]


def fused(tiles, data_ref, labels_ref, taps_ref, shift_ref, unpacked, raw, raw_labels, taps_buf, shift_buf, mixed, packed, packed_labels, held, held_labels, mats, est, coef, outgoing, incoming, leave, back, around, slab_coef, settled, sent, in_sem, data_sem, label_sem, mat_sem, swap_sem, back_sem, side_sem, send, send_side, late_sem):
    mesh_id = pl.DeviceIdType.MESH
    slab, depth, rows = data_ref.shape[1:]
    lanes = packed.shape[2]
    fold = lanes // depth
    groups = rows // fold
    width = held.shape[1]
    keep = width - 2
    cells = held.shape[2]
    span = back.shape[1]
    pad = (span - slab) // 2
    view = lax.axis_index("view")
    tile = lax.axis_index("tile")
    part = lax.axis_index("parts")
    half = view // 2
    core = view % 2
    workers = tiles - 2
    ends = tiles - workers
    works = (tile > 0) & (tile <= workers)
    idle = (tile == 0) | (tile > workers)
    flip_x = (view == 1) | (view == 2)
    flip_z = view >= 2

    def at_device(h, t):
        return (part, 2 * h + core, t)

    across = (part, 2 * half + 1 - core, tile)

    barrier = pltpu.get_barrier_semaphore()

    @pl.when(works)
    def _():
        for d in range(1, tiles):
            for h in (1 - half, half):
                pl.semaphore_signal(
                    barrier,
                    inc=1,
                    device_id=at_device(h, (tile + d) % tiles),
                    device_id_type=mesh_id,
                )
        pl.semaphore_signal(
            barrier, inc=1, device_id=at_device(1 - half, tile), device_id_type=mesh_id
        )

    pl.semaphore_signal(barrier, inc=1, device_id=across, device_id_type=mesh_id)

    small = [
        pltpu.make_async_copy(taps_ref, taps_buf, in_sem.at[2]),
        pltpu.make_async_copy(shift_ref, shift_buf, in_sem.at[3]),
    ]
    for copy in small:
        copy.start()

    for source, target, sem in ((data_ref, raw, 0), (labels_ref, raw_labels, 1)):
        for x in range(slab):
            at = jnp.where(flip_x, slab - 1 - x, x)
            pltpu.make_async_copy(
                source.at[0, x],
                target.at[pl.ds(pl.multiple_of(at * depth, 8), depth)],
                in_sem.at[sem],
            ).start()
    def whole(ref, sem):
        pltpu.make_async_copy(ref, ref, sem).wait()

    same_block, turn = turning(lanes, depth, flip_z)
    slot = lax.broadcasted_iota(jnp.int32, (mixed.shape[1] // fold, lanes), 1) // depth
    blocks = slab * depth // lanes

    def pack(source, target, fill, turner):
        edge = jnp.full((1, slab, lanes), fill, jnp.float32)
        target[0:1] = edge
        target[groups + 1 : groups + 2] = edge
        for j in range(blocks):
            mixed[j, 0:rows] = turner(source[lanes * j : lanes * (j + 1), :])
        for j in range(blocks):
            parts = [
                mixed[j, pl.ds(b, mixed.shape[1] // fold, stride=fold), :] for b in range(fold)
            ]
            for k in range(fold):
                line = gathered(parts, [k] * fold, slot, depth)
                target[1 : groups + 1, fold * j + k, :] = line[:groups]

    def turned_labels(block):
        block = block.astype(jnp.float32).T.astype(jnp.bfloat16)
        return product(block, turn.astype(jnp.bfloat16), ((1,), (0,)))

    place = jnp.where(flip_x, tiles - 1 - tile, tile)
    spot = pl.ds(pl.multiple_of(place * slab, 8), slab)

    last = 2 * workers - 1
    homes = [(h, t) for t in range(1, workers + 1) for h in range(2)]

    def scatter(source, target, sem):
        for a in range(2):
            for own in range(tiles):

                @pl.when((half == a) & (tile == own))
                def _():
                    for h, t in sorted(homes, key=lambda ht: (-abs(ht[1] - own), ht[0] == a)):
                        number = 2 * (t - 1) + h
                        low = 1 if number == 0 else 0
                        size = width - (number in (0, last))
                        src = source.at[pl.ds(keep * number + low, size)]
                        dst = target.at[a, pl.ds(low, size), spot, :]
                        if (h, t) == (a, own):
                            copy = pltpu.make_async_copy(src, dst, sem)
                        else:
                            copy = pltpu.make_async_remote_copy(
                                src_ref=src,
                                dst_ref=dst,
                                send_sem=send,
                                recv_sem=sem,
                                device_id=at_device(h, t),
                                device_id_type=mesh_id,
                            )
                        copy.start()

    for copy in small:
        copy.wait()
    @pl.when(works)
    def _():
        count = taps_buf.shape[0]
        taps = [jnp.concatenate([taps_buf[k]] * fold, axis=1) for k in range(count)]
        scale = taps[0]
        for k in range(1, count):
            scale = scale + taps[k]
        shift = jnp.concatenate([shift_buf[...]] * fold, axis=1)
        level = lax.broadcasted_iota(jnp.int32, (1, lanes), 1) % depth
        strip_row = lax.broadcasted_iota(jnp.int32, (depth, lanes), 0)
        strip_aim = jnp.where(flip_z, depth - 1 - strip_row, strip_row)
        strip = jnp.zeros((depth, lanes), jnp.float32)
        for k in range(count):
            index = jnp.clip(level + (k - 4) + shift, 0, depth - 1)
            strip = strip + jnp.where(index == strip_aim, taps[k] / scale, 0.0)
        strip = exact(strip, turn)
        mats[pl.ds(half, 1)] = strip[None]

    mat_copy = pltpu.make_async_remote_copy(
        src_ref=mats.at[half],
        dst_ref=mats.at[half],
        send_sem=send,
        recv_sem=mat_sem,
        device_id=at_device(1 - half, tile),
        device_id_type=mesh_id,
    )

    whole(raw, in_sem.at[0])
    pack(raw, packed, 1.0, lambda v: permuted(v.T, turn))
    pl.semaphore_wait(barrier, jnp.where(works, 2 * workers, 2 * workers + 1))

    @pl.when(idle)
    def _():
        for t in range(1, workers + 1):
            for h in (1 - half, half):
                pl.semaphore_signal(
                    late_sem, inc=1, device_id=at_device(h, t), device_id_type=mesh_id
                )

    pl.when(works)(mat_copy.start)
    scatter(packed, held, data_sem)

    whole(raw_labels, in_sem.at[1])
    pack(raw_labels, packed_labels, 0.0, turned_labels)
    pl.when((core == 1) & idle)(lambda: pl.delay(2000))
    scatter(packed_labels, held_labels, label_sem)

    inner_labels = packed_labels.at[pl.ds(1, groups)]

    def beside(side):
        onto = place + 1 - 2 * side
        t = jnp.where(flip_x, tiles - 1 - onto, onto)
        return pltpu.make_async_remote_copy(
            src_ref=inner_labels,
            dst_ref=around.at[:, pl.ds(2 * slab * side, slab), :],
            send_sem=send_side.at[side],
            recv_sem=side_sem.at[side],
            device_id=(part, view, jnp.clip(t, 0, tiles - 1)),
            device_id_type=mesh_id,
        )

    has_above = place < tiles - 1
    has_below = place > 0

    def start_sides():
        @pl.when(has_above)
        def _():
            beside(0).start()

        @pl.when(has_below)
        def _():
            beside(1).start()

    @pl.when(jnp.logical_not(has_below))
    def _():
        around[:, 0:slab, :] = jnp.zeros((groups, slab, lanes), jnp.float32)

    @pl.when(jnp.logical_not(has_above))
    def _():
        around[:, 2 * slab : 3 * slab, :] = jnp.zeros((groups, slab, lanes), jnp.float32)

    around[:, slab : 2 * slab, :] = packed_labels[1 : groups + 1]
    for s in range(2):
        for k in range(leave.shape[1]):
            leave[s, k, 0:pad] = jnp.zeros((pad, lanes), jnp.float32)
            leave[s, k, pad + cells : 2 * pad + cells] = jnp.zeros((pad, lanes), jnp.float32)

    lane = lax.broadcasted_iota(jnp.int32, (cells, lanes), 1)
    sub = lax.broadcasted_iota(jnp.int32, (cells, lanes), 0)
    block = 2 * (tile - 1) + half
    edge = (block == 0) | (block == last)

    def landed(ref, fill, sem):
        @pl.when(edge)
        def _():
            whole(ref.at[:, pl.ds(0, width - 1)], sem)

        @pl.when(jnp.logical_not(edge))
        def _():
            whole(ref, sem)

        for number, slot_at in ((0, 0), (last, width - 1)):

            @pl.when(block == number)
            def _():
                for s in range(2):
                    ref[s, slot_at] = jnp.full((cells, lanes), fill, jnp.float32)

    first = keep * block - 1

    def lanes_of(field):
        return lane[: field.shape[0]]

    def ahead_y(fields, g):
        after = fields[(g + 1) % len(fields)]
        return jnp.where(
            lanes_of(fields[g]) < lanes - depth,
            pltpu.roll(fields[g], lanes - depth, 1),
            pltpu.roll(after, lanes - depth, 1),
        )

    def behind_y(fields, g):
        return jnp.where(
            lanes_of(fields[g]) < depth,
            pltpu.roll(fields[g - 1], depth, 1),
            pltpu.roll(fields[g], depth, 1),
        )

    def steps(mask):
        return jnp.where(mask, TAU, 0.0), jnp.where(mask, TAU * WEAK, 0.0)

    def limits(high, count, x_inside, y_first):
        lane_of = lane[:high]
        along_y = []
        for g in range(count):
            y = fold * (y_first + g) + lane_of // depth
            along_y.append(steps((y >= 0) & (y < rows - 1)))
        return steps(x_inside), along_y, steps(lane_of % depth < depth - 1)

    def weights(regions, bounds):
        along_x, along_y, along_z = bounds
        high = regions[0].shape[0]
        count = len(regions)
        up_y = [jnp.where(ahead_y(regions, g) == regions[g], *along_y[g]) for g in range(count)]
        result = []
        for g in range(count):
            mine = regions[g]
            up_x = jnp.where(pltpu.roll(mine, high - 1, 0) == mine, *along_x)
            up_z = jnp.where(pltpu.roll(mine, lanes - 1, 1) == mine, *along_z)
            down_x = pltpu.roll(up_x, 1, 0)
            down_z = pltpu.roll(up_z, 1, 1)
            down_y = behind_y(up_y, g)
            middle = 1.0 - (((up_x + down_x) + (up_z + down_z)) + (up_y[g] + down_y))
            result.append((middle, up_x, down_x, up_y[g], down_y, up_z, down_z))
        return result

    def swept(fields, factors, g):
        f = fields[g]
        high = f.shape[0]
        middle, up_x, down_x, up_y, down_y, up_z, down_z = factors
        return (
            (middle * f + up_x * pltpu.roll(f, high - 1, 0))
            + (down_x * pltpu.roll(f, 1, 0) + up_z * pltpu.roll(f, lanes - 1, 1))
        ) + (
            down_z * pltpu.roll(f, 1, 1)
            + (up_y * ahead_y(fields, g) + down_y * behind_y(fields, g))
        )

    def transposed(p):
        result = []
        for start in range(0, p.shape[0] // cells, fold):
            chunk = p[cells * start : cells * (start + fold)]
            found = chunk.shape[0] // cells
            flipped = jnp.concatenate([chunk] + [chunk[:cells]] * (fold - found), axis=0).T
            for g in range(found):
                piece = flipped[0:depth]
                if g:
                    piece = pltpu.roll(piece, (lanes - depth * g) % lanes, 1)
                for b in range(1, fold):
                    part_b = flipped[depth * b : depth * (b + 1)]
                    amount = (depth * (b - g)) % lanes
                    if amount:
                        part_b = pltpu.roll(part_b, amount, 1)
                    piece = jnp.where(lane // depth == b, part_b, piece)
                result.append(piece)
        return result

    @pl.when(works)
    def _():
        mat_copy.wait_recv()
        bounds = limits(cells, width, sub < cells - 1, first)
        blurs = []
        for s in range(2):
            matrix = jnp.where(same_block, jnp.concatenate([mats[s]] * fold, axis=0), 0.0)
            blurs.append((widened(matrix), widened(matrix.T)))
        landed(held, 1.0, data_sem)

        def paired_of(chosen, currents):
            corrections = []
            for s in range(2):
                recorded = jnp.concatenate([held[s, g] for g in chosen], axis=0)
                current = recorded if currents is None else jnp.concatenate(currents[s], axis=0)
                ratio = recorded / blurred(current, blurs[s][0])
                corrections.append(blurred(ratio, blurs[s][1]))
            return jnp.sqrt(corrections[0] * corrections[1])

        def swapped_over(step, begin, size):
            copy = pltpu.make_async_remote_copy(
                src_ref=outgoing.at[step, pl.ds(begin, size)],
                dst_ref=incoming.at[step, pl.ds(begin, size)],
                send_sem=send,
                recv_sem=swap_sem.at[step],
                device_id=across,
                device_id_type=mesh_id,
            )
            copy.start()
            return copy

        paired = paired_of(range(width), None)
        for g, piece in enumerate(transposed(paired)):
            outgoing[0, g] = piece
        swap = swapped_over(0, 0, width)
        pl.semaphore_wait(late_sem, 2 * ends)
        start_sides()
        landed(held_labels, 0.0, label_sem)
        for s in range(2):
            found = weights([held_labels[s, g] for g in range(width)], bounds)
            for g in range(width):
                for i in range(len(found[g])):
                    coef[i, s, g] = found[g][i]
        swap.wait_recv()
        joined = [
            jnp.sqrt(paired[cells * g : cells * (g + 1)] * incoming[0, g]) for g in range(width)
        ]
        fields = [[held[s, g] * joined[g] for g in range(width)] for s in range(2)]
        inner = range(1, width - 1)
        for sweep in range(SWEEPS):
            kept = inner if sweep == SWEEPS - 1 else range(width)
            fresh = [list(fields[s]) for s in range(2)]
            for s in range(2):
                for g in kept:
                    factors = [coef[i, s, g] for i in range(coef.shape[0])]
                    fresh[s][g] = swept(fields[s], factors, g)
            fields = fresh

        currents = [[fields[s][g] for g in inner] for s in range(2)]
        paired = paired_of(inner, currents)
        for s in range(2):
            for k in range(len(inner)):
                est[s, k] = currents[s][k]
        for k, piece in enumerate(transposed(paired)):
            outgoing[1, k] = piece
        swap = swapped_over(1, 0, len(inner))
        swap.wait_recv()
        for k in range(len(inner)):
            joined = jnp.sqrt(paired[cells * k : cells * (k + 1)] * incoming[1, k])
            for s in range(2):
                leave[s, k, pad : pad + cells] = est[s, k] * joined

        def window(h, t):
            flipped = core == 1 - h
            return pl.ds(pl.multiple_of(jnp.where(flipped, tiles - 1 - t, t) * slab, 8), span)

        def returned(h, t):
            return pltpu.make_async_remote_copy(
                src_ref=leave.at[h, :, window(h, t), :],
                dst_ref=back.at[own],
                send_sem=send,
                recv_sem=back_sem,
                device_id=at_device(h, t),
                device_id_type=mesh_id,
            )

        own = pl.ds(keep * block, keep)
        returned(0, 0).start()
        returned(1, tiles - 1).start()
        returned(0, tiles - 1).start()
        returned(1, 0).start()
        for t in range(1, tiles - 1):
            returned(1 - half, t).start()

            @pl.when(tile == t)
            def _():
                pltpu.make_async_copy(
                    leave.at[half, :, window(half, t), :], back.at[own], back_sem
                ).start()

            @pl.when(tile != t)
            def _():
                returned(half, t).start()

    pl.when(idle)(start_sides)

    @pl.when(has_below)
    def _():
        beside(0).wait_recv()

    @pl.when(has_above)
    def _():
        beside(1).wait_recv()

    x_at = place * slab - pad + sub[:span]
    x_inside = (x_at >= 0) & (x_at < cells - 1) & (sub[:span] < span - 1)
    bounds = limits(span, groups, x_inside, 0)
    found = weights([around[g, slab - pad : 2 * slab + pad] for g in range(groups)], bounds)
    for g in range(groups):
        for i in range(len(found[g])):
            slab_coef[i, g] = found[g][i]

    @pl.when(has_above)
    def _():
        beside(0).wait_send()

    @pl.when(has_below)
    def _():
        beside(1).wait_send()

    swaps = (width + keep) * cells
    pieces = 2 * workers * width - 2

    def all_sent(kept_back, more):
        whole(sent.at[pl.ds(0, 2 * (pieces - kept_back) * slab + more)], send)

    after = depth + swaps + (2 * tiles - 1) * keep * span
    pl.when(works & edge)(lambda: all_sent(width - 1, after))
    pl.when(works & jnp.logical_not(edge))(lambda: all_sent(width, after))
    pl.when(idle)(lambda: all_sent(0, 0))
    turned_twice = turn.astype(jnp.bfloat16)
    whole(back, back_sem)
    fields = [back[g] for g in range(groups)]
    for sweep in range(SWEEPS):
        fields = [
            swept(fields, [slab_coef[i, g] for i in range(slab_coef.shape[0])], g)
            for g in range(groups)
        ]
    for g in range(groups):
        settled[g] = fields[g][pad : pad + slab]
    for j in range(blocks):
        parts = []
        for k in range(fold):
            line = settled[:, fold * j + k, :]
            parts.append(
                jnp.concatenate(
                    [line, jnp.zeros((mixed.shape[1] // fold - groups, lanes), jnp.float32)], axis=0
                )
            )
        for b in range(fold):
            mixed[j, pl.ds(b, mixed.shape[1] // fold, stride=fold), :] = gathered(
                parts, [b] * fold, slot, depth
            )
        lined = product(
            jnp.concatenate([turned_twice] * 2, axis=1),
            jnp.concatenate(halves(mixed[j, 0:rows]), axis=1),
            ((1,), (1,)),
        )
        for k in range(fold):
            x = fold * j + k
            at = jnp.where(flip_x, slab - 1 - x, x)
            unpacked[pl.ds(at, 1)] = lined[depth * k : depth * (k + 1)][None]


def by_rows(data, labels, kernel, offsets):
    tiles = lax.axis_size("tile")
    _, slab, rows, depth = data.shape
    fold = 128 // depth
    tall = -(-rows // (8 * fold)) * 8 * fold
    groups = rows // fold
    cells = slab * tiles
    kept = groups // (2 * (tiles - 2))
    width = kept + 2
    span = slab + 2 * SWEEPS
    flat = (slab * depth, rows)
    wide = (2, width, cells, 128)
    strips = (groups + 2, slab, 128)
    sent = 4 * tiles * width * slab + depth + (width + kept) * cells + 2 * tiles * kept * span
    dma = pltpu.SemaphoreType.DMA
    taps = kernel.transpose(2, 0, 1)
    ready = pl.pallas_call(
        functools.partial(fused, tiles),
        out_shape=pltpu.VMEM((slab, depth, rows), jnp.float32),
        in_specs=[pl.BlockSpec(memory_space=pltpu.HBM)] * 4,
        out_specs=pl.BlockSpec(memory_space=pltpu.VMEM),
        scratch_shapes=[
            pltpu.VMEM(flat, jnp.float32),
            pltpu.VMEM(flat, jnp.int32),
            pltpu.VMEM(taps.shape, jnp.float32),
            pltpu.VMEM(offsets.shape, jnp.int32),
            pltpu.VMEM((slab * depth // 128, tall, 128), jnp.float32),
            pltpu.VMEM(strips, jnp.float32),
            pltpu.VMEM(strips, jnp.float32),
            pltpu.VMEM(wide, jnp.float32),
            pltpu.VMEM(wide, jnp.float32),
            pltpu.VMEM((2, depth, 128), jnp.float32),
            pltpu.VMEM((2, kept, cells, 128), jnp.float32),
            pltpu.VMEM((7,) + wide, jnp.float32),
            pltpu.VMEM((ITERS,) + wide[1:], jnp.float32),
            pltpu.VMEM((ITERS,) + wide[1:], jnp.float32),
            pltpu.VMEM((2, kept, cells + span - slab, 128), jnp.float32),
            pltpu.VMEM((groups, span, 128), jnp.float32),
            pltpu.VMEM((groups, 3 * slab, 128), jnp.float32),
            pltpu.VMEM((7, groups, span, 128), jnp.float32),
            pltpu.VMEM((groups, slab, 128), jnp.float32),
            pltpu.VMEM((sent, 128), jnp.float32),
            dma((4,)),
            dma(()),
            dma(()),
            dma(()),
            dma((ITERS,)),
            dma(()),
            dma((2,)),
            dma(()),
            dma((2,)),
            pltpu.SemaphoreType.REGULAR,
        ],
        compiler_params=pltpu.CompilerParams(
            collective_id=0, has_side_effects=True
        ),
    )(data.transpose(0, 1, 3, 2), labels.transpose(0, 1, 3, 2), taps, offsets)
    return ready[None].transpose(0, 1, 3, 2)


def fits(data, tiles, views):
    _, slab, rows, depth = data.shape
    return (
        views == 4
        and depth * 4 == 128
        and slab * tiles == depth
        and slab == 8
        and tiles > 2
        and rows % (8 * (tiles - 2)) == 0
    )


def program(data, labels, kernel, offsets):
    if fits(data, lax.axis_size("tile"), lax.axis_size("view")):
        return by_rows(data, labels, kernel, offsets)
    return on_device(data, labels, kernel, offsets)


def solution(mesh):
    placed = (
        P(("parts", "view"), "tile", None, None),
        P(("parts", "view"), "tile", None, None),
        P("view", None, None),
        P("view", None),
    )
    return jax.shard_map(
        program,
        mesh=mesh,
        in_specs=placed,
        out_specs=P(("parts", "view"), "tile", None, None),
        check_vma=False,
    )
```

```python
import functools

import jax
import jax.numpy as jnp
from jax import lax
from jax.experimental import pallas as pl
from jax.experimental.pallas import tpu as pltpu
from jax.sharding import PartitionSpec as P

ITERS = 2
SWEEPS = 4


WEAK = 0.2
TAU = 0.15


def extended(cells, sides, width):
    for axis, dim in sides:
        count = lax.axis_size(axis)
        ends = count - 1
        head = lax.slice_in_dim(cells, 0, width, axis=dim)
        tail = lax.slice_in_dim(cells, cells.shape[dim] - width, cells.shape[dim], axis=dim)
        cells = jnp.concatenate(
            [
                lax.ppermute(tail, axis, [(i, (i + 1) % count) for i in range(ends)]),
                cells,
                lax.ppermute(head, axis, [((i + 1) % count, i) for i in range(ends)]),
            ],
            axis=dim,
        )
    return cells


def swapped(block, axis, stride):
    count = lax.axis_size(axis)
    route = []
    for low in range(count):
        high = low | 1 << stride
        if high != low and high < count:
            route += [(low, high), (high, low)]
    return lax.ppermute(block, axis, route)


def band(kernel, offsets):
    depth_cells = kernel.shape[0]
    taps = jnp.arange(kernel.shape[1], dtype=jnp.int32) - 4
    depth = jnp.arange(depth_cells, dtype=jnp.int32)
    index = jnp.clip(depth[:, None] + taps[None, :] + offsets[:, None], 0, depth_cells - 1)
    weight = kernel / jnp.sum(kernel, axis=1, keepdims=True)
    return (index, weight)


def axis_term(field, region, axis):
    count = field.shape[axis]
    upper = lax.slice_in_dim(field, 1, count, axis=axis)
    lower = lax.slice_in_dim(field, 0, count - 1, axis=axis)
    same = jnp.where(
        lax.slice_in_dim(region, 1, count, axis=axis)
        == lax.slice_in_dim(region, 0, count - 1, axis=axis),
        1.0,
        WEAK,
    )
    flux = same * (upper - lower)
    after = [(0, 0)] * 3
    before = [(0, 0)] * 3
    after[axis] = (0, 1)
    before[axis] = (1, 0)
    return jnp.pad(flux, after) - jnp.pad(flux, before)


def sweep_rows(field, region, first_row, total_rows):
    extent = field.shape[0]
    global_rows = first_row + jnp.arange(extent, dtype=jnp.int32)
    inside = ((global_rows >= 0) & (global_rows < total_rows)).astype(field.dtype)[:, None, None]
    same = jnp.where(region[1:] == region[:-1], 1.0, WEAK) * inside[1:] * inside[:-1]
    flux = same * (field[1:] - field[:-1])
    inner = field[1:-1]
    inner_labels = region[1:-1]
    total = (
        flux[1:] - flux[:-1] + axis_term(inner, inner_labels, 1) + axis_term(inner, inner_labels, 2)
    )
    return inner + TAU * total


def regroup(received, tiles):
    slab, rows, depth_cells = received.shape
    blocks = received.reshape(slab, rows, tiles, depth_cells // tiles)
    return blocks.transpose(3, 1, 2, 0).reshape(depth_cells // tiles, rows, depth_cells)


def on_device(data, labels, kernel, offsets):
    recorded = data[0]
    region = labels[0]
    index, weight = band(kernel[0], offsets[0])
    tiles = lax.axis_size("tile")
    slab, rows, depth_cells = recorded.shape
    total_rows = slab * tiles
    start = lax.axis_index("tile") * slab
    parity = lax.axis_index("view") % 2
    columns = jnp.arange(depth_cells, dtype=jnp.int32)
    matrix = jnp.sum(weight[:, :, None] * (index[:, :, None] == columns[None, None, :]), axis=1)
    label_ext = extended(region, (("tile", 0),), 4)
    current = recorded
    for step in range(ITERS):
        forward_flat = jnp.dot(
            current.reshape(-1, depth_cells), matrix.T, precision=lax.Precision.HIGHEST
        )
        field = recorded / forward_flat.reshape(current.shape)
        flat = jnp.dot(field.reshape(-1, depth_cells), matrix, precision=lax.Precision.HIGHEST)
        correction = flat.reshape(field.shape)
        turned = correction
        for repeat in range(2):
            turned = regroup(
                lax.all_to_all(
                    jnp.flip(turned, 2), "tile", split_axis=2, concat_axis=2, tiled=True
                ),
                tiles,
            )
        turned = swapped(turned, "view", 1)
        paired = jnp.sqrt(correction * turned)
        outgoing = jnp.where(parity == 0, jnp.flip(paired, 2), paired)
        rotated = regroup(
            lax.all_to_all(outgoing, "tile", split_axis=2, concat_axis=2, tiled=True), tiles
        )
        rotated = jnp.where(parity == 1, jnp.flip(rotated, 2), rotated)
        partner = swapped(rotated, "view", 0)
        current = current * jnp.sqrt(paired * partner)
        widened = extended(current, (("tile", 0),), 4)
        for sweep in range(SWEEPS):
            extent = widened.shape[0]
            widened = sweep_rows(
                widened, label_ext[sweep : sweep + extent], start - 4 + sweep, total_rows
            )
        current = widened
    return current[None]


def gathered(parts, b_of, slot, depth):
    fold = len(parts)
    lanes = parts[0].shape[1]
    total = None
    for k in range(fold):
        amount = (depth * (k - b_of[k])) % lanes
        piece = pltpu.roll(parts[k], amount, 1) if amount else parts[k]
        total = piece if total is None else jnp.where(slot == k, piece, total)
    return total


def turning(lanes, depth, flip_z):
    row_ids = lax.broadcasted_iota(jnp.int32, (lanes, lanes), 0)
    lane_ids = lax.broadcasted_iota(jnp.int32, (lanes, lanes), 1)
    same_block = (row_ids // depth) == (lane_ids // depth)
    aim = jnp.where(flip_z, depth - 1 - lane_ids % depth, lane_ids % depth)
    return same_block, jnp.where(same_block & (row_ids % depth == aim), 1.0, 0.0).astype(jnp.float32)


def exact(a, b):
    return jnp.dot(a, b, precision=lax.Precision.HIGHEST, preferred_element_type=jnp.float32)


def product(a, b, contract):
    return lax.dot_general(a, b, (contract, ((), ())), preferred_element_type=jnp.float32)


def halves(a):
    high = a.astype(jnp.bfloat16)
    return high, (a - high.astype(jnp.float32)).astype(jnp.bfloat16)


def permuted(a, turn):
    high, low = halves(a)
    turn = turn.astype(jnp.bfloat16)
    return product(high, turn, ((1,), (0,))) + product(low, turn, ((1,), (0,)))


def widened(matrix):
    high, low = halves(matrix)
    none = jnp.zeros_like(high)
    return jnp.concatenate(
        [jnp.concatenate([high, low], axis=1), jnp.concatenate([high, none], axis=1)], axis=0
    )


def blurred(a, wide):
    both = product(jnp.concatenate(halves(a), axis=1), wide, ((1,), (0,)))
    lanes = a.shape[1]
    return both[:, :lanes] + both[:, lanes:]


def fused(tiles, data_ref, labels_ref, taps_ref, shift_ref, unpacked, raw, raw_labels, taps_buf, shift_buf, mixed, packed, packed_labels, held, held_labels, mats, est, coef, outgoing, incoming, leave, back, around, slab_coef, settled, sent, in_sem, data_sem, label_sem, mat_sem, swap_sem, back_sem, side_sem, send, send_side, late_sem):
    mesh_id = pl.DeviceIdType.MESH
    slab, depth, rows = data_ref.shape[1:]
    lanes = packed.shape[2]
    fold = lanes // depth
    groups = rows // fold
    width = held.shape[1]
    keep = width - 2
    cells = held.shape[2]
    span = back.shape[1]
    pad = (span - slab) // 2
    view = lax.axis_index("view")
    tile = lax.axis_index("tile")
    part = lax.axis_index("parts")
    half = view // 2
    core = view % 2
    workers = tiles - 2
    ends = tiles - workers
    works = (tile > 0) & (tile <= workers)
    idle = (tile == 0) | (tile > workers)
    flip_x = (view == 1) | (view == 2)
    flip_z = view >= 2

    def at_device(h, t):
        return (part, 2 * h + core, t)

    across = (part, 2 * half + 1 - core, tile)

    barrier = pltpu.get_barrier_semaphore()

    @pl.when(works)
    def _():
        for d in range(1, tiles):
            for h in (1 - half, half):
                pl.semaphore_signal(
                    barrier,
                    inc=1,
                    device_id=at_device(h, (tile + d) % tiles),
                    device_id_type=mesh_id,
                )
        pl.semaphore_signal(
            barrier, inc=1, device_id=at_device(1 - half, tile), device_id_type=mesh_id
        )

    pl.semaphore_signal(barrier, inc=1, device_id=across, device_id_type=mesh_id)

    small = [
        pltpu.make_async_copy(taps_ref, taps_buf, in_sem.at[2]),
        pltpu.make_async_copy(shift_ref, shift_buf, in_sem.at[3]),
    ]
    for copy in small:
        copy.start()

    for source, target, sem in ((data_ref, raw, 0), (labels_ref, raw_labels, 1)):
        for x in range(slab):
            at = jnp.where(flip_x, slab - 1 - x, x)
            pltpu.make_async_copy(
                source.at[0, x],
                target.at[pl.ds(pl.multiple_of(at * depth, 8), depth)],
                in_sem.at[sem],
            ).start()
    def whole(ref, sem):
        pltpu.make_async_copy(ref, ref, sem).wait()

    same_block, turn = turning(lanes, depth, flip_z)
    slot = lax.broadcasted_iota(jnp.int32, (mixed.shape[1] // fold, lanes), 1) // depth
    blocks = slab * depth // lanes

    def pack(source, target, fill, turner):
        edge = jnp.full((1, slab, lanes), fill, jnp.float32)
        target[0:1] = edge
        target[groups + 1 : groups + 2] = edge
        for j in range(blocks):
            mixed[j, 0:rows] = turner(source[lanes * j : lanes * (j + 1), :])
        for j in range(blocks):
            parts = [
                mixed[j, pl.ds(b, mixed.shape[1] // fold, stride=fold), :] for b in range(fold)
            ]
            for k in range(fold):
                line = gathered(parts, [k] * fold, slot, depth)
                target[1 : groups + 1, fold * j + k, :] = line[:groups]

    def turned_labels(block):
        block = block.astype(jnp.float32).T.astype(jnp.bfloat16)
        return product(block, turn.astype(jnp.bfloat16), ((1,), (0,)))

    place = jnp.where(flip_x, tiles - 1 - tile, tile)
    spot = pl.ds(pl.multiple_of(place * slab, 8), slab)

    last = 2 * workers - 1
    homes = [(h, t) for t in range(1, workers + 1) for h in range(2)]

    def scatter(source, target, sem):
        for a in range(2):
            for own in range(tiles):

                @pl.when((half == a) & (tile == own))
                def _():
                    for h, t in sorted(homes, key=lambda ht: (-abs(ht[1] - own), ht[0] == a)):
                        number = 2 * (t - 1) + h
                        low = 1 if number == 0 else 0
                        size = width - (number in (0, last))
                        src = source.at[pl.ds(keep * number + low, size)]
                        dst = target.at[a, pl.ds(low, size), spot, :]
                        if (h, t) == (a, own):
                            copy = pltpu.make_async_copy(src, dst, sem)
                        else:
                            copy = pltpu.make_async_remote_copy(
                                src_ref=src,
                                dst_ref=dst,
                                send_sem=send,
                                recv_sem=sem,
                                device_id=at_device(h, t),
                                device_id_type=mesh_id,
                            )
                        copy.start()

    for copy in small:
        copy.wait()
    @pl.when(works)
    def _():
        count = taps_buf.shape[0]
        taps = [jnp.concatenate([taps_buf[k]] * fold, axis=1) for k in range(count)]
        scale = taps[0]
        for k in range(1, count):
            scale = scale + taps[k]
        shift = jnp.concatenate([shift_buf[...]] * fold, axis=1)
        level = lax.broadcasted_iota(jnp.int32, (1, lanes), 1) % depth
        strip_row = lax.broadcasted_iota(jnp.int32, (depth, lanes), 0)
        strip_aim = jnp.where(flip_z, depth - 1 - strip_row, strip_row)
        strip = jnp.zeros((depth, lanes), jnp.float32)
        for k in range(count):
            index = jnp.clip(level + (k - 4) + shift, 0, depth - 1)
            strip = strip + jnp.where(index == strip_aim, taps[k] / scale, 0.0)
        strip = exact(strip, turn)
        mats[pl.ds(half, 1)] = strip[None]

    mat_copy = pltpu.make_async_remote_copy(
        src_ref=mats.at[half],
        dst_ref=mats.at[half],
        send_sem=send,
        recv_sem=mat_sem,
        device_id=at_device(1 - half, tile),
        device_id_type=mesh_id,
    )

    whole(raw, in_sem.at[0])
    pack(raw, packed, 1.0, lambda v: permuted(v.T, turn))
    pl.semaphore_wait(barrier, jnp.where(works, 2 * workers, 2 * workers + 1))

    @pl.when(idle)
    def _():
        for t in range(1, workers + 1):
            for h in (1 - half, half):
                pl.semaphore_signal(
                    late_sem, inc=1, device_id=at_device(h, t), device_id_type=mesh_id
                )

    pl.when(works)(mat_copy.start)
    scatter(packed, held, data_sem)

    whole(raw_labels, in_sem.at[1])
    pack(raw_labels, packed_labels, 0.0, turned_labels)
    pl.when((core == 1) & idle)(lambda: pl.delay(2200))
    scatter(packed_labels, held_labels, label_sem)

    inner_labels = packed_labels.at[pl.ds(1, groups)]

    def beside(side):
        onto = place + 1 - 2 * side
        t = jnp.where(flip_x, tiles - 1 - onto, onto)
        return pltpu.make_async_remote_copy(
            src_ref=inner_labels,
            dst_ref=around.at[:, pl.ds(2 * slab * side, slab), :],
            send_sem=send_side.at[side],
            recv_sem=side_sem.at[side],
            device_id=(part, view, jnp.clip(t, 0, tiles - 1)),
            device_id_type=mesh_id,
        )

    has_above = place < tiles - 1
    has_below = place > 0

    def start_sides():
        @pl.when(has_above)
        def _():
            beside(0).start()

        @pl.when(has_below)
        def _():
            beside(1).start()

    @pl.when(jnp.logical_not(has_below))
    def _():
        around[:, 0:slab, :] = jnp.zeros((groups, slab, lanes), jnp.float32)

    @pl.when(jnp.logical_not(has_above))
    def _():
        around[:, 2 * slab : 3 * slab, :] = jnp.zeros((groups, slab, lanes), jnp.float32)

    around[:, slab : 2 * slab, :] = packed_labels[1 : groups + 1]
    for s in range(2):
        for k in range(leave.shape[1]):
            leave[s, k, 0:pad] = jnp.zeros((pad, lanes), jnp.float32)
            leave[s, k, pad + cells : 2 * pad + cells] = jnp.zeros((pad, lanes), jnp.float32)

    lane = lax.broadcasted_iota(jnp.int32, (cells, lanes), 1)
    sub = lax.broadcasted_iota(jnp.int32, (cells, lanes), 0)
    block = 2 * (tile - 1) + half
    edge = (block == 0) | (block == last)

    def landed(ref, fill, sem):
        @pl.when(edge)
        def _():
            whole(ref.at[:, pl.ds(0, width - 1)], sem)

        @pl.when(jnp.logical_not(edge))
        def _():
            whole(ref, sem)

        for number, slot_at in ((0, 0), (last, width - 1)):

            @pl.when(block == number)
            def _():
                for s in range(2):
                    ref[s, slot_at] = jnp.full((cells, lanes), fill, jnp.float32)

    first = keep * block - 1

    def lanes_of(field):
        return lane[: field.shape[0]]

    def ahead_y(fields, g):
        after = fields[(g + 1) % len(fields)]
        return jnp.where(
            lanes_of(fields[g]) < lanes - depth,
            pltpu.roll(fields[g], lanes - depth, 1),
            pltpu.roll(after, lanes - depth, 1),
        )

    def behind_y(fields, g):
        return jnp.where(
            lanes_of(fields[g]) < depth,
            pltpu.roll(fields[g - 1], depth, 1),
            pltpu.roll(fields[g], depth, 1),
        )

    def steps(mask):
        return jnp.where(mask, TAU, 0.0), jnp.where(mask, TAU * WEAK, 0.0)

    def limits(high, count, x_inside, y_first):
        lane_of = lane[:high]
        along_y = []
        for g in range(count):
            y = fold * (y_first + g) + lane_of // depth
            along_y.append(steps((y >= 0) & (y < rows - 1)))
        return steps(x_inside), along_y, steps(lane_of % depth < depth - 1)

    def weights(regions, bounds):
        along_x, along_y, along_z = bounds
        high = regions[0].shape[0]
        count = len(regions)
        up_y = [jnp.where(ahead_y(regions, g) == regions[g], *along_y[g]) for g in range(count)]
        result = []
        for g in range(count):
            mine = regions[g]
            up_x = jnp.where(pltpu.roll(mine, high - 1, 0) == mine, *along_x)
            up_z = jnp.where(pltpu.roll(mine, lanes - 1, 1) == mine, *along_z)
            down_x = pltpu.roll(up_x, 1, 0)
            down_z = pltpu.roll(up_z, 1, 1)
            down_y = behind_y(up_y, g)
            middle = 1.0 - (((up_x + down_x) + (up_z + down_z)) + (up_y[g] + down_y))
            result.append((middle, up_x, down_x, up_y[g], down_y, up_z, down_z))
        return result

    def swept(fields, factors, g):
        f = fields[g]
        high = f.shape[0]
        middle, up_x, down_x, up_y, down_y, up_z, down_z = factors
        return (
            (middle * f + up_x * pltpu.roll(f, high - 1, 0))
            + (down_x * pltpu.roll(f, 1, 0) + up_z * pltpu.roll(f, lanes - 1, 1))
        ) + (
            down_z * pltpu.roll(f, 1, 1)
            + (up_y * ahead_y(fields, g) + down_y * behind_y(fields, g))
        )

    def transposed(p):
        result = []
        for start in range(0, p.shape[0] // cells, fold):
            chunk = p[cells * start : cells * (start + fold)]
            found = chunk.shape[0] // cells
            flipped = jnp.concatenate([chunk] + [chunk[:cells]] * (fold - found), axis=0).T
            for g in range(found):
                piece = flipped[0:depth]
                if g:
                    piece = pltpu.roll(piece, (lanes - depth * g) % lanes, 1)
                for b in range(1, fold):
                    part_b = flipped[depth * b : depth * (b + 1)]
                    amount = (depth * (b - g)) % lanes
                    if amount:
                        part_b = pltpu.roll(part_b, amount, 1)
                    piece = jnp.where(lane // depth == b, part_b, piece)
                result.append(piece)
        return result

    @pl.when(works)
    def _():
        mat_copy.wait_recv()
        bounds = limits(cells, width, sub < cells - 1, first)
        blurs = []
        for s in range(2):
            matrix = jnp.where(same_block, jnp.concatenate([mats[s]] * fold, axis=0), 0.0)
            blurs.append((widened(matrix), widened(matrix.T)))
        landed(held, 1.0, data_sem)

        def paired_of(chosen, currents):
            corrections = []
            for s in range(2):
                recorded = jnp.concatenate([held[s, g] for g in chosen], axis=0)
                current = recorded if currents is None else jnp.concatenate(currents[s], axis=0)
                ratio = recorded / blurred(current, blurs[s][0])
                corrections.append(blurred(ratio, blurs[s][1]))
            return jnp.sqrt(corrections[0] * corrections[1])

        def swapped_over(step, begin, size):
            copy = pltpu.make_async_remote_copy(
                src_ref=outgoing.at[step, pl.ds(begin, size)],
                dst_ref=incoming.at[step, pl.ds(begin, size)],
                send_sem=send,
                recv_sem=swap_sem.at[step],
                device_id=across,
                device_id_type=mesh_id,
            )
            copy.start()
            return copy

        paired = paired_of(range(width), None)
        for g, piece in enumerate(transposed(paired)):
            outgoing[0, g] = piece
        swap = swapped_over(0, 0, width)
        pl.semaphore_wait(late_sem, 2 * ends)
        start_sides()
        landed(held_labels, 0.0, label_sem)
        for s in range(2):
            found = weights([held_labels[s, g] for g in range(width)], bounds)
            for g in range(width):
                for i in range(len(found[g])):
                    coef[i, s, g] = found[g][i]
        swap.wait_recv()
        joined = [
            jnp.sqrt(paired[cells * g : cells * (g + 1)] * incoming[0, g]) for g in range(width)
        ]
        fields = [[held[s, g] * joined[g] for g in range(width)] for s in range(2)]
        inner = range(1, width - 1)
        for sweep in range(SWEEPS):
            kept = inner if sweep == SWEEPS - 1 else range(width)
            fresh = [list(fields[s]) for s in range(2)]
            for s in range(2):
                for g in kept:
                    factors = [coef[i, s, g] for i in range(coef.shape[0])]
                    fresh[s][g] = swept(fields[s], factors, g)
            fields = fresh

        currents = [[fields[s][g] for g in inner] for s in range(2)]
        paired = paired_of(inner, currents)
        for s in range(2):
            for k in range(len(inner)):
                est[s, k] = currents[s][k]
        for k, piece in enumerate(transposed(paired)):
            outgoing[1, k] = piece
        swap = swapped_over(1, 0, len(inner))
        swap.wait_recv()
        for k in range(len(inner)):
            joined = jnp.sqrt(paired[cells * k : cells * (k + 1)] * incoming[1, k])
            for s in range(2):
                leave[s, k, pad : pad + cells] = est[s, k] * joined

        def window(h, t):
            flipped = core == 1 - h
            return pl.ds(pl.multiple_of(jnp.where(flipped, tiles - 1 - t, t) * slab, 8), span)

        def returned(h, t):
            return pltpu.make_async_remote_copy(
                src_ref=leave.at[h, :, window(h, t), :],
                dst_ref=back.at[own],
                send_sem=send,
                recv_sem=back_sem,
                device_id=at_device(h, t),
                device_id_type=mesh_id,
            )

        own = pl.ds(keep * block, keep)
        returned(0, 0).start()
        returned(1, 0).start()
        returned(1, tiles - 1).start()
        returned(0, tiles - 1).start()
        for t in range(1, tiles - 1):
            returned(1 - half, t).start()

            @pl.when(tile == t)
            def _():
                pltpu.make_async_copy(
                    leave.at[half, :, window(half, t), :], back.at[own], back_sem
                ).start()

            @pl.when(tile != t)
            def _():
                returned(half, t).start()

    pl.when(idle)(start_sides)

    @pl.when(has_below)
    def _():
        beside(0).wait_recv()

    @pl.when(has_above)
    def _():
        beside(1).wait_recv()

    x_at = place * slab - pad + sub[:span]
    x_inside = (x_at >= 0) & (x_at < cells - 1) & (sub[:span] < span - 1)
    bounds = limits(span, groups, x_inside, 0)
    found = weights([around[g, slab - pad : 2 * slab + pad] for g in range(groups)], bounds)
    for g in range(groups):
        for i in range(len(found[g])):
            slab_coef[i, g] = found[g][i]

    @pl.when(has_above)
    def _():
        beside(0).wait_send()

    @pl.when(has_below)
    def _():
        beside(1).wait_send()

    swaps = (width + keep) * cells
    pieces = 2 * workers * width - 2

    def all_sent(kept_back, more):
        whole(sent.at[pl.ds(0, 2 * (pieces - kept_back) * slab + more)], send)

    after = depth + swaps + (2 * tiles - 1) * keep * span
    pl.when(works & edge)(lambda: all_sent(width - 1, after))
    pl.when(works & jnp.logical_not(edge))(lambda: all_sent(width, after))
    pl.when(idle)(lambda: all_sent(0, 0))
    turned_twice = turn.astype(jnp.bfloat16)
    whole(back, back_sem)
    fields = [back[g] for g in range(groups)]
    for sweep in range(SWEEPS):
        fields = [
            swept(fields, [slab_coef[i, g] for i in range(slab_coef.shape[0])], g)
            for g in range(groups)
        ]
    for g in range(groups):
        settled[g] = fields[g][pad : pad + slab]
    for j in range(blocks):
        parts = []
        for k in range(fold):
            line = settled[:, fold * j + k, :]
            parts.append(
                jnp.concatenate(
                    [line, jnp.zeros((mixed.shape[1] // fold - groups, lanes), jnp.float32)], axis=0
                )
            )
        for b in range(fold):
            mixed[j, pl.ds(b, mixed.shape[1] // fold, stride=fold), :] = gathered(
                parts, [b] * fold, slot, depth
            )
        lined = product(
            jnp.concatenate([turned_twice] * 2, axis=1),
            jnp.concatenate(halves(mixed[j, 0:rows]), axis=1),
            ((1,), (1,)),
        )
        for k in range(fold):
            x = fold * j + k
            at = jnp.where(flip_x, slab - 1 - x, x)
            unpacked[pl.ds(at, 1)] = lined[depth * k : depth * (k + 1)][None]


def by_rows(data, labels, kernel, offsets):
    tiles = lax.axis_size("tile")
    _, slab, rows, depth = data.shape
    fold = 128 // depth
    tall = -(-rows // (8 * fold)) * 8 * fold
    groups = rows // fold
    cells = slab * tiles
    kept = groups // (2 * (tiles - 2))
    width = kept + 2
    span = slab + 2 * SWEEPS
    flat = (slab * depth, rows)
    wide = (2, width, cells, 128)
    strips = (groups + 2, slab, 128)
    sent = 4 * tiles * width * slab + depth + (width + kept) * cells + 2 * tiles * kept * span
    dma = pltpu.SemaphoreType.DMA
    taps = kernel.transpose(2, 0, 1)
    ready = pl.pallas_call(
        functools.partial(fused, tiles),
        out_shape=pltpu.VMEM((slab, depth, rows), jnp.float32),
        in_specs=[pl.BlockSpec(memory_space=pltpu.HBM)] * 4,
        out_specs=pl.BlockSpec(memory_space=pltpu.VMEM),
        scratch_shapes=[
            pltpu.VMEM(flat, jnp.float32),
            pltpu.VMEM(flat, jnp.int32),
            pltpu.VMEM(taps.shape, jnp.float32),
            pltpu.VMEM(offsets.shape, jnp.int32),
            pltpu.VMEM((slab * depth // 128, tall, 128), jnp.float32),
            pltpu.VMEM(strips, jnp.float32),
            pltpu.VMEM(strips, jnp.float32),
            pltpu.VMEM(wide, jnp.float32),
            pltpu.VMEM(wide, jnp.float32),
            pltpu.VMEM((2, depth, 128), jnp.float32),
            pltpu.VMEM((2, kept, cells, 128), jnp.float32),
            pltpu.VMEM((7,) + wide, jnp.float32),
            pltpu.VMEM((ITERS,) + wide[1:], jnp.float32),
            pltpu.VMEM((ITERS,) + wide[1:], jnp.float32),
            pltpu.VMEM((2, kept, cells + span - slab, 128), jnp.float32),
            pltpu.VMEM((groups, span, 128), jnp.float32),
            pltpu.VMEM((groups, 3 * slab, 128), jnp.float32),
            pltpu.VMEM((7, groups, span, 128), jnp.float32),
            pltpu.VMEM((groups, slab, 128), jnp.float32),
            pltpu.VMEM((sent, 128), jnp.float32),
            dma((4,)),
            dma(()),
            dma(()),
            dma(()),
            dma((ITERS,)),
            dma(()),
            dma((2,)),
            dma(()),
            dma((2,)),
            pltpu.SemaphoreType.REGULAR,
        ],
        compiler_params=pltpu.CompilerParams(
            collective_id=0, has_side_effects=True
        ),
    )(data.transpose(0, 1, 3, 2), labels.transpose(0, 1, 3, 2), taps, offsets)
    return ready[None].transpose(0, 1, 3, 2)


def fits(data, tiles, views):
    _, slab, rows, depth = data.shape
    return (
        views == 4
        and depth * 4 == 128
        and slab * tiles == depth
        and slab == 8
        and tiles > 2
        and rows % (8 * (tiles - 2)) == 0
    )


def program(data, labels, kernel, offsets):
    if fits(data, lax.axis_size("tile"), lax.axis_size("view")):
        return by_rows(data, labels, kernel, offsets)
    return on_device(data, labels, kernel, offsets)


def solution(mesh):
    placed = (
        P(("parts", "view"), "tile", None, None),
        P(("parts", "view"), "tile", None, None),
        P("view", None, None),
        P("view", None),
    )
    return jax.shard_map(
        program,
        mesh=mesh,
        in_specs=placed,
        out_specs=P(("parts", "view"), "tile", None, None),
        check_vma=False,
    )
```

```python
import functools

import jax
import jax.numpy as jnp
from jax import lax
from jax.experimental import pallas as pl
from jax.experimental.pallas import tpu as pltpu
from jax.sharding import PartitionSpec as P

ITERS = 2
SWEEPS = 4


WEAK = 0.2
TAU = 0.15


def extended(cells, sides, width):
    for axis, dim in sides:
        count = lax.axis_size(axis)
        ends = count - 1
        head = lax.slice_in_dim(cells, 0, width, axis=dim)
        tail = lax.slice_in_dim(cells, cells.shape[dim] - width, cells.shape[dim], axis=dim)
        cells = jnp.concatenate(
            [
                lax.ppermute(tail, axis, [(i, (i + 1) % count) for i in range(ends)]),
                cells,
                lax.ppermute(head, axis, [((i + 1) % count, i) for i in range(ends)]),
            ],
            axis=dim,
        )
    return cells


def swapped(block, axis, stride):
    count = lax.axis_size(axis)
    route = []
    for low in range(count):
        high = low | 1 << stride
        if high != low and high < count:
            route += [(low, high), (high, low)]
    return lax.ppermute(block, axis, route)


def band(kernel, offsets):
    depth_cells = kernel.shape[0]
    taps = jnp.arange(kernel.shape[1], dtype=jnp.int32) - 4
    depth = jnp.arange(depth_cells, dtype=jnp.int32)
    index = jnp.clip(depth[:, None] + taps[None, :] + offsets[:, None], 0, depth_cells - 1)
    weight = kernel / jnp.sum(kernel, axis=1, keepdims=True)
    return (index, weight)


def axis_term(field, region, axis):
    count = field.shape[axis]
    upper = lax.slice_in_dim(field, 1, count, axis=axis)
    lower = lax.slice_in_dim(field, 0, count - 1, axis=axis)
    same = jnp.where(
        lax.slice_in_dim(region, 1, count, axis=axis)
        == lax.slice_in_dim(region, 0, count - 1, axis=axis),
        1.0,
        WEAK,
    )
    flux = same * (upper - lower)
    after = [(0, 0)] * 3
    before = [(0, 0)] * 3
    after[axis] = (0, 1)
    before[axis] = (1, 0)
    return jnp.pad(flux, after) - jnp.pad(flux, before)


def sweep_rows(field, region, first_row, total_rows):
    extent = field.shape[0]
    global_rows = first_row + jnp.arange(extent, dtype=jnp.int32)
    inside = ((global_rows >= 0) & (global_rows < total_rows)).astype(field.dtype)[:, None, None]
    same = jnp.where(region[1:] == region[:-1], 1.0, WEAK) * inside[1:] * inside[:-1]
    flux = same * (field[1:] - field[:-1])
    inner = field[1:-1]
    inner_labels = region[1:-1]
    total = (
        flux[1:] - flux[:-1] + axis_term(inner, inner_labels, 1) + axis_term(inner, inner_labels, 2)
    )
    return inner + TAU * total


def regroup(received, tiles):
    slab, rows, depth_cells = received.shape
    blocks = received.reshape(slab, rows, tiles, depth_cells // tiles)
    return blocks.transpose(3, 1, 2, 0).reshape(depth_cells // tiles, rows, depth_cells)


def on_device(data, labels, kernel, offsets):
    recorded = data[0]
    region = labels[0]
    index, weight = band(kernel[0], offsets[0])
    tiles = lax.axis_size("tile")
    slab, rows, depth_cells = recorded.shape
    total_rows = slab * tiles
    start = lax.axis_index("tile") * slab
    parity = lax.axis_index("view") % 2
    columns = jnp.arange(depth_cells, dtype=jnp.int32)
    matrix = jnp.sum(weight[:, :, None] * (index[:, :, None] == columns[None, None, :]), axis=1)
    label_ext = extended(region, (("tile", 0),), 4)
    current = recorded
    for step in range(ITERS):
        forward_flat = jnp.dot(
            current.reshape(-1, depth_cells), matrix.T, precision=lax.Precision.HIGHEST
        )
        field = recorded / forward_flat.reshape(current.shape)
        flat = jnp.dot(field.reshape(-1, depth_cells), matrix, precision=lax.Precision.HIGHEST)
        correction = flat.reshape(field.shape)
        turned = correction
        for repeat in range(2):
            turned = regroup(
                lax.all_to_all(
                    jnp.flip(turned, 2), "tile", split_axis=2, concat_axis=2, tiled=True
                ),
                tiles,
            )
        turned = swapped(turned, "view", 1)
        paired = jnp.sqrt(correction * turned)
        outgoing = jnp.where(parity == 0, jnp.flip(paired, 2), paired)
        rotated = regroup(
            lax.all_to_all(outgoing, "tile", split_axis=2, concat_axis=2, tiled=True), tiles
        )
        rotated = jnp.where(parity == 1, jnp.flip(rotated, 2), rotated)
        partner = swapped(rotated, "view", 0)
        current = current * jnp.sqrt(paired * partner)
        widened = extended(current, (("tile", 0),), 4)
        for sweep in range(SWEEPS):
            extent = widened.shape[0]
            widened = sweep_rows(
                widened, label_ext[sweep : sweep + extent], start - 4 + sweep, total_rows
            )
        current = widened
    return current[None]


def gathered(parts, b_of, slot, depth):
    fold = len(parts)
    lanes = parts[0].shape[1]
    total = None
    for k in range(fold):
        amount = (depth * (k - b_of[k])) % lanes
        piece = pltpu.roll(parts[k], amount, 1) if amount else parts[k]
        total = piece if total is None else jnp.where(slot == k, piece, total)
    return total


def turning(lanes, depth, flip_z):
    row_ids = lax.broadcasted_iota(jnp.int32, (lanes, lanes), 0)
    lane_ids = lax.broadcasted_iota(jnp.int32, (lanes, lanes), 1)
    same_block = (row_ids // depth) == (lane_ids // depth)
    aim = jnp.where(flip_z, depth - 1 - lane_ids % depth, lane_ids % depth)
    return same_block, jnp.where(same_block & (row_ids % depth == aim), 1.0, 0.0).astype(jnp.float32)


def exact(a, b):
    return jnp.dot(a, b, precision=lax.Precision.HIGHEST, preferred_element_type=jnp.float32)


def product(a, b, contract):
    return lax.dot_general(a, b, (contract, ((), ())), preferred_element_type=jnp.float32)


def halves(a):
    high = a.astype(jnp.bfloat16)
    return high, (a - high.astype(jnp.float32)).astype(jnp.bfloat16)


def permuted(a, turn):
    high, low = halves(a)
    turn = turn.astype(jnp.bfloat16)
    return product(high, turn, ((1,), (0,))) + product(low, turn, ((1,), (0,)))


def widened(matrix):
    high, low = halves(matrix)
    none = jnp.zeros_like(high)
    return jnp.concatenate(
        [jnp.concatenate([high, low], axis=1), jnp.concatenate([high, none], axis=1)], axis=0
    )


def blurred(a, wide):
    both = product(jnp.concatenate(halves(a), axis=1), wide, ((1,), (0,)))
    lanes = a.shape[1]
    return both[:, :lanes] + both[:, lanes:]


def fused(tiles, data_ref, labels_ref, taps_ref, shift_ref, unpacked, raw, raw_labels, taps_buf, shift_buf, mixed, packed, packed_labels, held, held_labels, mats, est, coef, outgoing, incoming, leave, back, around, slab_coef, settled, sent, in_sem, data_sem, label_sem, mat_sem, swap_sem, back_sem, side_sem, send, late_sem):
    mesh_id = pl.DeviceIdType.MESH
    slab, depth, rows = data_ref.shape[1:]
    lanes = packed.shape[2]
    fold = lanes // depth
    groups = rows // fold
    width = held.shape[1]
    keep = width - 2
    cells = held.shape[2]
    span = back.shape[1]
    pad = (span - slab) // 2
    view = lax.axis_index("view")
    tile = lax.axis_index("tile")
    part = lax.axis_index("parts")
    half = view // 2
    core = view % 2
    workers = tiles - 2
    ends = tiles - workers
    works = (tile > 0) & (tile <= workers)
    idle = (tile == 0) | (tile > workers)
    flip_x = (view == 1) | (view == 2)
    flip_z = view >= 2

    def at_device(h, t):
        return (part, 2 * h + core, t)

    across = (part, 2 * half + 1 - core, tile)

    barrier = pltpu.get_barrier_semaphore()

    @pl.when(works)
    def _():
        for d in range(1, tiles):
            for h in (1 - half, half):
                pl.semaphore_signal(
                    barrier,
                    inc=1,
                    device_id=at_device(h, (tile + d) % tiles),
                    device_id_type=mesh_id,
                )
        pl.semaphore_signal(
            barrier, inc=1, device_id=at_device(1 - half, tile), device_id_type=mesh_id
        )

    pl.semaphore_signal(barrier, inc=1, device_id=across, device_id_type=mesh_id)

    small = [
        pltpu.make_async_copy(taps_ref, taps_buf, in_sem.at[2]),
        pltpu.make_async_copy(shift_ref, shift_buf, in_sem.at[3]),
    ]
    for copy in small:
        copy.start()

    for source, target, sem in ((data_ref, raw, 0), (labels_ref, raw_labels, 1)):
        for x in range(slab):
            at = jnp.where(flip_x, slab - 1 - x, x)
            pltpu.make_async_copy(
                source.at[0, x],
                target.at[pl.ds(pl.multiple_of(at * depth, 8), depth)],
                in_sem.at[sem],
            ).start()
    def whole(ref, sem):
        pltpu.make_async_copy(ref, ref, sem).wait()

    same_block, turn = turning(lanes, depth, flip_z)
    slot = lax.broadcasted_iota(jnp.int32, (mixed.shape[1] // fold, lanes), 1) // depth
    blocks = slab * depth // lanes

    def pack(source, target, fill, turner):
        edge = jnp.full((1, slab, lanes), fill, jnp.float32)
        target[0:1] = edge
        target[groups + 1 : groups + 2] = edge
        for j in range(blocks):
            mixed[j, 0:rows] = turner(source[lanes * j : lanes * (j + 1), :])
        for j in range(blocks):
            parts = [
                mixed[j, pl.ds(b, mixed.shape[1] // fold, stride=fold), :] for b in range(fold)
            ]
            for k in range(fold):
                line = gathered(parts, [k] * fold, slot, depth)
                target[1 : groups + 1, fold * j + k, :] = line[:groups]

    def turned_labels(block):
        block = block.astype(jnp.float32).T.astype(jnp.bfloat16)
        return product(block, turn.astype(jnp.bfloat16), ((1,), (0,)))

    place = jnp.where(flip_x, tiles - 1 - tile, tile)
    spot = pl.ds(pl.multiple_of(place * slab, 8), slab)

    last = 2 * workers - 1
    homes = [(h, t) for t in range(1, workers + 1) for h in range(2)]

    def scatter(source, target, sem):
        for a in range(2):
            for own in range(tiles):

                @pl.when((half == a) & (tile == own))
                def _():
                    for h, t in sorted(homes, key=lambda ht: (-abs(ht[1] - own), ht[0] == a)):
                        number = 2 * (t - 1) + h
                        low = 1 if number == 0 else 0
                        size = width - (number in (0, last))
                        src = source.at[pl.ds(keep * number + low, size)]
                        dst = target.at[a, pl.ds(low, size), spot, :]
                        if (h, t) == (a, own):
                            copy = pltpu.make_async_copy(src, dst, sem)
                        else:
                            copy = pltpu.make_async_remote_copy(
                                src_ref=src,
                                dst_ref=dst,
                                send_sem=send,
                                recv_sem=sem,
                                device_id=at_device(h, t),
                                device_id_type=mesh_id,
                            )
                        copy.start()

    for copy in small:
        copy.wait()
    @pl.when(works)
    def _():
        count = taps_buf.shape[0]
        taps = [jnp.concatenate([taps_buf[k]] * fold, axis=1) for k in range(count)]
        scale = taps[0]
        for k in range(1, count):
            scale = scale + taps[k]
        shift = jnp.concatenate([shift_buf[...]] * fold, axis=1)
        level = lax.broadcasted_iota(jnp.int32, (1, lanes), 1) % depth
        strip_row = lax.broadcasted_iota(jnp.int32, (depth, lanes), 0)
        strip_aim = jnp.where(flip_z, depth - 1 - strip_row, strip_row)
        strip = jnp.zeros((depth, lanes), jnp.float32)
        for k in range(count):
            index = jnp.clip(level + (k - 4) + shift, 0, depth - 1)
            strip = strip + jnp.where(index == strip_aim, taps[k] / scale, 0.0)
        strip = exact(strip, turn)
        mats[pl.ds(half, 1)] = strip[None]

    mat_copy = pltpu.make_async_remote_copy(
        src_ref=mats.at[half],
        dst_ref=mats.at[half],
        send_sem=send,
        recv_sem=mat_sem,
        device_id=at_device(1 - half, tile),
        device_id_type=mesh_id,
    )

    whole(raw, in_sem.at[0])
    pack(raw, packed, 1.0, lambda v: permuted(v.T, turn))
    pl.semaphore_wait(barrier, jnp.where(works, 2 * workers, 2 * workers + 1))

    @pl.when(idle)
    def _():
        for t in range(1, workers + 1):
            for h in (1 - half, half):
                pl.semaphore_signal(
                    late_sem, inc=1, device_id=at_device(h, t), device_id_type=mesh_id
                )

    pl.when(works)(mat_copy.start)
    scatter(packed, held, data_sem)

    whole(raw_labels, in_sem.at[1])
    pack(raw_labels, packed_labels, 0.0, turned_labels)
    pl.when((core == 1) & idle)(lambda: pl.delay(2200))
    scatter(packed_labels, held_labels, label_sem)

    inner_labels = packed_labels.at[pl.ds(1, groups)]

    def beside(side):
        onto = place + 1 - 2 * side
        t = jnp.where(flip_x, tiles - 1 - onto, onto)
        return pltpu.make_async_remote_copy(
            src_ref=inner_labels,
            dst_ref=around.at[:, pl.ds(2 * slab * side, slab), :],
            send_sem=send,
            recv_sem=side_sem.at[side],
            device_id=(part, view, jnp.clip(t, 0, tiles - 1)),
            device_id_type=mesh_id,
        )

    has_above = place < tiles - 1
    has_below = place > 0

    def start_sides():
        @pl.when(has_above)
        def _():
            beside(0).start()

        @pl.when(has_below)
        def _():
            beside(1).start()

    @pl.when(jnp.logical_not(has_below))
    def _():
        around[:, 0:slab, :] = jnp.zeros((groups, slab, lanes), jnp.float32)

    @pl.when(jnp.logical_not(has_above))
    def _():
        around[:, 2 * slab : 3 * slab, :] = jnp.zeros((groups, slab, lanes), jnp.float32)

    around[:, slab : 2 * slab, :] = packed_labels[1 : groups + 1]
    for s in range(2):
        for k in range(leave.shape[1]):
            leave[s, k, 0:pad] = jnp.zeros((pad, lanes), jnp.float32)
            leave[s, k, pad + cells : 2 * pad + cells] = jnp.zeros((pad, lanes), jnp.float32)

    lane = lax.broadcasted_iota(jnp.int32, (cells, lanes), 1)
    sub = lax.broadcasted_iota(jnp.int32, (cells, lanes), 0)
    block = 2 * (tile - 1) + half
    edge = (block == 0) | (block == last)

    def landed(ref, fill, sem):
        @pl.when(edge)
        def _():
            whole(ref.at[:, pl.ds(0, width - 1)], sem)

        @pl.when(jnp.logical_not(edge))
        def _():
            whole(ref, sem)

        for number, slot_at in ((0, 0), (last, width - 1)):

            @pl.when(block == number)
            def _():
                for s in range(2):
                    ref[s, slot_at] = jnp.full((cells, lanes), fill, jnp.float32)

    first = keep * block - 1

    def lanes_of(field):
        return lane[: field.shape[0]]

    def ahead_y(fields, g):
        after = fields[(g + 1) % len(fields)]
        return jnp.where(
            lanes_of(fields[g]) < lanes - depth,
            pltpu.roll(fields[g], lanes - depth, 1),
            pltpu.roll(after, lanes - depth, 1),
        )

    def behind_y(fields, g):
        return jnp.where(
            lanes_of(fields[g]) < depth,
            pltpu.roll(fields[g - 1], depth, 1),
            pltpu.roll(fields[g], depth, 1),
        )

    def steps(mask):
        return jnp.where(mask, TAU, 0.0), jnp.where(mask, TAU * WEAK, 0.0)

    def limits(high, count, x_inside, y_first):
        lane_of = lane[:high]
        along_y = []
        for g in range(count):
            y = fold * (y_first + g) + lane_of // depth
            along_y.append(steps((y >= 0) & (y < rows - 1)))
        return steps(x_inside), along_y, steps(lane_of % depth < depth - 1)

    def weights(regions, bounds):
        along_x, along_y, along_z = bounds
        high = regions[0].shape[0]
        count = len(regions)
        up_y = [jnp.where(ahead_y(regions, g) == regions[g], *along_y[g]) for g in range(count)]
        result = []
        for g in range(count):
            mine = regions[g]
            up_x = jnp.where(pltpu.roll(mine, high - 1, 0) == mine, *along_x)
            up_z = jnp.where(pltpu.roll(mine, lanes - 1, 1) == mine, *along_z)
            down_x = pltpu.roll(up_x, 1, 0)
            down_z = pltpu.roll(up_z, 1, 1)
            down_y = behind_y(up_y, g)
            middle = 1.0 - (((up_x + down_x) + (up_z + down_z)) + (up_y[g] + down_y))
            result.append((middle, up_x, down_x, up_y[g], down_y, up_z, down_z))
        return result

    def swept(fields, factors, g):
        f = fields[g]
        high = f.shape[0]
        middle, up_x, down_x, up_y, down_y, up_z, down_z = factors
        return (
            (middle * f + up_x * pltpu.roll(f, high - 1, 0))
            + (down_x * pltpu.roll(f, 1, 0) + up_z * pltpu.roll(f, lanes - 1, 1))
        ) + (
            down_z * pltpu.roll(f, 1, 1)
            + (up_y * ahead_y(fields, g) + down_y * behind_y(fields, g))
        )

    def transposed(p):
        result = []
        for start in range(0, p.shape[0] // cells, fold):
            chunk = p[cells * start : cells * (start + fold)]
            found = chunk.shape[0] // cells
            flipped = jnp.concatenate([chunk] + [chunk[:cells]] * (fold - found), axis=0).T
            for g in range(found):
                piece = flipped[0:depth]
                if g:
                    piece = pltpu.roll(piece, (lanes - depth * g) % lanes, 1)
                for b in range(1, fold):
                    part_b = flipped[depth * b : depth * (b + 1)]
                    amount = (depth * (b - g)) % lanes
                    if amount:
                        part_b = pltpu.roll(part_b, amount, 1)
                    piece = jnp.where(lane // depth == b, part_b, piece)
                result.append(piece)
        return result

    @pl.when(works)
    def _():
        mat_copy.wait_recv()
        bounds = limits(cells, width, sub < cells - 1, first)
        blurs = []
        for s in range(2):
            matrix = jnp.where(same_block, jnp.concatenate([mats[s]] * fold, axis=0), 0.0)
            blurs.append((widened(matrix), widened(matrix.T)))
        landed(held, 1.0, data_sem)

        def paired_of(chosen, currents):
            corrections = []
            for s in range(2):
                recorded = jnp.concatenate([held[s, g] for g in chosen], axis=0)
                current = recorded if currents is None else jnp.concatenate(currents[s], axis=0)
                ratio = recorded / blurred(current, blurs[s][0])
                corrections.append(blurred(ratio, blurs[s][1]))
            return jnp.sqrt(corrections[0] * corrections[1])

        def swapped_over(step, begin, size):
            copy = pltpu.make_async_remote_copy(
                src_ref=outgoing.at[step, pl.ds(begin, size)],
                dst_ref=incoming.at[step, pl.ds(begin, size)],
                send_sem=send,
                recv_sem=swap_sem.at[step],
                device_id=across,
                device_id_type=mesh_id,
            )
            copy.start()
            return copy

        paired = paired_of(range(width), None)
        for g, piece in enumerate(transposed(paired)):
            outgoing[0, g] = piece
        swap = swapped_over(0, 0, width)
        pl.semaphore_wait(late_sem, 2 * ends)
        start_sides()
        landed(held_labels, 0.0, label_sem)
        for s in range(2):
            found = weights([held_labels[s, g] for g in range(width)], bounds)
            for g in range(width):
                for i in range(len(found[g])):
                    coef[i, s, g] = found[g][i]
        swap.wait_recv()
        joined = [
            jnp.sqrt(paired[cells * g : cells * (g + 1)] * incoming[0, g]) for g in range(width)
        ]
        fields = [[held[s, g] * joined[g] for g in range(width)] for s in range(2)]
        inner = range(1, width - 1)
        for sweep in range(SWEEPS):
            kept = inner if sweep == SWEEPS - 1 else range(width)
            fresh = [list(fields[s]) for s in range(2)]
            for s in range(2):
                for g in kept:
                    factors = [coef[i, s, g] for i in range(coef.shape[0])]
                    fresh[s][g] = swept(fields[s], factors, g)
            fields = fresh

        currents = [[fields[s][g] for g in inner] for s in range(2)]
        paired = paired_of(inner, currents)
        for s in range(2):
            for k in range(len(inner)):
                est[s, k] = currents[s][k]
        for k, piece in enumerate(transposed(paired)):
            outgoing[1, k] = piece
        swap = swapped_over(1, 0, len(inner))
        swap.wait_recv()
        for k in range(len(inner)):
            joined = jnp.sqrt(paired[cells * k : cells * (k + 1)] * incoming[1, k])
            for s in range(2):
                leave[s, k, pad : pad + cells] = est[s, k] * joined

        def window(h, t):
            flipped = core == 1 - h
            return pl.ds(pl.multiple_of(jnp.where(flipped, tiles - 1 - t, t) * slab, 8), span)

        def returned(h, t):
            return pltpu.make_async_remote_copy(
                src_ref=leave.at[h, :, window(h, t), :],
                dst_ref=back.at[own],
                send_sem=send,
                recv_sem=back_sem,
                device_id=at_device(h, t),
                device_id_type=mesh_id,
            )

        own = pl.ds(keep * block, keep)
        returned(0, 0).start()
        returned(1, 0).start()
        returned(1, tiles - 1).start()
        returned(0, tiles - 1).start()
        for t in range(1, tiles - 1):
            returned(1 - half, t).start()

            @pl.when(tile == t)
            def _():
                pltpu.make_async_copy(
                    leave.at[half, :, window(half, t), :], back.at[own], back_sem
                ).start()

            @pl.when(tile != t)
            def _():
                returned(half, t).start()

    pl.when(idle)(start_sides)

    @pl.when(has_below)
    def _():
        beside(0).wait_recv()

    @pl.when(has_above)
    def _():
        beside(1).wait_recv()

    x_at = place * slab - pad + sub[:span]
    x_inside = (x_at >= 0) & (x_at < cells - 1) & (sub[:span] < span - 1)
    bounds = limits(span, groups, x_inside, 0)
    found = weights([around[g, slab - pad : 2 * slab + pad] for g in range(groups)], bounds)
    for g in range(groups):
        for i in range(len(found[g])):
            slab_coef[i, g] = found[g][i]

    swaps = (width + keep) * cells
    pieces = 2 * workers * width - 2

    def all_sent(kept_back, more):
        whole(sent.at[pl.ds(0, 2 * (pieces - kept_back) * slab + more)], send)

    sides = groups * slab
    after = depth + swaps + (2 * tiles - 1) * keep * span + 2 * sides
    pl.when(works & edge)(lambda: all_sent(width - 1, after))
    pl.when(works & jnp.logical_not(edge))(lambda: all_sent(width, after))
    pl.when(idle)(lambda: all_sent(0, sides))
    turned_twice = turn.astype(jnp.bfloat16)
    whole(back, back_sem)
    fields = [back[g] for g in range(groups)]
    for sweep in range(SWEEPS):
        fields = [
            swept(fields, [slab_coef[i, g] for i in range(slab_coef.shape[0])], g)
            for g in range(groups)
        ]
    for g in range(groups):
        settled[g] = fields[g][pad : pad + slab]
    for j in range(blocks):
        parts = []
        for k in range(fold):
            line = settled[:, fold * j + k, :]
            parts.append(
                jnp.concatenate(
                    [line, jnp.zeros((mixed.shape[1] // fold - groups, lanes), jnp.float32)], axis=0
                )
            )
        for b in range(fold):
            mixed[j, pl.ds(b, mixed.shape[1] // fold, stride=fold), :] = gathered(
                parts, [b] * fold, slot, depth
            )
        lined = product(
            jnp.concatenate([turned_twice] * 2, axis=1),
            jnp.concatenate(halves(mixed[j, 0:rows]), axis=1),
            ((1,), (1,)),
        )
        for k in range(fold):
            x = fold * j + k
            at = jnp.where(flip_x, slab - 1 - x, x)
            unpacked[pl.ds(at, 1)] = lined[depth * k : depth * (k + 1)][None]


def by_rows(data, labels, kernel, offsets):
    tiles = lax.axis_size("tile")
    _, slab, rows, depth = data.shape
    fold = 128 // depth
    tall = -(-rows // (8 * fold)) * 8 * fold
    groups = rows // fold
    cells = slab * tiles
    kept = groups // (2 * (tiles - 2))
    width = kept + 2
    span = slab + 2 * SWEEPS
    flat = (slab * depth, rows)
    wide = (2, width, cells, 128)
    strips = (groups + 2, slab, 128)
    sent = 4 * tiles * width * slab + depth + (width + kept) * cells + 2 * tiles * kept * span
    dma = pltpu.SemaphoreType.DMA
    taps = kernel.transpose(2, 0, 1)
    ready = pl.pallas_call(
        functools.partial(fused, tiles),
        out_shape=pltpu.VMEM((slab, depth, rows), jnp.float32),
        in_specs=[pl.BlockSpec(memory_space=pltpu.HBM)] * 4,
        out_specs=pl.BlockSpec(memory_space=pltpu.VMEM),
        scratch_shapes=[
            pltpu.VMEM(flat, jnp.float32),
            pltpu.VMEM(flat, jnp.int32),
            pltpu.VMEM(taps.shape, jnp.float32),
            pltpu.VMEM(offsets.shape, jnp.int32),
            pltpu.VMEM((slab * depth // 128, tall, 128), jnp.float32),
            pltpu.VMEM(strips, jnp.float32),
            pltpu.VMEM(strips, jnp.float32),
            pltpu.VMEM(wide, jnp.float32),
            pltpu.VMEM(wide, jnp.float32),
            pltpu.VMEM((2, depth, 128), jnp.float32),
            pltpu.VMEM((2, kept, cells, 128), jnp.float32),
            pltpu.VMEM((7,) + wide, jnp.float32),
            pltpu.VMEM((ITERS,) + wide[1:], jnp.float32),
            pltpu.VMEM((ITERS,) + wide[1:], jnp.float32),
            pltpu.VMEM((2, kept, cells + span - slab, 128), jnp.float32),
            pltpu.VMEM((groups, span, 128), jnp.float32),
            pltpu.VMEM((groups, 3 * slab, 128), jnp.float32),
            pltpu.VMEM((7, groups, span, 128), jnp.float32),
            pltpu.VMEM((groups, slab, 128), jnp.float32),
            pltpu.VMEM((sent, 128), jnp.float32),
            dma((4,)),
            dma(()),
            dma(()),
            dma(()),
            dma((ITERS,)),
            dma(()),
            dma((2,)),
            dma(()),
            pltpu.SemaphoreType.REGULAR,
        ],
        compiler_params=pltpu.CompilerParams(
            collective_id=0, has_side_effects=True
        ),
    )(data.transpose(0, 1, 3, 2), labels.transpose(0, 1, 3, 2), taps, offsets)
    return ready[None].transpose(0, 1, 3, 2)


def fits(data, tiles, views):
    _, slab, rows, depth = data.shape
    return (
        views == 4
        and depth * 4 == 128
        and slab * tiles == depth
        and slab == 8
        and tiles > 2
        and rows % (8 * (tiles - 2)) == 0
    )


def program(data, labels, kernel, offsets):
    if fits(data, lax.axis_size("tile"), lax.axis_size("view")):
        return by_rows(data, labels, kernel, offsets)
    return on_device(data, labels, kernel, offsets)


def solution(mesh):
    placed = (
        P(("parts", "view"), "tile", None, None),
        P(("parts", "view"), "tile", None, None),
        P("view", None, None),
        P("view", None),
    )
    return jax.shard_map(
        program,
        mesh=mesh,
        in_specs=placed,
        out_specs=P(("parts", "view"), "tile", None, None),
        check_vma=False,
    )
```

```python
import functools

import jax
import jax.numpy as jnp
from jax import lax
from jax.experimental import pallas as pl
from jax.experimental.pallas import tpu as pltpu
from jax.sharding import PartitionSpec as P

ITERS = 2
SWEEPS = 4


WEAK = 0.2
TAU = 0.15


def extended(cells, sides, width):
    for axis, dim in sides:
        count = lax.axis_size(axis)
        ends = count - 1
        head = lax.slice_in_dim(cells, 0, width, axis=dim)
        tail = lax.slice_in_dim(cells, cells.shape[dim] - width, cells.shape[dim], axis=dim)
        cells = jnp.concatenate(
            [
                lax.ppermute(tail, axis, [(i, (i + 1) % count) for i in range(ends)]),
                cells,
                lax.ppermute(head, axis, [((i + 1) % count, i) for i in range(ends)]),
            ],
            axis=dim,
        )
    return cells


def swapped(block, axis, stride):
    count = lax.axis_size(axis)
    route = []
    for low in range(count):
        high = low | 1 << stride
        if high != low and high < count:
            route += [(low, high), (high, low)]
    return lax.ppermute(block, axis, route)


def band(kernel, offsets):
    depth_cells = kernel.shape[0]
    taps = jnp.arange(kernel.shape[1], dtype=jnp.int32) - 4
    depth = jnp.arange(depth_cells, dtype=jnp.int32)
    index = jnp.clip(depth[:, None] + taps[None, :] + offsets[:, None], 0, depth_cells - 1)
    weight = kernel / jnp.sum(kernel, axis=1, keepdims=True)
    return (index, weight)


def axis_term(field, region, axis):
    count = field.shape[axis]
    upper = lax.slice_in_dim(field, 1, count, axis=axis)
    lower = lax.slice_in_dim(field, 0, count - 1, axis=axis)
    same = jnp.where(
        lax.slice_in_dim(region, 1, count, axis=axis)
        == lax.slice_in_dim(region, 0, count - 1, axis=axis),
        1.0,
        WEAK,
    )
    flux = same * (upper - lower)
    after = [(0, 0)] * 3
    before = [(0, 0)] * 3
    after[axis] = (0, 1)
    before[axis] = (1, 0)
    return jnp.pad(flux, after) - jnp.pad(flux, before)


def sweep_rows(field, region, first_row, total_rows):
    extent = field.shape[0]
    global_rows = first_row + jnp.arange(extent, dtype=jnp.int32)
    inside = ((global_rows >= 0) & (global_rows < total_rows)).astype(field.dtype)[:, None, None]
    same = jnp.where(region[1:] == region[:-1], 1.0, WEAK) * inside[1:] * inside[:-1]
    flux = same * (field[1:] - field[:-1])
    inner = field[1:-1]
    inner_labels = region[1:-1]
    total = (
        flux[1:] - flux[:-1] + axis_term(inner, inner_labels, 1) + axis_term(inner, inner_labels, 2)
    )
    return inner + TAU * total


def regroup(received, tiles):
    slab, rows, depth_cells = received.shape
    blocks = received.reshape(slab, rows, tiles, depth_cells // tiles)
    return blocks.transpose(3, 1, 2, 0).reshape(depth_cells // tiles, rows, depth_cells)


def on_device(data, labels, kernel, offsets):
    recorded = data[0]
    region = labels[0]
    index, weight = band(kernel[0], offsets[0])
    tiles = lax.axis_size("tile")
    slab, rows, depth_cells = recorded.shape
    total_rows = slab * tiles
    start = lax.axis_index("tile") * slab
    parity = lax.axis_index("view") % 2
    columns = jnp.arange(depth_cells, dtype=jnp.int32)
    matrix = jnp.sum(weight[:, :, None] * (index[:, :, None] == columns[None, None, :]), axis=1)
    label_ext = extended(region, (("tile", 0),), 4)
    current = recorded
    for step in range(ITERS):
        forward_flat = jnp.dot(
            current.reshape(-1, depth_cells), matrix.T, precision=lax.Precision.HIGHEST
        )
        field = recorded / forward_flat.reshape(current.shape)
        flat = jnp.dot(field.reshape(-1, depth_cells), matrix, precision=lax.Precision.HIGHEST)
        correction = flat.reshape(field.shape)
        turned = correction
        for repeat in range(2):
            turned = regroup(
                lax.all_to_all(
                    jnp.flip(turned, 2), "tile", split_axis=2, concat_axis=2, tiled=True
                ),
                tiles,
            )
        turned = swapped(turned, "view", 1)
        paired = jnp.sqrt(correction * turned)
        outgoing = jnp.where(parity == 0, jnp.flip(paired, 2), paired)
        rotated = regroup(
            lax.all_to_all(outgoing, "tile", split_axis=2, concat_axis=2, tiled=True), tiles
        )
        rotated = jnp.where(parity == 1, jnp.flip(rotated, 2), rotated)
        partner = swapped(rotated, "view", 0)
        current = current * jnp.sqrt(paired * partner)
        widened = extended(current, (("tile", 0),), 4)
        for sweep in range(SWEEPS):
            extent = widened.shape[0]
            widened = sweep_rows(
                widened, label_ext[sweep : sweep + extent], start - 4 + sweep, total_rows
            )
        current = widened
    return current[None]


def gathered(parts, b_of, slot, depth):
    fold = len(parts)
    lanes = parts[0].shape[1]
    total = None
    for k in range(fold):
        amount = (depth * (k - b_of[k])) % lanes
        piece = pltpu.roll(parts[k], amount, 1) if amount else parts[k]
        total = piece if total is None else jnp.where(slot == k, piece, total)
    return total


def turning(lanes, depth, flip_z):
    row_ids = lax.broadcasted_iota(jnp.int32, (lanes, lanes), 0)
    lane_ids = lax.broadcasted_iota(jnp.int32, (lanes, lanes), 1)
    same_block = (row_ids // depth) == (lane_ids // depth)
    aim = jnp.where(flip_z, depth - 1 - lane_ids % depth, lane_ids % depth)
    return same_block, jnp.where(same_block & (row_ids % depth == aim), 1.0, 0.0).astype(jnp.float32)


def exact(a, b):
    return jnp.dot(a, b, precision=lax.Precision.HIGHEST, preferred_element_type=jnp.float32)


def product(a, b, contract):
    return lax.dot_general(a, b, (contract, ((), ())), preferred_element_type=jnp.float32)


def halves(a):
    high = a.astype(jnp.bfloat16)
    return high, (a - high.astype(jnp.float32)).astype(jnp.bfloat16)


def permuted(a, turn):
    high, low = halves(a)
    turn = turn.astype(jnp.bfloat16)
    return product(high, turn, ((1,), (0,))) + product(low, turn, ((1,), (0,)))


def widened(matrix):
    high, low = halves(matrix)
    none = jnp.zeros_like(high)
    return jnp.concatenate(
        [jnp.concatenate([high, low], axis=1), jnp.concatenate([high, none], axis=1)], axis=0
    )


def blurred(a, wide):
    both = product(jnp.concatenate(halves(a), axis=1), wide, ((1,), (0,)))
    lanes = a.shape[1]
    return both[:, :lanes] + both[:, lanes:]


def fused(tiles, data_ref, labels_ref, taps_ref, shift_ref, unpacked, raw, raw_labels, taps_buf, shift_buf, mixed, packed, packed_labels, held, held_labels, mats, est, coef, outgoing, incoming, leave, back, around, slab_coef, settled, sent, in_sem, data_sem, label_sem, mat_sem, swap_sem, back_sem, side_sem, send, late_sem):
    mesh_id = pl.DeviceIdType.MESH
    slab, depth, rows = data_ref.shape[1:]
    lanes = packed.shape[2]
    fold = lanes // depth
    groups = rows // fold
    width = held.shape[1]
    keep = width - 2
    cells = held.shape[2]
    span = back.shape[1]
    pad = (span - slab) // 2
    view = lax.axis_index("view")
    tile = lax.axis_index("tile")
    part = lax.axis_index("parts")
    half = view // 2
    core = view % 2
    workers = tiles - 2
    ends = tiles - workers
    works = (tile > 0) & (tile <= workers)
    idle = (tile == 0) | (tile > workers)
    flip_x = (view == 1) | (view == 2)
    flip_z = view >= 2

    def at_device(h, t):
        return (part, 2 * h + core, t)

    across = (part, 2 * half + 1 - core, tile)

    barrier = pltpu.get_barrier_semaphore()

    @pl.when(works)
    def _():
        for d in range(1, tiles):
            for h in (1 - half, half):
                pl.semaphore_signal(
                    barrier,
                    inc=1,
                    device_id=at_device(h, (tile + d) % tiles),
                    device_id_type=mesh_id,
                )
        pl.semaphore_signal(
            barrier, inc=1, device_id=at_device(1 - half, tile), device_id_type=mesh_id
        )

    pl.semaphore_signal(barrier, inc=1, device_id=across, device_id_type=mesh_id)

    small = [
        pltpu.make_async_copy(taps_ref, taps_buf, in_sem.at[2]),
        pltpu.make_async_copy(shift_ref, shift_buf, in_sem.at[3]),
    ]
    for copy in small:
        copy.start()

    for source, target, sem in ((data_ref, raw, 0), (labels_ref, raw_labels, 1)):
        for x in range(slab):
            at = jnp.where(flip_x, slab - 1 - x, x)
            pltpu.make_async_copy(
                source.at[0, x],
                target.at[pl.ds(pl.multiple_of(at * depth, 8), depth)],
                in_sem.at[sem],
            ).start()
    def whole(ref, sem):
        pltpu.make_async_copy(ref, ref, sem).wait()

    same_block, turn = turning(lanes, depth, flip_z)
    slot = lax.broadcasted_iota(jnp.int32, (mixed.shape[1] // fold, lanes), 1) // depth
    blocks = slab * depth // lanes

    def pack(source, target, fill, turner):
        for j in range(blocks):
            mixed[j, 0:rows] = turner(source[lanes * j : lanes * (j + 1), :])
        for j in range(blocks):
            parts = [
                mixed[j, pl.ds(b, mixed.shape[1] // fold, stride=fold), :] for b in range(fold)
            ]
            for k in range(fold):
                line = gathered(parts, [k] * fold, slot, depth)
                target[1 : groups + 1, fold * j + k, :] = line[:groups]

    def turned_labels(block):
        block = block.astype(jnp.float32).T.astype(jnp.bfloat16)
        return product(block, turn.astype(jnp.bfloat16), ((1,), (0,)))

    place = jnp.where(flip_x, tiles - 1 - tile, tile)
    spot = pl.ds(pl.multiple_of(place * slab, 8), slab)

    last = 2 * workers - 1
    homes = [(h, t) for t in range(1, workers + 1) for h in range(2)]

    def scatter(source, target, sem):
        for a in range(2):
            for own in range(tiles):

                @pl.when((half == a) & (tile == own))
                def _():
                    for h, t in sorted(homes, key=lambda ht: (-abs(ht[1] - own), ht[0] == a)):
                        number = 2 * (t - 1) + h
                        low = 1 if number == 0 else 0
                        size = width - (number in (0, last))
                        src = source.at[pl.ds(keep * number + low, size)]
                        dst = target.at[a, pl.ds(low, size), spot, :]
                        if (h, t) == (a, own):
                            copy = pltpu.make_async_copy(src, dst, sem)
                        else:
                            copy = pltpu.make_async_remote_copy(
                                src_ref=src,
                                dst_ref=dst,
                                send_sem=send,
                                recv_sem=sem,
                                device_id=at_device(h, t),
                                device_id_type=mesh_id,
                            )
                        copy.start()

    for copy in small:
        copy.wait()
    @pl.when(works)
    def _():
        count = taps_buf.shape[0]
        taps = [jnp.concatenate([taps_buf[k]] * fold, axis=1) for k in range(count)]
        scale = taps[0]
        for k in range(1, count):
            scale = scale + taps[k]
        shift = jnp.concatenate([shift_buf[...]] * fold, axis=1)
        level = lax.broadcasted_iota(jnp.int32, (1, lanes), 1) % depth
        strip_row = lax.broadcasted_iota(jnp.int32, (depth, lanes), 0)
        strip_aim = jnp.where(flip_z, depth - 1 - strip_row, strip_row)
        strip = jnp.zeros((depth, lanes), jnp.float32)
        for k in range(count):
            index = jnp.clip(level + (k - 4) + shift, 0, depth - 1)
            strip = strip + jnp.where(index == strip_aim, taps[k] / scale, 0.0)
        strip = exact(strip, turn)
        mats[pl.ds(half, 1)] = strip[None]

    mat_copy = pltpu.make_async_remote_copy(
        src_ref=mats.at[half],
        dst_ref=mats.at[half],
        send_sem=send,
        recv_sem=mat_sem,
        device_id=at_device(1 - half, tile),
        device_id_type=mesh_id,
    )

    whole(raw, in_sem.at[0])
    pack(raw, packed, 1.0, lambda v: permuted(v.T, turn))
    pl.semaphore_wait(barrier, jnp.where(works, 2 * workers, 2 * workers + 1))

    @pl.when(idle)
    def _():
        for t in range(1, workers + 1):
            for h in (1 - half, half):
                pl.semaphore_signal(
                    late_sem, inc=1, device_id=at_device(h, t), device_id_type=mesh_id
                )

    pl.when(works)(mat_copy.start)
    scatter(packed, held, data_sem)

    whole(raw_labels, in_sem.at[1])
    pack(raw_labels, packed_labels, 0.0, turned_labels)
    pl.when((core == 1) & idle)(lambda: pl.delay(2200))
    scatter(packed_labels, held_labels, label_sem)

    inner_labels = packed_labels.at[pl.ds(1, groups)]

    def beside(side):
        onto = place + 1 - 2 * side
        t = jnp.where(flip_x, tiles - 1 - onto, onto)
        return pltpu.make_async_remote_copy(
            src_ref=inner_labels,
            dst_ref=around.at[:, pl.ds(2 * slab * side, slab), :],
            send_sem=send,
            recv_sem=side_sem.at[side],
            device_id=(part, view, jnp.clip(t, 0, tiles - 1)),
            device_id_type=mesh_id,
        )

    has_above = place < tiles - 1
    has_below = place > 0

    def start_sides():
        @pl.when(has_above)
        def _():
            beside(0).start()

        @pl.when(has_below)
        def _():
            beside(1).start()

    @pl.when(jnp.logical_not(has_below))
    def _():
        around[:, 0:slab, :] = jnp.zeros((groups, slab, lanes), jnp.float32)

    @pl.when(jnp.logical_not(has_above))
    def _():
        around[:, 2 * slab : 3 * slab, :] = jnp.zeros((groups, slab, lanes), jnp.float32)

    around[:, slab : 2 * slab, :] = packed_labels[1 : groups + 1]
    for s in range(2):
        for k in range(leave.shape[1]):
            leave[s, k, 0:pad] = jnp.zeros((pad, lanes), jnp.float32)
            leave[s, k, pad + cells : 2 * pad + cells] = jnp.zeros((pad, lanes), jnp.float32)

    lane = lax.broadcasted_iota(jnp.int32, (cells, lanes), 1)
    sub = lax.broadcasted_iota(jnp.int32, (cells, lanes), 0)
    block = 2 * (tile - 1) + half
    edge = (block == 0) | (block == last)

    def landed(ref, fill, sem):
        @pl.when(edge)
        def _():
            whole(ref.at[:, pl.ds(0, width - 1)], sem)

        @pl.when(jnp.logical_not(edge))
        def _():
            whole(ref, sem)

        for number, slot_at in ((0, 0), (last, width - 1)):

            @pl.when(block == number)
            def _():
                for s in range(2):
                    ref[s, slot_at] = jnp.full((cells, lanes), fill, jnp.float32)

    first = keep * block - 1

    def lanes_of(field):
        return lane[: field.shape[0]]

    def ahead_y(fields, g):
        after = fields[(g + 1) % len(fields)]
        return jnp.where(
            lanes_of(fields[g]) < lanes - depth,
            pltpu.roll(fields[g], lanes - depth, 1),
            pltpu.roll(after, lanes - depth, 1),
        )

    def behind_y(fields, g):
        return jnp.where(
            lanes_of(fields[g]) < depth,
            pltpu.roll(fields[g - 1], depth, 1),
            pltpu.roll(fields[g], depth, 1),
        )

    def steps(mask):
        return jnp.where(mask, TAU, 0.0), jnp.where(mask, TAU * WEAK, 0.0)

    def limits(high, count, x_inside, y_first):
        lane_of = lane[:high]
        along_y = []
        for g in range(count):
            y = fold * (y_first + g) + lane_of // depth
            along_y.append(steps((y >= 0) & (y < rows - 1)))
        return steps(x_inside), along_y, steps(lane_of % depth < depth - 1)

    def weights(regions, bounds):
        along_x, along_y, along_z = bounds
        high = regions[0].shape[0]
        count = len(regions)
        up_y = [jnp.where(ahead_y(regions, g) == regions[g], *along_y[g]) for g in range(count)]
        result = []
        for g in range(count):
            mine = regions[g]
            up_x = jnp.where(pltpu.roll(mine, high - 1, 0) == mine, *along_x)
            up_z = jnp.where(pltpu.roll(mine, lanes - 1, 1) == mine, *along_z)
            down_x = pltpu.roll(up_x, 1, 0)
            down_z = pltpu.roll(up_z, 1, 1)
            down_y = behind_y(up_y, g)
            middle = 1.0 - (((up_x + down_x) + (up_z + down_z)) + (up_y[g] + down_y))
            result.append((middle, up_x, down_x, up_y[g], down_y, up_z, down_z))
        return result

    def swept(fields, factors, g):
        f = fields[g]
        high = f.shape[0]
        middle, up_x, down_x, up_y, down_y, up_z, down_z = factors
        return (
            (middle * f + up_x * pltpu.roll(f, high - 1, 0))
            + (down_x * pltpu.roll(f, 1, 0) + up_z * pltpu.roll(f, lanes - 1, 1))
        ) + (
            down_z * pltpu.roll(f, 1, 1)
            + (up_y * ahead_y(fields, g) + down_y * behind_y(fields, g))
        )

    def transposed(p):
        result = []
        for start in range(0, p.shape[0] // cells, fold):
            chunk = p[cells * start : cells * (start + fold)]
            found = chunk.shape[0] // cells
            flipped = jnp.concatenate([chunk] + [chunk[:cells]] * (fold - found), axis=0).T
            for g in range(found):
                piece = flipped[0:depth]
                if g:
                    piece = pltpu.roll(piece, (lanes - depth * g) % lanes, 1)
                for b in range(1, fold):
                    part_b = flipped[depth * b : depth * (b + 1)]
                    amount = (depth * (b - g)) % lanes
                    if amount:
                        part_b = pltpu.roll(part_b, amount, 1)
                    piece = jnp.where(lane // depth == b, part_b, piece)
                result.append(piece)
        return result

    @pl.when(works)
    def _():
        mat_copy.wait_recv()
        bounds = limits(cells, width, sub < cells - 1, first)
        blurs = []
        for s in range(2):
            matrix = jnp.where(same_block, jnp.concatenate([mats[s]] * fold, axis=0), 0.0)
            blurs.append((widened(matrix), widened(matrix.T)))
        landed(held, 1.0, data_sem)

        def paired_of(chosen, currents):
            corrections = []
            for s in range(2):
                recorded = jnp.concatenate([held[s, g] for g in chosen], axis=0)
                current = recorded if currents is None else jnp.concatenate(currents[s], axis=0)
                ratio = recorded / blurred(current, blurs[s][0])
                corrections.append(blurred(ratio, blurs[s][1]))
            return jnp.sqrt(corrections[0] * corrections[1])

        def swapped_over(step, begin, size):
            copy = pltpu.make_async_remote_copy(
                src_ref=outgoing.at[step, pl.ds(begin, size)],
                dst_ref=incoming.at[step, pl.ds(begin, size)],
                send_sem=send,
                recv_sem=swap_sem.at[step],
                device_id=across,
                device_id_type=mesh_id,
            )
            copy.start()
            return copy

        paired = paired_of(range(width), None)
        for g, piece in enumerate(transposed(paired)):
            outgoing[0, g] = piece
        swap = swapped_over(0, 0, width)
        pl.semaphore_wait(late_sem, 2 * ends)
        start_sides()
        landed(held_labels, 0.0, label_sem)
        for s in range(2):
            found = weights([held_labels[s, g] for g in range(width)], bounds)
            for g in range(width):
                for i in range(len(found[g])):
                    coef[i, s, g] = found[g][i]
        swap.wait_recv()
        joined = [
            jnp.sqrt(paired[cells * g : cells * (g + 1)] * incoming[0, g]) for g in range(width)
        ]
        fields = [[held[s, g] * joined[g] for g in range(width)] for s in range(2)]
        inner = range(1, width - 1)
        for sweep in range(SWEEPS):
            kept = inner if sweep == SWEEPS - 1 else range(width)
            fresh = [list(fields[s]) for s in range(2)]
            for s in range(2):
                for g in kept:
                    factors = [coef[i, s, g] for i in range(coef.shape[0])]
                    fresh[s][g] = swept(fields[s], factors, g)
            fields = fresh

        currents = [[fields[s][g] for g in inner] for s in range(2)]
        paired = paired_of(inner, currents)
        for s in range(2):
            for k in range(len(inner)):
                est[s, k] = currents[s][k]
        for k, piece in enumerate(transposed(paired)):
            outgoing[1, k] = piece
        swap = swapped_over(1, 0, len(inner))
        swap.wait_recv()
        for k in range(len(inner)):
            joined = jnp.sqrt(paired[cells * k : cells * (k + 1)] * incoming[1, k])
            for s in range(2):
                leave[s, k, pad : pad + cells] = est[s, k] * joined

        def window(h, t):
            flipped = core == 1 - h
            return pl.ds(pl.multiple_of(jnp.where(flipped, tiles - 1 - t, t) * slab, 8), span)

        def returned(h, t):
            return pltpu.make_async_remote_copy(
                src_ref=leave.at[h, :, window(h, t), :],
                dst_ref=back.at[own],
                send_sem=send,
                recv_sem=back_sem,
                device_id=at_device(h, t),
                device_id_type=mesh_id,
            )

        own = pl.ds(keep * block, keep)
        returned(0, 0).start()
        returned(1, 0).start()
        returned(1, tiles - 1).start()
        returned(0, tiles - 1).start()
        for t in range(1, tiles - 1):
            returned(1 - half, t).start()

            @pl.when(tile == t)
            def _():
                pltpu.make_async_copy(
                    leave.at[half, :, window(half, t), :], back.at[own], back_sem
                ).start()

            @pl.when(tile != t)
            def _():
                returned(half, t).start()

    pl.when(idle)(start_sides)

    @pl.when(has_below)
    def _():
        beside(0).wait_recv()

    @pl.when(has_above)
    def _():
        beside(1).wait_recv()

    x_at = place * slab - pad + sub[:span]
    x_inside = (x_at >= 0) & (x_at < cells - 1) & (sub[:span] < span - 1)
    bounds = limits(span, groups, x_inside, 0)
    found = weights([around[g, slab - pad : 2 * slab + pad] for g in range(groups)], bounds)
    for g in range(groups):
        for i in range(len(found[g])):
            slab_coef[i, g] = found[g][i]

    swaps = (width + keep) * cells
    pieces = 2 * workers * width - 2

    def all_sent(kept_back, more):
        whole(sent.at[pl.ds(0, 2 * (pieces - kept_back) * slab + more)], send)

    sides = groups * slab
    after = depth + swaps + (2 * tiles - 1) * keep * span + 2 * sides
    pl.when(works & edge)(lambda: all_sent(width - 1, after))
    pl.when(works & jnp.logical_not(edge))(lambda: all_sent(width, after))
    pl.when(idle)(lambda: all_sent(0, sides))
    turned_twice = turn.astype(jnp.bfloat16)
    whole(back, back_sem)
    fields = [back[g] for g in range(groups)]
    for sweep in range(SWEEPS):
        fields = [
            swept(fields, [slab_coef[i, g] for i in range(slab_coef.shape[0])], g)
            for g in range(groups)
        ]
    for g in range(groups):
        settled[g] = fields[g][pad : pad + slab]
    for j in range(blocks):
        parts = []
        for k in range(fold):
            line = settled[:, fold * j + k, :]
            parts.append(
                jnp.concatenate(
                    [line, jnp.zeros((mixed.shape[1] // fold - groups, lanes), jnp.float32)], axis=0
                )
            )
        for b in range(fold):
            mixed[j, pl.ds(b, mixed.shape[1] // fold, stride=fold), :] = gathered(
                parts, [b] * fold, slot, depth
            )
        lined = product(
            jnp.concatenate([turned_twice] * 2, axis=1),
            jnp.concatenate(halves(mixed[j, 0:rows]), axis=1),
            ((1,), (1,)),
        )
        for k in range(fold):
            x = fold * j + k
            at = jnp.where(flip_x, slab - 1 - x, x)
            unpacked[pl.ds(at, 1)] = lined[depth * k : depth * (k + 1)][None]


def by_rows(data, labels, kernel, offsets):
    tiles = lax.axis_size("tile")
    _, slab, rows, depth = data.shape
    fold = 128 // depth
    tall = -(-rows // (8 * fold)) * 8 * fold
    groups = rows // fold
    cells = slab * tiles
    kept = groups // (2 * (tiles - 2))
    width = kept + 2
    span = slab + 2 * SWEEPS
    flat = (slab * depth, rows)
    wide = (2, width, cells, 128)
    strips = (groups + 2, slab, 128)
    sent = 4 * tiles * width * slab + depth + (width + kept) * cells + 2 * tiles * kept * span
    dma = pltpu.SemaphoreType.DMA
    taps = kernel.transpose(2, 0, 1)
    ready = pl.pallas_call(
        functools.partial(fused, tiles),
        out_shape=pltpu.VMEM((slab, depth, rows), jnp.float32),
        in_specs=[pl.BlockSpec(memory_space=pltpu.HBM)] * 4,
        out_specs=pl.BlockSpec(memory_space=pltpu.VMEM),
        scratch_shapes=[
            pltpu.VMEM(flat, jnp.float32),
            pltpu.VMEM(flat, jnp.int32),
            pltpu.VMEM(taps.shape, jnp.float32),
            pltpu.VMEM(offsets.shape, jnp.int32),
            pltpu.VMEM((slab * depth // 128, tall, 128), jnp.float32),
            pltpu.VMEM(strips, jnp.float32),
            pltpu.VMEM(strips, jnp.float32),
            pltpu.VMEM(wide, jnp.float32),
            pltpu.VMEM(wide, jnp.float32),
            pltpu.VMEM((2, depth, 128), jnp.float32),
            pltpu.VMEM((2, kept, cells, 128), jnp.float32),
            pltpu.VMEM((7,) + wide, jnp.float32),
            pltpu.VMEM((ITERS,) + wide[1:], jnp.float32),
            pltpu.VMEM((ITERS,) + wide[1:], jnp.float32),
            pltpu.VMEM((2, kept, cells + span - slab, 128), jnp.float32),
            pltpu.VMEM((groups, span, 128), jnp.float32),
            pltpu.VMEM((groups, 3 * slab, 128), jnp.float32),
            pltpu.VMEM((7, groups, span, 128), jnp.float32),
            pltpu.VMEM((groups, slab, 128), jnp.float32),
            pltpu.VMEM((sent, 128), jnp.float32),
            dma((4,)),
            dma(()),
            dma(()),
            dma(()),
            dma((ITERS,)),
            dma(()),
            dma((2,)),
            dma(()),
            pltpu.SemaphoreType.REGULAR,
        ],
        compiler_params=pltpu.CompilerParams(
            collective_id=0, has_side_effects=True
        ),
    )(data.transpose(0, 1, 3, 2), labels.transpose(0, 1, 3, 2), taps, offsets)
    return ready[None].transpose(0, 1, 3, 2)


def fits(data, tiles, views):
    _, slab, rows, depth = data.shape
    return (
        views == 4
        and depth * 4 == 128
        and slab * tiles == depth
        and slab == 8
        and tiles > 2
        and rows % (8 * (tiles - 2)) == 0
    )


def program(data, labels, kernel, offsets):
    if fits(data, lax.axis_size("tile"), lax.axis_size("view")):
        return by_rows(data, labels, kernel, offsets)
    return on_device(data, labels, kernel, offsets)


def solution(mesh):
    placed = (
        P(("parts", "view"), "tile", None, None),
        P(("parts", "view"), "tile", None, None),
        P("view", None, None),
        P("view", None),
    )
    return jax.shard_map(
        program,
        mesh=mesh,
        in_specs=placed,
        out_specs=P(("parts", "view"), "tile", None, None),
        check_vma=False,
    )
```
